32 devices in a mesh: image: 8 (over z, x), space: 4 (over y, core).
Axes of the slice: x: 2, y: 2, z: 4, core: 2. Of those that a mesh axis runs over, the one named last changes fastest.
Arguments:
- magnet: float32 [16, 3, 8, 256, 256], P('image', None, None, 'space'), may hold values from -1 to 1, as said below
- anisotropy: float32 [256], P('space'), may hold values from 0.25 to 10
- kernel: float32 [6, 16, 512, 512], P(None, 'space'), as said below
Outputs:
- updated_magnet: float32 [16, 3, 8, 256, 256], P('image', None, None, 'space')
- band_force: float32 [16, 3, 8, 256, 256], P('image', None, None, 'space')
- energy: float32 [16], P('image')
The draws below stay inside these ranges and needn't reach their ends.
Inputs may be any that keep to these rules, and one draw needn't show every extreme that they name: `magnet`: each cell's three components form a unit vector. `kernel`: each component is even under k -> -k modulo the padded length along every frequency index, except that xy is odd along x and y, xz odd along x and z, and yz odd along y and z.
All inputs are finite; a program needn't handle non-finite values.
Results may differ from the reference program's by a relative error of at most 0.0003.
Values sent between devices are 32-bit elements; how exact they have to be, the bound alone decides.
A program may use at most 256 MiB of HBM per device.

```python
import math
import jax
import jax.numpy as jnp
from jax import lax

NX = 256
NY = 256
NZ = 8
IMAGES = 16


def mirror_part(values, dimension, parity):
    mirrored = jnp.roll(jnp.flip(values, dimension), 1, dimension)
    return 0.5 * (values + parity * mirrored)


def draw_kernel(key, part):
    array_dims = (6, 2 * NZ, 2 * NX, 2 * NY)
    samples = jax.random.normal(key, array_dims, jnp.float32)
    parities = ((1.0, 1.0, 1.0), (1.0, 1.0, 1.0), (1.0, 1.0, 1.0), (-1.0, -1.0, 1.0), (-1.0, 1.0, -1.0), (1.0, -1.0, -1.0))
    components = []
    for component_index in range(6):
        parity_x, parity_y, parity_z = parities[component_index]
        component = mirror_part(samples[component_index], 0, parity_z)
        component = mirror_part(component, 1, parity_x)
        component = mirror_part(component, 2, parity_y)
        if component_index < 3:
            components.append(0.3 + 2.5 * component)
        else:
            components.append(2.0 * component)
    return jnp.stack(components)


def draw_anisotropy(key, part):
    position = jnp.arange(NX, dtype=jnp.float32) / (NX - 1)
    factor = jax.random.uniform(key, (NX,), jnp.float32, 0.5, 2.0)
    return 0.5 * jnp.power(10.0, position) * factor


def draw_magnet(key, part):
    array_dims = (IMAGES, 3, NZ, NX, NY)
    position = jnp.arange(NX, dtype=jnp.float32) / (NX - 1)
    samples = jax.random.normal(key, array_dims, jnp.float32)
    growth = 0.15 * jnp.power(3.0, position)
    lateral = 0.0
    scaled = samples * growth[None, None, None, :, None]
    scaled = scaled.at[0].set(samples[0])
    wandering = jnp.cumsum(scaled, axis=0)
    image_pos = jnp.arange(IMAGES, dtype=jnp.float32) / (IMAGES - 1)
    polar_offset = 2.0 * jnp.cos(math.pi * image_pos)
    offsets = jnp.stack([jnp.zeros_like(polar_offset), jnp.full_like(polar_offset, lateral), polar_offset], axis=1)
    direction = wandering + offsets[:, :, None, None, None]
    return direction / jnp.sqrt(jnp.sum(direction * direction, axis=1, keepdims=True))


def setup_inputs(seed: int = 0) -> dict:
    key_list = jax.random.split(jax.random.key(seed), 4)
    return {
        "magnet": draw_magnet(jax.random.fold_in(key_list[3], 71), 0),
        "anisotropy": draw_anisotropy(jax.random.fold_in(key_list[3], 71), 0),
        "kernel": draw_kernel(jax.random.fold_in(key_list[3], 71), 0),
    }


exchange_strength = 0.25
chiral_strength = 0.3
spring_strength = 10.0
step_limit = 1.0
rotation_limit = 0.5
epsilon = 1e-06

def lift_axes(values):
    return values[:, None, None, None, None]

def total_cells(values):
    return lax.optimization_barrier(jnp.sum(values, axis=tuple(range(1, values.ndim))))

def project(vector, magnet):
    return vector - lax.optimization_barrier(jnp.sum(vector * magnet, axis=1, keepdims=True)) * magnet

def angle_squared(first, second):
    normal_part = jnp.cross(first, second, axis=1)
    sine_value = jnp.sqrt(lax.optimization_barrier(jnp.sum(normal_part * normal_part, axis=1)))
    cosine = lax.optimization_barrier(jnp.sum(first * second, axis=1))
    return jnp.arctan2(sine_value, cosine) ** 2

def tangent_weights(energy_total, energy_next, energy_prior):
    rise_next = energy_next - energy_total
    rise_prior = energy_total - energy_prior
    upward = (rise_next > 0) & (rise_prior > 0)
    downward = (rise_next < 0) & (rise_prior < 0)
    larger = jnp.maximum(jnp.abs(rise_next), jnp.abs(rise_prior))
    smaller = jnp.minimum(jnp.abs(rise_next), jnp.abs(rise_prior))
    toward_next = energy_next > energy_prior
    weight_next = jnp.where(upward, 1.0, jnp.where(downward, 0.0, jnp.where(toward_next, larger, smaller)))
    weight_prior = jnp.where(upward, 0.0, jnp.where(downward, 1.0, jnp.where(toward_next, smaller, larger)))
    return (weight_next, weight_prior)

def local_fields(magnet, anisotropy):
    padded = jnp.pad(magnet, ((0, 0), (0, 0), (1, 1), (1, 1), (1, 1)))
    z_plus = padded[:, :, 2:, 1:-1, 1:-1]
    z_minus = padded[:, :, :-2, 1:-1, 1:-1]
    x_plus = padded[:, :, 1:-1, 2:, 1:-1]
    x_minus = padded[:, :, 1:-1, :-2, 1:-1]
    y_plus = padded[:, :, 1:-1, 1:-1, 2:]
    y_minus = padded[:, :, 1:-1, 1:-1, :-2]
    layer_pos = lax.broadcasted_iota(jnp.int32, (NZ, NX, NY), 0)
    row_pos = lax.broadcasted_iota(jnp.int32, (NZ, NX, NY), 1)
    column_pos = lax.broadcasted_iota(jnp.int32, (NZ, NX, NY), 2)
    boundary = (layer_pos == 0).astype(jnp.float32) + (layer_pos == NZ - 1).astype(jnp.float32)
    boundary = boundary + (row_pos == 0).astype(jnp.float32) + (row_pos == NX - 1).astype(jnp.float32)
    boundary = boundary + (column_pos == 0).astype(jnp.float32) + (column_pos == NY - 1).astype(jnp.float32)
    present = 6.0 - boundary
    neighbours = x_plus + x_minus + y_plus + y_minus + z_plus + z_minus
    exchange_part = exchange_strength * (neighbours - present * magnet)
    chiral_x = chiral_strength * (x_plus[:, 2] - x_minus[:, 2])
    chiral_y = chiral_strength * (y_plus[:, 2] - y_minus[:, 2])
    chiral_z = -chiral_strength * (x_plus[:, 0] - x_minus[:, 0] + (y_plus[:, 1] - y_minus[:, 1]))
    easy_axis = 2.0 * anisotropy[:, None] * magnet[:, 2]
    return exchange_part + jnp.stack([chiral_x, chiral_y, chiral_z + easy_axis], axis=1)

def demag_one(magnet_one, kernel):
    padded = jnp.pad(magnet_one, ((0, 0), (0, NZ), (0, NX), (0, NY)))
    spectrum = jnp.fft.fftn(padded, axes=(1, 2, 3))
    spec_x = spectrum[0]
    spec_y = spectrum[1]
    spec_z = spectrum[2]
    field_x = kernel[0] * spec_x + kernel[3] * spec_y + kernel[4] * spec_z
    field_y = kernel[3] * spec_x + kernel[1] * spec_y + kernel[5] * spec_z
    field_z = kernel[4] * spec_x + kernel[5] * spec_y + kernel[2] * spec_z
    inverse = jnp.fft.ifftn(jnp.stack([field_x, field_y, field_z]), axes=(1, 2, 3))
    return -jnp.real(inverse)[:, :NZ, :NX, :NY]

def reference(magnet, anisotropy, kernel):
    cell_count = NZ * NX * NY

    def one_image(magnet_one):
        return demag_one(magnet_one, kernel)
    demag = lax.map(one_image, magnet)
    fields = local_fields(magnet, anisotropy) + demag
    energy_total = -0.5 * total_cells(magnet * fields)
    next_image = jnp.concatenate([magnet[1:], magnet[-1:]], axis=0)
    prior_image = jnp.concatenate([magnet[:1], magnet[:-1]], axis=0)
    energy_next = jnp.concatenate([energy_total[1:], energy_total[-1:]])
    energy_prior = jnp.concatenate([energy_total[:1], energy_total[:-1]])
    true_force = project(fields, magnet)
    tangent_next = project(next_image - magnet, magnet)
    tangent_prior = project(magnet - prior_image, magnet)
    distance_next = jnp.sqrt(total_cells(angle_squared(magnet, next_image)) / cell_count)
    distance_prior = jnp.sqrt(total_cells(angle_squared(magnet, prior_image)) / cell_count)
    weight_next, weight_prior = tangent_weights(energy_total, energy_next, energy_prior)
    tangent = lift_axes(weight_next) * tangent_next + lift_axes(weight_prior) * tangent_prior
    length_mean = total_cells(tangent * tangent) / cell_count
    unit_tangent = tangent / lift_axes(jnp.sqrt(length_mean + epsilon))
    parallel = total_cells(true_force * unit_tangent) / cell_count
    spring = spring_strength * (distance_next - distance_prior)
    image_index = jnp.arange(IMAGES)
    interior = (image_index > 0) & (image_index < IMAGES - 1)
    band_force = jnp.where(lift_axes(interior), true_force + lift_axes(spring - parallel) * unit_tangent, 0.0)
    largest = lax.optimization_barrier(jnp.max(jnp.sqrt(lax.optimization_barrier(jnp.sum(band_force * band_force, axis=1))), axis=(1, 2, 3)))
    move_scale = jnp.minimum(step_limit, rotation_limit / (largest + epsilon))
    stepped = magnet + lift_axes(move_scale) * band_force
    updated = stepped / jnp.sqrt(lax.optimization_barrier(jnp.sum(stepped * stepped, axis=1, keepdims=True)))
    return (updated, band_force, energy_total / cell_count)
```

```python
import functools

import jax
import jax.numpy as jnp
import numpy as np
from jax import lax
from jax.experimental import pallas as pl
from jax.experimental.pallas import tpu as pltpu
from jax.sharding import PartitionSpec as P

exchange_strength = 0.25
chiral_strength = 0.3
spring_strength = 10.0
step_limit = 1.0
rotation_limit = 0.5
epsilon = 1e-06


def extended(cells, sides, width):
    for axis, dim in sides:
        count = lax.axis_size(axis)
        ends = count - 1
        head = lax.slice_in_dim(cells, 0, width, axis=dim)
        tail = lax.slice_in_dim(cells, cells.shape[dim] - width, cells.shape[dim], axis=dim)
        cells = jnp.concatenate(
            [
                lax.ppermute(tail, axis, [(i, (i + 1) % count) for i in range(ends)]),
                cells,
                lax.ppermute(head, axis, [((i + 1) % count, i) for i in range(ends)]),
            ],
            axis=dim,
        )
    return cells


def lift_axes(values):
    return values[:, None, None, None, None]


def total_cells(values):
    return jnp.sum(values, axis=tuple(range(1, values.ndim)))


def project(vector, magnet):
    return vector - jnp.sum(vector * magnet, axis=1, keepdims=True) * magnet


def angle_squared(first, second):
    normal_part = jnp.cross(first, second, axis=1)
    sine_value = jnp.sqrt(jnp.sum(normal_part * normal_part, axis=1))
    cosine = jnp.sum(first * second, axis=1)
    return jnp.arctan2(sine_value, cosine) ** 2


def tangent_weights(energy_total, energy_next, energy_prior):
    rise_next = energy_next - energy_total
    rise_prior = energy_total - energy_prior
    upward = (rise_next > 0) & (rise_prior > 0)
    downward = (rise_next < 0) & (rise_prior < 0)
    larger = jnp.maximum(jnp.abs(rise_next), jnp.abs(rise_prior))
    smaller = jnp.minimum(jnp.abs(rise_next), jnp.abs(rise_prior))
    toward_next = energy_next > energy_prior
    weight_next = jnp.where(
        upward, 1.0, jnp.where(downward, 0.0, jnp.where(toward_next, larger, smaller))
    )
    weight_prior = jnp.where(
        upward, 0.0, jnp.where(downward, 1.0, jnp.where(toward_next, smaller, larger))
    )
    return (weight_next, weight_prior)


def split_limbs(values):
    upper = values.astype(jnp.bfloat16)
    return upper, (values - upper.astype(jnp.float32)).astype(jnp.bfloat16)


def table_limbs(table):
    upper = table.astype(np.float32).astype(jnp.bfloat16)
    lower = (table - upper.astype(np.float64)).astype(np.float32).astype(jnp.bfloat16)
    return np.stack([upper, lower])


def parity_table(count):
    position = np.arange(count)[:, None]
    slot = np.arange(count)[None, :]
    turn = np.pi / count
    even_part = np.cos(turn * (position * slot % (2 * count)))
    odd_part = np.sin(turn * (position * slot % (2 * count)))
    odd_part[:, 0] = np.cos(turn * (position[:, 0] * count % (2 * count)))
    return np.concatenate([even_part, odd_part], axis=1)


def parity_weights(count):
    weights = np.full((2 * count,), 2.0)
    weights[0] = 1.0
    weights[count] = 1.0
    return weights


def half_table(count):
    place = np.arange(count)
    angle = np.pi * (place[:, None] * place[None, :] % (2 * count)) / count
    cosine, sine = np.cos(angle), np.sin(angle)
    cosine[np.abs(cosine) < 1e-12] = 0.0
    sine[np.abs(sine) < 1e-12] = 0.0
    return cosine, sine


def weighted(terms):
    total = None
    for weight, value in terms:
        weight = float(weight)
        if weight == 0.0:
            continue
        if total is None:
            total = value if weight == 1.0 else -value if weight == -1.0 else weight * value
        elif weight == 1.0:
            total = total + value
        elif weight == -1.0:
            total = total - value
        else:
            total = total + weight * value
    return total


def layers_to_spectrum(layers):
    count = len(layers)
    half = count // 2
    cosine, sine = half_table(count)
    sums = {z: layers[z] + layers[count - z] for z in range(1, half)}
    gaps = {z: layers[z] - layers[count - z] for z in range(1, half)}
    spectrum = []
    for k in range(count):
        near, far = (sums, gaps) if k % 2 == 0 else (gaps, sums)
        re = weighted(
            [(1.0, layers[0]), (cosine[half, k], layers[half])]
            + [(cosine[z, k], near[z]) for z in range(1, half)]
        )
        im = weighted(
            [(-sine[half, k], layers[half])] + [(-sine[z, k], far[z]) for z in range(1, half)]
        )
        spectrum.append((re, jnp.zeros_like(re) if im is None else im))
    return spectrum


def spectrum_to_layers(spectrum):
    count = len(spectrum)
    half = count // 2
    cosine, sine = half_table(count)
    layers = [None] * count
    evens, odds = range(2, count, 2), range(1, count, 2)
    layers[0] = weighted([(1.0, spectrum[0][0])] + [(2.0, spectrum[k][0]) for k in range(1, count)])
    layers[half] = weighted(
        [(1.0, spectrum[0][0])]
        + [(2.0 * cosine[half, k], spectrum[k][0]) for k in range(1, count)]
        + [(-2.0 * sine[half, k], spectrum[k][1]) for k in range(1, count)]
    )
    for z in range(1, half):
        even_re = weighted(
            [(1.0, spectrum[0][0])] + [(2.0 * cosine[z, k], spectrum[k][0]) for k in evens]
        )
        odd_re = weighted([(2.0 * cosine[z, k], spectrum[k][0]) for k in odds])
        even_im = weighted([(2.0 * sine[z, k], spectrum[k][1]) for k in evens])
        odd_im = weighted([(2.0 * sine[z, k], spectrum[k][1]) for k in odds])
        layers[z] = (even_re - odd_im) + (odd_re - even_im)
        layers[count - z] = (even_re - odd_im) - (odd_re - even_im)
    return layers


def dot32(left, right):
    return jnp.dot(left, right, preferred_element_type=jnp.float32)


def three_limbs(values, axis):
    upper, lower = split_limbs(values)
    return jnp.concatenate([upper, lower, upper], axis=axis)


def tensor_part(c, spec_ref, kernel_ref, out_ref):
    rows_full, columns_full = out_ref.shape[1] // 2, out_ref.shape[2] // 2
    lane = 128
    sub = 8
    row_pos = lax.broadcasted_iota(jnp.int32, (sub, lane), 0)
    lane_pos = lax.broadcasted_iota(jnp.int32, (sub, lane), 1)

    def step(i, carry):
        row_start = pl.multiple_of(i * sub, sub)
        top = (row_pos + row_start) == 0
        for start in range(0, columns_full, lane):

            def pick(component, odd_x, odd_y):
                def at(rows):
                    inner = kernel_ref[component, rows, start : start + lane]
                    if odd_y and start == 0:
                        edge = kernel_ref[component, rows, columns_full : columns_full + lane]
                        inner = jnp.where(lane_pos == 0, edge, inner)
                    return inner

                values = at(pl.ds(row_start, sub))
                if odd_x:
                    values = jnp.where(top, at(pl.ds(rows_full, sub)), values)
                return values

            def place(px, py):
                return (
                    pl.ds(row_start + px * rows_full, sub),
                    slice(py * columns_full + start, py * columns_full + start + lane),
                )

            def spec(px, py, f):
                rows, columns = place(px, py)
                return spec_ref[f, rows, columns]

            for px in range(2):
                for py in range(2):
                    sx = 1.0 if px else -1.0
                    sy = 1.0 if py else -1.0
                    own = pick(c, px, py)
                    if c < 2:
                        both = -(sx * sy) * pick(3, 0, 0)
                    if c != 1:
                        k_xz = sx * pick(4, 0, py)
                    if c != 0:
                        k_yz = sy * pick(5, px, 0)
                    for part in range(2):
                        turn = 1.0 if part else -1.0
                        other = 1 - part
                        total = own * spec(px, py, 2 * c + part)
                        if c == 0:
                            total = (
                                total
                                + both * spec(1 - px, 1 - py, 2 + part)
                                + turn * (k_xz * spec(1 - px, py, 4 + other))
                            )
                        elif c == 1:
                            total = (
                                both * spec(1 - px, 1 - py, part)
                                + total
                                + turn * (k_yz * spec(px, 1 - py, 4 + other))
                            )
                        else:
                            total = total + turn * (
                                k_xz * spec(1 - px, py, other) + k_yz * spec(px, 1 - py, 2 + other)
                            )
                        rows, columns = place(px, py)
                        out_ref[part, rows, columns] = total
        return carry

    lax.fori_loop(0, rows_full // sub, step, 0)


def demag_kernel(
    scale,
    magnet_ref,
    kernel_ref,
    fy_ref,
    fx_ref,
    gx_ref,
    gy_ref,
    out_ref,
    cells_ref,
    film_ref,
    stage_ref,
    pair_ref,
    extra_ref,
    send_ref,
    back_ref,
    held_ref,
    spec_ref,
    field_ref,
    tensor_ref,
    result_ref,
    own_sem,
    tensor_sem,
    film_send,
    film_recv,
    pair_send,
    pair_recv,
    plane_send,
    plane_recv,
    back_send,
    back_recv,
    extra_send,
    extra_recv,
    last_send,
    last_recv,
):
    groups, local_planes = held_ref.shape[1], held_ref.shape[2]
    slab, columns_full = held_ref.shape[4], held_ref.shape[5]
    layer_count = cells_ref.shape[2]
    rows_full = groups * slab
    parts = groups // 2
    me = lax.axis_index("space")
    half, seat = me // parts, lax.rem(me, parts)
    partner = lax.rem(me + parts, groups)
    flip = (1 - 2 * half).astype(jnp.float32)
    row_step = 8

    def remote(src, dst, send, recv, target):
        return pltpu.make_async_remote_copy(
            src_ref=src,
            dst_ref=dst,
            send_sem=send,
            recv_sem=recv,
            device_id={"space": target},
            device_id_type=pl.DeviceIdType.MESH,
        )

    def row_loop(step):
        def chunk(i, carry):
            step(pl.ds(pl.multiple_of(i * row_step, row_step), row_step))
            return carry

        lax.fori_loop(0, slab // row_step, chunk, 0)

    def own_copy(c):
        return pltpu.make_async_copy(magnet_ref.at[:, c], cells_ref.at[:, c], own_sem.at[c])

    def tensor_copy(q):
        return pltpu.make_async_copy(
            kernel_ref.at[:, q, pl.ds(0, rows_full + 8), pl.ds(0, columns_full + 128)],
            tensor_ref.at[q],
            tensor_sem.at[q],
        )

    def film_copy(c):
        return remote(
            magnet_ref.at[1 - half, c], film_ref.at[c], film_send.at[c], film_recv.at[c], partner
        )

    def pair_copy(side, source):
        return remote(
            stage_ref.at[side],
            pair_ref.at[source],
            pair_send.at[side],
            pair_recv.at[source],
            side * parts,
        )

    def place_of(seat_index, kind):
        return lax.rem((half + kind) * parts + seat_index, groups)

    def plane_copy(c, kind, slot):
        target = lax.rem(seat + 1 + slot, parts)
        return remote(
            send_ref.at[c, kind, slot],
            held_ref.at[c, place_of(seat, kind)],
            plane_send.at[c, kind, slot],
            plane_recv.at[c, kind, parts - 2 - slot],
            half * parts + target,
        )

    def plane_arrival(c, kind, slot):
        source = lax.rem(seat + 1 + slot, parts)
        return remote(
            send_ref.at[c, kind, slot],
            held_ref.at[c, place_of(source, kind)],
            plane_send.at[c, kind, slot],
            plane_recv.at[c, kind, slot],
            half * parts + source,
        )

    def back_copy(c, kind, slot):
        target = lax.rem(seat + 1 + slot, parts)
        return remote(
            held_ref.at[c, place_of(target, kind)],
            back_ref.at[c, kind, parts - 2 - slot],
            back_send.at[c, kind, slot],
            back_recv.at[c, kind, parts - 2 - slot],
            half * parts + target,
        )

    def back_arrival(c, kind, slot):
        source = lax.rem(seat + 1 + slot, parts)
        return remote(
            held_ref.at[c, place_of(source, kind)],
            back_ref.at[c, kind, slot],
            back_send.at[c, kind, slot],
            back_recv.at[c, kind, slot],
            half * parts + source,
        )

    def extra_copy(c, step):
        target = lax.rem(me + step, groups)
        return remote(
            held_ref.at[c, target, 0, 1],
            extra_ref.at[half, c],
            extra_send.at[c, step],
            extra_recv.at[half, c],
            target,
        )

    def extra_arrival(side, c):
        return remote(
            held_ref.at[c, 0, 0, 1],
            extra_ref.at[side, c],
            extra_send.at[c, 0],
            extra_recv.at[side, c],
            side * parts,
        )

    def last_copy(c):
        return remote(
            film_ref.at[c], field_ref.at[half, c], last_send.at[c], last_recv.at[c], partner
        )

    def last_arrival(c):
        return remote(
            film_ref.at[c], field_ref.at[1 - half, c], last_send.at[c], last_recv.at[c], partner
        )

    def transform_layers(c, kind):
        place = place_of(seat, kind)

        def variant(here):
            def step(rows):
                if kind == 0:
                    layers = [cells_ref[half, c, z, rows, :] for z in range(layer_count)]
                else:
                    layers = [film_ref[c, z, rows, :] for z in range(layer_count)]
                layers = [v * flip if z % 2 else v for z, v in enumerate(layers)]
                spectrum = layers_to_spectrum(layers)
                for k in range(layer_count):
                    target, q = k // local_planes, k % local_planes
                    slot = (target - here) % parts - 1
                    for part in range(2):
                        if target == here:
                            held_ref[c, place, q, part, rows, :] = spectrum[k][part]
                        else:
                            send_ref[c, kind, slot, q, part, rows, :] = spectrum[k][part]

            row_loop(step)

        for here in range(parts):
            pl.when(seat == here)(functools.partial(variant, here))
        for slot in range(parts - 1):
            plane_copy(c, kind, slot).start()

    def transform_planes(c, kind):
        place = place_of(seat, kind)

        def variant(here):
            def step(rows):
                spectrum = []
                for k in range(layer_count):
                    source, q = k // local_planes, k % local_planes
                    slot = (source - here) % parts - 1
                    if source == here:
                        spectrum.append(
                            [held_ref[c, place, q, part, rows, :] for part in range(2)]
                        )
                    else:
                        spectrum.append(
                            [back_ref[c, kind, slot, q, part, rows, :] for part in range(2)]
                        )
                for z, value in enumerate(spectrum_to_layers(spectrum)):
                    value = value * (scale * flip if z % 2 else scale)
                    if kind == 0:
                        field_ref[half, c, z, rows, :] = value
                    else:
                        film_ref[c, z, rows, :] = value

            row_loop(step)

        for here in range(parts):
            pl.when(seat == here)(functools.partial(variant, here))

    barrier = pltpu.get_barrier_semaphore()
    for d in range(1, groups):
        pl.semaphore_signal(
            barrier,
            inc=1,
            device_id={"space": lax.rem(me + d, groups)},
            device_id_type=pl.DeviceIdType.MESH,
        )
    for c in range(3):
        own_copy(c).start()
    pl.semaphore_wait(barrier, groups - 1)
    film_copy(0).start()
    for c in range(3):
        own_copy(c).wait()
    for side in range(2):

        def sum_layers(rows):
            for c in range(3):
                layers = [cells_ref[1 - side, c, z, rows, :] for z in range(layer_count)]
                stage_ref[side, c, rows, :] = weighted(
                    [((-1.0) ** (z * side), layers[z]) for z in range(layer_count)]
                )

        row_loop(sum_layers)

        @pl.when(me == side * parts)
        def _():
            pair_ref[me] = stage_ref[side]

        @pl.when(me != side * parts)
        def _():
            pair_copy(side, me).start()

    for c in range(1, 3):
        film_copy(c).start()
    for q in range(local_planes):
        tensor_copy(q).start()

    for c in range(3):
        transform_layers(c, 0)

    for c in range(3):
        film_copy(c).wait_recv()
        transform_layers(c, 1)
        for kind in range(2):
            for slot in range(parts - 1):
                plane_arrival(c, kind, slot).wait_recv()

        def forward(i, carry):
            q = local_planes - 1 - i

            @pl.when((seat == 0) & (q == 0))
            def _():
                if c == 0:
                    for d in range(1, groups):
                        pair_copy(0, lax.rem(me + d, groups)).wait_recv()
                for g in range(groups):
                    held_ref[c, g, 0, 1] = pair_ref[g, c]

            fy = jnp.concatenate([fy_ref[0], fy_ref[0], fy_ref[1]], axis=0)
            fx = jnp.concatenate([fx_ref[0], fx_ref[0], fx_ref[1]], axis=1)
            cells = jnp.concatenate(
                [held_ref[c, g, q, part] for part in range(2) for g in range(groups)], axis=0
            )
            lines = dot32(three_limbs(cells, 1), fy)
            for part in range(2):
                spec_ref[q, 2 * c + part] = dot32(
                    fx, three_limbs(lines[part * rows_full : (part + 1) * rows_full], 0)
                )
            return carry

        lax.fori_loop(0, local_planes, forward, 0)

    for q in range(local_planes):
        tensor_copy(q).wait()

    for c in range(3):

        def backward(q, carry):
            tensor_part(c, spec_ref.at[q], tensor_ref.at[q], result_ref)
            gx = jnp.concatenate([gx_ref[0], gx_ref[0], gx_ref[1]], axis=1)
            gy = jnp.concatenate([gy_ref[0], gy_ref[0], gy_ref[1]], axis=0)
            for part in range(2):
                lines = dot32(gx, three_limbs(result_ref[part], 0))
                cells = dot32(three_limbs(lines, 1), gy)
                for g in range(groups):
                    held_ref[c, g, q, part] = cells[g * slab : (g + 1) * slab]
            return carry

        lax.fori_loop(0, local_planes, backward, 0)
        for kind in (1, 0):
            for slot in range(parts - 1):
                back_copy(c, kind, slot).start()

        @pl.when(seat == 0)
        def _():
            extra_ref[half, c] = held_ref[c, me, 0, 1]
            for step in range(1, groups):
                extra_copy(c, step).start()

        for slot in range(parts - 1):
            back_arrival(c, 1, slot).wait_recv()
        transform_planes(c, 1)
        last_copy(c).start()
        for slot in range(parts - 1):
            back_arrival(c, 0, slot).wait_recv()
        transform_planes(c, 0)

    for c in range(3):
        last_arrival(c).wait_recv()
        for side in range(2):

            @pl.when(me != side * parts)
            def _():
                extra_arrival(side, c).wait_recv()

        for image in range(2):

            def add_extra(rows):
                extra = scale * extra_ref[1 - image, c, rows, :]
                for z in range(layer_count):
                    sign = (-1.0) ** (z * (1 - image))
                    value = field_ref[image, c, z, rows, :]
                    field_ref[image, c, z, rows, :] = value + extra if sign > 0 else value - extra

            row_loop(add_extra)
        pltpu.make_async_copy(field_ref.at[:, c], out_ref.at[:, c], own_sem.at[c]).start()

    for c in range(3):
        pltpu.make_async_copy(field_ref.at[:, c], out_ref.at[:, c], own_sem.at[c]).wait()
        film_copy(c).wait_send()
        last_copy(c).wait_send()
        for kind in range(2):
            for slot in range(parts - 1):
                plane_copy(c, kind, slot).wait_send()
                back_copy(c, kind, slot).wait_send()

    @pl.when(seat == 0)
    def _():
        for c in range(3):
            for step in range(1, groups):
                extra_copy(c, step).wait_send()

    for side in range(2):

        @pl.when(me != side * parts)
        def _():
            pair_copy(side, me).wait_send()


def demag_field(magnet, kernel):
    layer_count, row_count, column_count = magnet.shape[2:]
    groups = lax.axis_size("space")
    local_planes = 2 * layer_count // groups
    full_rows = row_count * groups
    slots = groups // 2 - 1
    table_y = parity_table(column_count)
    table_x = parity_table(full_rows)
    tables = [
        table_limbs(table_y),
        table_limbs(table_x.T),
        table_limbs(table_x * parity_weights(full_rows)[None, :]),
        table_limbs((table_y * parity_weights(column_count)[None, :]).T),
    ]
    slab = (row_count, column_count)
    film = (layer_count,) + slab
    block = (local_planes, 2) + slab
    anywhere = pl.BlockSpec(memory_space=pl.ANY)
    inside = pl.BlockSpec(memory_space=pltpu.VMEM)
    dots = 6 * local_planes * 4 * full_rows * column_count * 3 * (full_rows + column_count // 2)
    padded_cells = 8 * layer_count * full_rows * column_count
    signals = pltpu.SemaphoreType.DMA
    return pl.pallas_call(
        functools.partial(demag_kernel, -1.0 / padded_cells),
        in_specs=[anywhere, anywhere] + [inside] * len(tables),
        out_specs=anywhere,
        out_shape=jax.ShapeDtypeStruct(magnet.shape, jnp.float32),
        scratch_shapes=[
            pltpu.VMEM((2, 3) + film, jnp.float32),
            pltpu.VMEM((3,) + film, jnp.float32),
            pltpu.VMEM((2, 3) + slab, jnp.float32),
            pltpu.VMEM((groups, 3) + slab, jnp.float32),
            pltpu.VMEM((2, 3) + slab, jnp.float32),
            pltpu.VMEM((3, 2, slots) + block, jnp.float32),
            pltpu.VMEM((3, 2, slots) + block, jnp.float32),
            pltpu.VMEM((3, groups) + block, jnp.float32),
            pltpu.VMEM((local_planes, 6, 2 * full_rows, 2 * column_count), jnp.float32),
            pltpu.VMEM((2, 3) + film, jnp.float32),
            pltpu.VMEM((local_planes, 6, full_rows + 8, column_count + 128), jnp.float32),
            pltpu.VMEM((2, 2 * full_rows, 2 * column_count), jnp.float32),
            signals((3,)),
            signals((local_planes,)),
            signals((3,)),
            signals((3,)),
            signals((2,)),
            signals((groups,)),
            signals((3, 2, slots)),
            signals((3, 2, slots)),
            signals((3, 2, slots)),
            signals((3, 2, slots)),
            signals((3, groups)),
            signals((2, 3)),
            signals((3,)),
            signals((3,)),
        ],
        compiler_params=pltpu.CompilerParams(
            vmem_limit_bytes=67043328, collective_id=0, has_side_effects=True
        ),
        cost_estimate=pl.CostEstimate(
            flops=4 * dots, bytes_accessed=4 * magnet.size * 4, transcendentals=0
        ),
        name="demag_kernel",
    )(magnet, kernel, *[jnp.asarray(t) for t in tables])


def swap_kernel(shifts, combine, tile_ref, out_ref, held_ref, send_sem, recv_sem):
    groups, images = lax.axis_size("space"), lax.axis_size("image")
    me, image = lax.axis_index("space"), lax.axis_index("image")
    routes = [
        (n, shift, d)
        for n, shift in enumerate(shifts)
        for d in range(groups)
        if shift != 0 or d != 0
    ]

    def target(shift, d):
        return {"image": lax.rem(image - shift + images, images), "space": lax.rem(me + d, groups)}

    barrier = pltpu.get_barrier_semaphore()
    for n, shift, d in routes:
        pl.semaphore_signal(
            barrier, inc=1, device_id=target(shift, d), device_id_type=pl.DeviceIdType.MESH
        )
    pl.semaphore_wait(barrier, len(routes))

    def copy_of(n, shift, d, slot):
        return pltpu.make_async_remote_copy(
            src_ref=tile_ref,
            dst_ref=held_ref.at[n, slot],
            send_sem=send_sem.at[n, d],
            recv_sem=recv_sem.at[n, d],
            device_id=target(shift, d),
            device_id_type=pl.DeviceIdType.MESH,
        )

    for n, shift, d in routes:
        copy_of(n, shift, d, me).start()
    held_ref[shifts.index(0), me] = tile_ref[...]
    for n, shift, d in routes:
        copy_of(n, shift, d, lax.rem(me + groups - d, groups)).wait_recv()
    for n in range(len(shifts)):
        total = held_ref[n, 0]
        for g in range(1, groups):
            total = combine(total, held_ref[n, g])
        out_ref[n] = total
    for n, shift, d in routes:
        copy_of(n, shift, d, me).wait_send()


def swapped(values, shifts, combine, collective_id):
    rows, columns = values.shape
    tile = jnp.pad(values, ((0, -rows % 8), (0, -columns % 128)))
    groups = lax.axis_size("space")
    inside = pl.BlockSpec(memory_space=pltpu.VMEM)
    result = pl.pallas_call(
        functools.partial(swap_kernel, shifts, combine),
        in_specs=[inside],
        out_specs=inside,
        out_shape=jax.ShapeDtypeStruct((len(shifts),) + tile.shape, jnp.float32),
        scratch_shapes=[
            pltpu.VMEM((len(shifts), groups) + tile.shape, jnp.float32),
            pltpu.SemaphoreType.DMA((len(shifts), groups)),
            pltpu.SemaphoreType.DMA((len(shifts), groups)),
        ],
        compiler_params=pltpu.CompilerParams(
            collective_id=collective_id, has_side_effects=True
        ),
        name="swap_kernel",
    )(tile)
    return result[:, :rows, :columns]


def local_fields(magnet, anisotropy, rimmed):
    layer_count = magnet.shape[2]
    row_count = magnet.shape[3]
    column_count = magnet.shape[4]
    x_plus = rimmed[:, :, :, 2:]
    x_minus = rimmed[:, :, :, :-2]
    padded = jnp.pad(magnet, ((0, 0), (0, 0), (1, 1), (0, 0), (1, 1)))
    z_plus = padded[:, :, 2:, :, 1:-1]
    z_minus = padded[:, :, :-2, :, 1:-1]
    y_plus = padded[:, :, 1:-1, :, 2:]
    y_minus = padded[:, :, 1:-1, :, :-2]
    first_row = lax.axis_index("space") * row_count
    full_rows = row_count * lax.axis_size("space")
    layer_pos = lax.broadcasted_iota(jnp.int32, (layer_count, row_count, column_count), 0)
    row_pos = lax.broadcasted_iota(jnp.int32, (layer_count, row_count, column_count), 1) + first_row
    column_pos = lax.broadcasted_iota(jnp.int32, (layer_count, row_count, column_count), 2)
    boundary = (layer_pos == 0).astype(jnp.float32) + (layer_pos == layer_count - 1).astype(
        jnp.float32
    )
    boundary = (
        boundary
        + (row_pos == 0).astype(jnp.float32)
        + (row_pos == full_rows - 1).astype(jnp.float32)
    )
    boundary = (
        boundary
        + (column_pos == 0).astype(jnp.float32)
        + (column_pos == column_count - 1).astype(jnp.float32)
    )
    present = 6.0 - boundary
    neighbours = x_plus + x_minus + y_plus + y_minus + z_plus + z_minus
    exchange_part = exchange_strength * (neighbours - present * magnet)
    chiral_x = chiral_strength * (x_plus[:, 2] - x_minus[:, 2])
    chiral_y = chiral_strength * (y_plus[:, 2] - y_minus[:, 2])
    chiral_z = -chiral_strength * (x_plus[:, 0] - x_minus[:, 0] + (y_plus[:, 1] - y_minus[:, 1]))
    easy_axis = 2.0 * anisotropy[:, None] * magnet[:, 2]
    local_part = exchange_part + jnp.stack([chiral_x, chiral_y, chiral_z + easy_axis], axis=1)
    return local_part


def body(magnet, anisotropy, kernel):
    image_count = magnet.shape[0]
    cell_count = magnet.shape[2] * magnet.shape[3] * lax.axis_size("space") * magnet.shape[4]
    framed = extended(magnet, (("image", 0),), 1)
    rimmed = extended(magnet, (("space", 3),), 1)

    prior_image = framed[:-2]
    next_image = framed[2:]
    demag = demag_field(magnet, kernel)
    ahead = project(next_image - magnet, magnet)
    behind = project(magnet - prior_image, magnet)
    early = (
        local_fields(magnet, anisotropy, rimmed),
        total_cells(angle_squared(magnet, next_image)),
        total_cells(ahead * ahead),
        total_cells(ahead * behind),
        total_cells(behind * behind),
    )
    fields = early[0] + demag
    true_force = project(fields, magnet)
    tangent_next = project(next_image - magnet, magnet)
    tangent_prior = project(magnet - prior_image, magnet)
    sums = jnp.stack(
        [
            -0.5 * total_cells(magnet * fields),
            *early[1:],
            total_cells(true_force * tangent_next),
            total_cells(true_force * tangent_prior),
        ],
        axis=1,
    )
    band_size = image_count * lax.axis_size("image")
    swaps = swapped(sums, (-1, 0, 1), jnp.add, 64)
    band = jnp.concatenate([swaps[0, -1:], swaps[1], swaps[2, :1]], axis=0)
    energy_band, distance_band = band[:, 0], jnp.sqrt(band[:, 1] / cell_count)
    weight_next, weight_prior = tangent_weights(
        energy_band, jnp.roll(energy_band, -1), jnp.roll(energy_band, 1)
    )
    length_squares = (
        weight_next * weight_next * band[:, 2]
        + 2.0 * weight_next * weight_prior * band[:, 3]
        + weight_prior * weight_prior * band[:, 4]
    )
    drive_total = weight_next * band[:, 5] + weight_prior * band[:, 6]
    tangent_scale = jnp.sqrt(jnp.maximum(length_squares, 0.0) / cell_count + epsilon)
    parallel = drive_total / (cell_count * tangent_scale)
    spring = spring_strength * (distance_band - jnp.roll(distance_band, 1))
    first_image = lax.axis_index("image") * image_count
    image_index = first_image - 1 + jnp.arange(image_count + 2)
    interior = ((image_index > 0) & (image_index < band_size - 1)).astype(jnp.float32)
    pull = (spring - parallel) / tangent_scale
    mine = jnp.stack([energy_band, pull * weight_next, pull * weight_prior, interior], axis=1)[1:-1]
    energy_total = mine[:, 0]
    band_force = jnp.where(
        lift_axes(mine[:, 3]) > 0.0,
        true_force + lift_axes(mine[:, 1]) * tangent_next + lift_axes(mine[:, 2]) * tangent_prior,
        0.0,
    )
    local_largest = jnp.max(jnp.sqrt(jnp.sum(band_force * band_force, axis=1)), axis=(1, 2, 3))
    largest = swapped(local_largest[None, :], (0,), jnp.maximum, 65)[0, 0]
    move_scale = jnp.minimum(step_limit, rotation_limit / (largest + epsilon))
    stepped = magnet + lift_axes(move_scale) * band_force
    updated = stepped / jnp.sqrt(jnp.sum(stepped * stepped, axis=1, keepdims=True))
    return (updated, band_force, energy_total / cell_count)


def solution(mesh):
    in_specs = (P("image", None, None, "space", None), P("space"), P(None, "space", None, None))
    out_specs = (
        P("image", None, None, "space", None),
        P("image", None, None, "space", None),
        P("image"),
    )
    return jax.shard_map(body, mesh=mesh, in_specs=in_specs, out_specs=out_specs, check_vma=False)
```

```python
import functools
import math

import jax
import jax.numpy as jnp
import numpy as np
from jax import lax
from jax.experimental import pallas as pl
from jax.experimental.pallas import tpu as pltpu
from jax.sharding import PartitionSpec as P

exchange_strength = 0.25
chiral_strength = 0.3
spring_strength = 10.0
step_limit = 1.0
rotation_limit = 0.5
epsilon = 1e-06


def lift_axes(values):
    return values[:, None, None, None, None]


def tangent_weights(energy_total, energy_next, energy_prior):
    rise_next = energy_next - energy_total
    rise_prior = energy_total - energy_prior
    upward = (rise_next > 0) & (rise_prior > 0)
    downward = (rise_next < 0) & (rise_prior < 0)
    larger = jnp.maximum(jnp.abs(rise_next), jnp.abs(rise_prior))
    smaller = jnp.minimum(jnp.abs(rise_next), jnp.abs(rise_prior))
    toward_next = energy_next > energy_prior
    weight_next = jnp.where(
        upward, 1.0, jnp.where(downward, 0.0, jnp.where(toward_next, larger, smaller))
    )
    weight_prior = jnp.where(
        upward, 0.0, jnp.where(downward, 1.0, jnp.where(toward_next, smaller, larger))
    )
    return (weight_next, weight_prior)


def split_limbs(values):
    upper = values.astype(jnp.bfloat16)
    return upper, (values - upper.astype(jnp.float32)).astype(jnp.bfloat16)


def table_limbs(table):
    upper = table.astype(np.float32).astype(jnp.bfloat16)
    lower = (table - upper.astype(np.float64)).astype(np.float32).astype(jnp.bfloat16)
    return np.stack([upper, lower])


def parity_table(count):
    position = np.arange(count)[:, None]
    slot = np.arange(count)[None, :]
    turn = np.pi / count
    even_part = np.cos(turn * (position * slot % (2 * count)))
    odd_part = np.sin(turn * (position * slot % (2 * count)))
    odd_part[:, 0] = np.cos(turn * (position[:, 0] * count % (2 * count)))
    return np.concatenate([even_part, odd_part], axis=1)


def half_table(count):
    place = np.arange(count)
    angle = np.pi * (place[:, None] * place[None, :] % (2 * count)) / count
    cosine, sine = np.cos(angle), np.sin(angle)
    cosine[np.abs(cosine) < 1e-12] = 0.0
    sine[np.abs(sine) < 1e-12] = 0.0
    return cosine, sine


def weighted(terms):
    total = None
    for weight, value in terms:
        weight = float(weight)
        if weight == 0.0:
            continue
        if total is None:
            total = value if weight == 1.0 else -value if weight == -1.0 else weight * value
        elif weight == 1.0:
            total = total + value
        elif weight == -1.0:
            total = total - value
        else:
            total = total + weight * value
    return total


def layers_to_spectrum(layers):
    count = len(layers)
    half = count // 2
    cosine, sine = half_table(count)
    sums = {z: layers[z] + layers[count - z] for z in range(1, half)}
    gaps = {z: layers[z] - layers[count - z] for z in range(1, half)}
    spectrum = []
    for k in range(count):
        near, far = (sums, gaps) if k % 2 == 0 else (gaps, sums)
        re = weighted(
            [(1.0, layers[0]), (cosine[half, k], layers[half])]
            + [(cosine[z, k], near[z]) for z in range(1, half)]
        )
        im = weighted(
            [(-sine[half, k], layers[half])] + [(-sine[z, k], far[z]) for z in range(1, half)]
        )
        spectrum.append((re, jnp.zeros_like(re) if im is None else im))
    return spectrum


def spectrum_to_layers(spectrum):
    count = len(spectrum)
    half = count // 2
    cosine, sine = half_table(count)
    layers = [None] * count
    evens, odds = range(2, count, 2), range(1, count, 2)
    layers[0] = weighted([(1.0, spectrum[0][0])] + [(2.0, spectrum[k][0]) for k in range(1, count)])
    layers[half] = weighted(
        [(1.0, spectrum[0][0])]
        + [(2.0 * cosine[half, k], spectrum[k][0]) for k in range(1, count)]
        + [(-2.0 * sine[half, k], spectrum[k][1]) for k in range(1, count)]
    )
    for z in range(1, half):
        even_re = weighted(
            [(1.0, spectrum[0][0])] + [(2.0 * cosine[z, k], spectrum[k][0]) for k in evens]
        )
        odd_re = weighted([(2.0 * cosine[z, k], spectrum[k][0]) for k in odds])
        even_im = weighted([(2.0 * sine[z, k], spectrum[k][1]) for k in evens])
        odd_im = weighted([(2.0 * sine[z, k], spectrum[k][1]) for k in odds])
        layers[z] = (even_re - odd_im) + (odd_re - even_im)
        layers[count - z] = (even_re - odd_im) - (odd_re - even_im)
    return layers


def dot32(left, right):
    return jnp.dot(left, right, preferred_element_type=jnp.float32)


def three_limbs(values, axis):
    upper, lower = split_limbs(values)
    return jnp.concatenate([upper, lower, upper], axis=axis)


def tensor_part(c, spec_ref, kernel_ref, out_ref):
    rows_full, columns_full = out_ref.shape[1] // 2, out_ref.shape[2] // 2
    lane = 128
    sub = 8
    row_pos = lax.broadcasted_iota(jnp.int32, (sub, lane), 0)
    lane_pos = lax.broadcasted_iota(jnp.int32, (sub, lane), 1)

    def step(i, carry):
        row_start = pl.multiple_of(i * sub, sub)
        top = (row_pos + row_start) == 0
        for start in range(0, columns_full, lane):

            def pick(component, odd_x, odd_y):
                def at(rows):
                    inner = kernel_ref[component, rows, start : start + lane]
                    if odd_y and start == 0:
                        edge = kernel_ref[component, rows, columns_full : columns_full + lane]
                        inner = jnp.where(lane_pos == 0, edge, inner)
                    return inner

                values = at(pl.ds(row_start, sub))
                if odd_x:
                    values = jnp.where(top, at(pl.ds(rows_full, sub)), values)
                return values

            def place(px, py):
                return (
                    pl.ds(row_start + px * rows_full, sub),
                    slice(py * columns_full + start, py * columns_full + start + lane),
                )

            def spec(px, py, f):
                rows, columns = place(px, py)
                return spec_ref[f, rows, columns]

            for px in range(2):
                for py in range(2):
                    sx = 1.0 if px else -1.0
                    sy = 1.0 if py else -1.0
                    own = pick(c, px, py)
                    if c < 2:
                        both = -(sx * sy) * pick(3, 0, 0)
                    if c != 1:
                        k_xz = sx * pick(4, 0, py)
                    if c != 0:
                        k_yz = sy * pick(5, px, 0)
                    for part in range(2):
                        turn = 1.0 if part else -1.0
                        other = 1 - part
                        total = own * spec(px, py, 2 * c + part)
                        if c == 0:
                            total = (
                                total
                                + both * spec(1 - px, 1 - py, 2 + part)
                                + turn * (k_xz * spec(1 - px, py, 4 + other))
                            )
                        elif c == 1:
                            total = (
                                both * spec(1 - px, 1 - py, part)
                                + total
                                + turn * (k_yz * spec(px, 1 - py, 4 + other))
                            )
                        else:
                            total = total + turn * (
                                k_xz * spec(1 - px, py, other) + k_yz * spec(px, 1 - py, 2 + other)
                            )
                        total = jnp.where(top, 0.5 * total, total)
                        if start == 0:
                            total = jnp.where(lane_pos == 0, 0.5 * total, total)
                        rows, columns = place(px, py)
                        out_ref[part, rows, columns] = total
        return carry

    lax.fori_loop(0, rows_full // sub, step, 0)


def arc_angle(sine, cosine):
    size = jnp.abs(cosine)
    low, high = jnp.minimum(sine, size), jnp.maximum(sine, size)
    ratio = low / jnp.maximum(high, 1e-37)
    wide = ratio > 0.41421356
    ratio = jnp.where(wide, (ratio - 1.0) / (ratio + 1.0), ratio)
    square = ratio * ratio
    series = ((8.05374449538e-2 * square - 1.38776856032e-1) * square + 1.99777106478e-1) * square
    angle = (series - 3.33329491539e-1) * square * ratio + ratio
    angle = jnp.where(wide, angle + 0.25 * math.pi, angle)
    angle = jnp.where(sine > size, 0.5 * math.pi - angle, angle)
    return jnp.where(cosine < 0.0, math.pi - angle, angle)


def dot3(first, second):
    return first[0] * second[0] + first[1] * second[1] + first[2] * second[2]


def band_kernel(
    scale,
    magnet_ref,
    kernel_ref,
    ease_ref,
    fy_ref,
    fx_ref,
    gx_ref,
    gy_ref,
    force_ref,
    small_ref,
    cells_ref,
    film_ref,
    stage_ref,
    pair_ref,
    extra_ref,
    send_ref,
    back_ref,
    held_ref,
    spec_ref,
    field_ref,
    arrive_ref,
    next_ref,
    prior_ref,
    rim_out_ref,
    rim_ref,
    present_ref,
    sums_ref,
    tile_ref,
    swap_ref,
    peak_ref,
    tensor_ref,
    result_ref,
    own_sem,
    tensor_sem,
    film_send,
    film_recv,
    pair_send,
    pair_recv,
    plane_send,
    plane_recv,
    back_send,
    back_recv,
    extra_send,
    extra_recv,
    last_send,
    last_recv,
    image_send,
    image_recv,
    rim_send,
    rim_recv,
    swap_send,
    swap_recv,
    peak_send,
    peak_recv,
    force_sem,
):
    groups, local_planes = held_ref.shape[1], held_ref.shape[2]
    slab, columns_full = held_ref.shape[4], held_ref.shape[5]
    layer_count = cells_ref.shape[2]
    rows_full = groups * slab
    parts = groups // 2
    me = lax.axis_index("space")
    half, seat = me // parts, lax.rem(me, parts)
    partner = lax.rem(me + parts, groups)
    flip = (1 - 2 * half).astype(jnp.float32)
    row_step = 8
    images, image = lax.axis_size("image"), lax.axis_index("image")
    first, last = image == 0, image == images - 1
    shifts = (-1, 0, 1)
    routes = [
        (n, shift, d)
        for n, shift in enumerate(shifts)
        for d in range(groups)
        if shift != 0 or d != 0
    ]

    def target_of(shift, d):
        return {"image": lax.rem(image - shift + images, images), "space": lax.rem(me + d, groups)}

    def remote(src, dst, send, recv, target):
        return pltpu.make_async_remote_copy(
            src_ref=src,
            dst_ref=dst,
            send_sem=send,
            recv_sem=recv,
            device_id=target if isinstance(target, dict) else {"space": target},
            device_id_type=pl.DeviceIdType.MESH,
        )

    def row_loop(step):
        def chunk(i, carry):
            step(pl.ds(pl.multiple_of(i * row_step, row_step), row_step))
            return carry

        lax.fori_loop(0, slab // row_step, chunk, 0)

    def own_copy(c):
        return pltpu.make_async_copy(magnet_ref.at[:, c], cells_ref.at[:, c], own_sem.at[c])

    def tensor_copy(q):
        return pltpu.make_async_copy(
            kernel_ref.at[:, q, pl.ds(0, rows_full + 8), pl.ds(0, columns_full + 128)],
            tensor_ref.at[q],
            tensor_sem.at[q],
        )

    def film_copy(c):
        return remote(
            magnet_ref.at[1 - half, c], film_ref.at[c], film_send.at[c], film_recv.at[c], partner
        )

    def pair_copy(side, source):
        return remote(
            stage_ref.at[side],
            pair_ref.at[source],
            pair_send.at[side],
            pair_recv.at[source],
            side * parts,
        )

    def place_of(seat_index, kind):
        return lax.rem((half + kind) * parts + seat_index, groups)

    def plane_copy(c, kind, slot):
        target = lax.rem(seat + 1 + slot, parts)
        return remote(
            send_ref.at[c, kind, slot],
            held_ref.at[c, place_of(seat, kind)],
            plane_send.at[c, kind, slot],
            plane_recv.at[c, kind, parts - 2 - slot],
            half * parts + target,
        )

    def plane_arrival(c, kind, slot):
        source = lax.rem(seat + 1 + slot, parts)
        return remote(
            send_ref.at[c, kind, slot],
            held_ref.at[c, place_of(source, kind)],
            plane_send.at[c, kind, slot],
            plane_recv.at[c, kind, slot],
            half * parts + source,
        )

    def back_copy(c, kind, slot):
        target = lax.rem(seat + 1 + slot, parts)
        return remote(
            held_ref.at[c, place_of(target, kind)],
            back_ref.at[c, kind, parts - 2 - slot],
            back_send.at[c, kind, slot],
            back_recv.at[c, kind, parts - 2 - slot],
            half * parts + target,
        )

    def back_arrival(c, kind, slot):
        source = lax.rem(seat + 1 + slot, parts)
        return remote(
            held_ref.at[c, place_of(source, kind)],
            back_ref.at[c, kind, slot],
            back_send.at[c, kind, slot],
            back_recv.at[c, kind, slot],
            half * parts + source,
        )

    def extra_copy(c, step):
        target = lax.rem(me + step, groups)
        return remote(
            held_ref.at[c, target, 0, 1],
            extra_ref.at[half, c],
            extra_send.at[c, step],
            extra_recv.at[half, c],
            target,
        )

    def extra_arrival(side, c):
        return remote(
            held_ref.at[c, 0, 0, 1],
            extra_ref.at[side, c],
            extra_send.at[c, 0],
            extra_recv.at[side, c],
            side * parts,
        )

    def last_copy(c):
        return remote(
            film_ref.at[c], arrive_ref.at[c], last_send.at[c], last_recv.at[c], partner
        )

    def ahead_copy():
        return remote(
            magnet_ref.at[1],
            prior_ref,
            image_send.at[0],
            image_recv.at[0],
            {"image": lax.rem(image + 1, images)},
        )

    def behind_copy():
        return remote(
            magnet_ref.at[0],
            next_ref,
            image_send.at[1],
            image_recv.at[1],
            {"image": lax.rem(image + images - 1, images)},
        )

    def rim_copy(side):
        return remote(
            rim_out_ref.at[side],
            rim_ref.at[side],
            rim_send.at[side],
            rim_recv.at[side],
            lax.rem(me + (1 if side == 0 else groups - 1), groups),
        )

    def swap_copy(n, shift, d, slot):
        return remote(
            tile_ref, swap_ref.at[n, slot], swap_send.at[n, d], swap_recv.at[n, d], target_of(shift, d)
        )

    def peak_copy(d, slot):
        return remote(
            tile_ref.at[pl.ds(0, 8)],
            peak_ref.at[slot],
            peak_send.at[d],
            peak_recv.at[d],
            lax.rem(me + d, groups),
        )

    def force_copy(i):
        return pltpu.make_async_copy(field_ref.at[i], force_ref.at[i], force_sem.at[i])

    def transform_layers(c, kind):
        place = place_of(seat, kind)

        def variant(here):
            def step(rows):
                if kind == 0:
                    layers = [cells_ref[half, c, z, rows, :] for z in range(layer_count)]
                else:
                    layers = [film_ref[c, z, rows, :] for z in range(layer_count)]
                layers = [v * flip if z % 2 else v for z, v in enumerate(layers)]
                spectrum = layers_to_spectrum(layers)
                for k in range(layer_count):
                    target, q = k // local_planes, k % local_planes
                    slot = (target - here) % parts - 1
                    for part in range(2):
                        if target == here:
                            held_ref[c, place, q, part, rows, :] = spectrum[k][part]
                        else:
                            send_ref[c, kind, slot, q, part, rows, :] = spectrum[k][part]

            row_loop(step)

        for here in range(parts):
            pl.when(seat == here)(functools.partial(variant, here))
        for slot in range(parts - 1):
            plane_copy(c, kind, slot).start()

    def transform_planes(c, kind):
        place = place_of(seat, kind)

        def variant(here):
            def step(rows):
                spectrum = []
                for k in range(layer_count):
                    source, q = k // local_planes, k % local_planes
                    slot = (source - here) % parts - 1
                    if source == here:
                        spectrum.append(
                            [held_ref[c, place, q, part, rows, :] for part in range(2)]
                        )
                    else:
                        spectrum.append(
                            [back_ref[c, kind, slot, q, part, rows, :] for part in range(2)]
                        )
                for z, value in enumerate(spectrum_to_layers(spectrum)):
                    value = value * (scale * flip if z % 2 else scale)
                    if kind == 0:
                        field_ref[half, c, z, rows, :] = field_ref[half, c, z, rows, :] + value
                    else:
                        film_ref[c, z, rows, :] = value

            row_loop(step)

        for here in range(parts):
            pl.when(seat == here)(functools.partial(variant, here))

    def fill_rims():
        def step(f, carry):
            i, c = f // 3, lax.rem(f, 3)
            for side in range(2):
                row = slab - 1 if side == 0 else 0
                rim_out_ref[side, i, c] = jnp.concatenate(
                    [cells_ref[i, c, z, row : row + 1, :] for z in range(layer_count)], axis=0
                )
            return carry

        lax.fori_loop(0, 6, step, 0)
        row_pos = lax.broadcasted_iota(jnp.int32, (slab, columns_full), 0) + me * slab
        column_pos = lax.broadcasted_iota(jnp.int32, (slab, columns_full), 1)
        faces = [row_pos == 0, row_pos == rows_full - 1]
        faces += [column_pos == 0, column_pos == columns_full - 1]
        present_ref[...] = 6.0 - sum(jnp.where(face, 1.0, 0.0) for face in faces)
        for side in range(2):
            open_side = me != groups - 1 if side == 0 else me != 0

            @pl.when(open_side)
            def _():
                rim_copy(side).start()

            no_source = me == 0 if side == 0 else me == groups - 1

            @pl.when(no_source)
            def _():
                rim_ref[side] = jnp.zeros(rim_ref.shape[1:], jnp.float32)

    def local_fields():
        for side in range(2):
            has_source = me != 0 if side == 0 else me != groups - 1

            @pl.when(has_source)
            def _():
                rim_copy(side).wait_recv()

        row_pos = lax.broadcasted_iota(jnp.int32, (slab, columns_full), 0)
        column_pos = lax.broadcasted_iota(jnp.int32, (slab, columns_full), 1)

        def step(index, carry):
            i, z = index // layer_count, lax.rem(index, layer_count)
            below, above = jnp.maximum(z - 1, 0), jnp.minimum(z + 1, layer_count - 1)
            has_below = (z > 0).astype(jnp.float32)
            has_above = (z < layer_count - 1).astype(jnp.float32)
            present = present_ref[...] - (2.0 - has_below - has_above)
            tilt = []
            for c in range(3):
                cells = cells_ref[i, c, z]
                x_plus = jnp.where(
                    row_pos == slab - 1,
                    rim_ref[1, i, c, pl.ds(z, 1), :],
                    pltpu.roll(cells, slab - 1, 0),
                )
                x_minus = jnp.where(
                    row_pos == 0, rim_ref[0, i, c, pl.ds(z, 1), :], pltpu.roll(cells, 1, 0)
                )
                y_plus = jnp.where(
                    column_pos == columns_full - 1, 0.0, pltpu.roll(cells, columns_full - 1, 1)
                )
                y_minus = jnp.where(column_pos == 0, 0.0, pltpu.roll(cells, 1, 1))
                around = x_plus + x_minus + y_plus + y_minus
                around = around + has_above * cells_ref[i, c, above] + has_below * cells_ref[i, c, below]
                part = exchange_strength * (around - present * cells)
                if c == 0:
                    tilt.append(x_plus - x_minus)
                    field_ref[i, 0, z] = part
                elif c == 1:
                    tilt.append(y_plus - y_minus)
                    field_ref[i, 1, z] = part
                else:
                    ease = 2.0 * ease_ref[...] * cells
                    field_ref[i, 2, z] = part + (ease - chiral_strength * (tilt[0] + tilt[1]))
                    field_ref[i, 0, z] = field_ref[i, 0, z] + chiral_strength * (x_plus - x_minus)
                    field_ref[i, 1, z] = field_ref[i, 1, z] + chiral_strength * (y_plus - y_minus)
            return carry

        lax.fori_loop(0, 2 * layer_count, step, 0)

    lane = columns_full

    def cell_loop(step, carry):
        steps = slab // row_step

        def chunk(index, carry):
            z = index // steps
            start = pl.multiple_of(lax.rem(index, steps) * row_step, row_step)
            return step(z, start, carry)

        return lax.fori_loop(0, layer_count * steps, chunk, carry)

    def zeros(count):
        return tuple(jnp.zeros((row_step, lane), jnp.float32) for _ in range(count))

    def tangent_rows(z, start):
        return pl.ds(pl.multiple_of(z * slab + start, row_step), row_step)

    def neighbour_sums():
        @pl.when(jnp.logical_not(first))
        def _():
            ahead_copy().wait_recv()

        @pl.when(first)
        def _():
            for c in range(3):
                prior_ref[c] = cells_ref[0, c]

        @pl.when(jnp.logical_not(last))
        def _():
            behind_copy().wait_recv()

        @pl.when(last)
        def _():
            for c in range(3):
                next_ref[c] = cells_ref[1, c]

        for i in range(2):

            def step(z, start, carry):
                rows = pl.ds(start, row_step)
                here = [cells_ref[i, c, z, rows, :] for c in range(3)]
                if i == 0:
                    ahead = [cells_ref[1, c, z, rows, :] for c in range(3)]
                    behind = [prior_ref[c, z, rows, :] for c in range(3)]
                else:
                    ahead = [next_ref[c, z, rows, :] for c in range(3)]
                    behind = [cells_ref[0, c, z, rows, :] for c in range(3)]
                normal = [
                    here[1] * ahead[2] - here[2] * ahead[1],
                    here[2] * ahead[0] - here[0] * ahead[2],
                    here[0] * ahead[1] - here[1] * ahead[0],
                ]
                angle = arc_angle(jnp.sqrt(dot3(normal, normal)), dot3(here, ahead))
                ahead = [ahead[c] - here[c] for c in range(3)]
                behind = [here[c] - behind[c] for c in range(3)]
                ahead_on, behind_on = dot3(ahead, here), dot3(behind, here)
                ahead = [ahead[c] - ahead_on * here[c] for c in range(3)]
                behind = [behind[c] - behind_on * here[c] for c in range(3)]
                for c in range(3):
                    place = tangent_rows(z, start)
                    spec_ref[0, 3 * i + c, place, 0:columns_full] = ahead[c]
                    spec_ref[0, 3 * i + c, place, columns_full : 2 * columns_full] = behind[c]
                values = (
                    angle * angle,
                    dot3(ahead, ahead),
                    dot3(ahead, behind),
                    dot3(behind, behind),
                )
                return tuple(total + value for total, value in zip(carry, values))

            totals = cell_loop(step, zeros(4))
            for k in range(4):
                sums_ref[i, k + 1] = totals[k]

    def field_sums(i, arrived):
        turn = (2 * i - 1).astype(jnp.float32)

        def step(z, start, carry):
            rows = pl.ds(start, row_step)
            place = tangent_rows(z, start)
            sign = scale * jnp.where(lax.rem(z, 2) == 1, turn, 1.0)
            here = [cells_ref[i, c, z, rows, :] for c in range(3)]
            ahead = [spec_ref[0, 3 * i + c, place, 0:columns_full] for c in range(3)]
            behind = [
                spec_ref[0, 3 * i + c, place, columns_full : 2 * columns_full] for c in range(3)
            ]
            field = []
            for c in range(3):
                value = field_ref[i, c, z, rows, :] + sign * extra_ref[1 - i, c, rows, :]
                if arrived:
                    value = value + arrive_ref[c, z, rows, :]
                field_ref[i, c, z, rows, :] = value
                field.append(value)
            values = (dot3(here, field), dot3(field, ahead), dot3(field, behind))
            return tuple(total + value for total, value in zip(carry, values))

        totals = cell_loop(step, zeros(3))
        for k, slot in enumerate((0, 5, 6)):
            sums_ref[i, slot] = totals[k]

    barrier = pltpu.get_barrier_semaphore()
    for n, shift, d in routes:
        pl.semaphore_signal(
            barrier, inc=1, device_id=target_of(shift, d), device_id_type=pl.DeviceIdType.MESH
        )
    for c in range(3):
        own_copy(c).start()
    pl.semaphore_wait(barrier, len(routes))
    film_copy(0).start()

    @pl.when(jnp.logical_not(last))
    def _():
        ahead_copy().start()

    @pl.when(jnp.logical_not(first))
    def _():
        behind_copy().start()

    for c in range(3):
        own_copy(c).wait()
    fill_rims()
    for side in range(2):

        def sum_layers(rows):
            for c in range(3):
                layers = [cells_ref[1 - side, c, z, rows, :] for z in range(layer_count)]
                stage_ref[side, c, rows, :] = weighted(
                    [((-1.0) ** (z * side), layers[z]) for z in range(layer_count)]
                )

        row_loop(sum_layers)

        @pl.when(me == side * parts)
        def _():
            pair_ref[me] = stage_ref[side]

        @pl.when(me != side * parts)
        def _():
            pair_copy(side, me).start()

    for c in range(1, 3):
        film_copy(c).start()
    for q in range(local_planes):
        tensor_copy(q).start()

    for c in range(3):
        transform_layers(c, 0)
    local_fields()

    for c in range(3):
        film_copy(c).wait_recv()
        transform_layers(c, 1)
        for kind in range(2):
            for slot in range(parts - 1):
                plane_arrival(c, kind, slot).wait_recv()

        def forward(i, carry):
            q = local_planes - 1 - i

            @pl.when((seat == 0) & (q == 0))
            def _():
                if c == 0:
                    for d in range(1, groups):
                        pair_copy(0, lax.rem(me + d, groups)).wait_recv()
                for g in range(groups):
                    held_ref[c, g, 0, 1] = pair_ref[g, c]

            fy = jnp.concatenate([fy_ref[0], fy_ref[0], fy_ref[1]], axis=0)
            fx = jnp.concatenate([fx_ref[0], fx_ref[0], fx_ref[1]], axis=1)
            cells = jnp.concatenate(
                [held_ref[c, g, q, part] for part in range(2) for g in range(groups)], axis=0
            )
            lines = dot32(three_limbs(cells, 1), fy)
            for part in range(2):
                spec_ref[q, 2 * c + part] = dot32(
                    fx, three_limbs(lines[part * rows_full : (part + 1) * rows_full], 0)
                )
            return carry

        lax.fori_loop(0, local_planes, forward, 0)

    for q in range(local_planes):
        tensor_copy(q).wait()

    for c in range(3):

        def backward(q, carry):
            tensor_part(c, spec_ref.at[q], tensor_ref.at[q], result_ref)
            gx = jnp.concatenate([gx_ref[0], gx_ref[0], gx_ref[1]], axis=1)
            gy = jnp.concatenate([gy_ref[0], gy_ref[0], gy_ref[1]], axis=0)
            for part in range(2):
                lines = dot32(gx, three_limbs(result_ref[part], 0))
                cells = dot32(three_limbs(lines, 1), gy)
                for g in range(groups):
                    held_ref[c, g, q, part] = cells[g * slab : (g + 1) * slab]
            return carry

        lax.fori_loop(0, local_planes, backward, 0)
        for kind in (1, 0):
            for slot in range(parts - 1):
                back_copy(c, kind, slot).start()

        @pl.when(seat == 0)
        def _():
            extra_ref[half, c] = held_ref[c, me, 0, 1]
            for step in range(1, groups):
                extra_copy(c, step).start()

        for slot in range(parts - 1):
            back_arrival(c, 1, slot).wait_recv()
        transform_planes(c, 1)
        last_copy(c).start()
        for slot in range(parts - 1):
            back_arrival(c, 0, slot).wait_recv()
        transform_planes(c, 0)

    neighbour_sums()
    for c in range(3):
        for side in range(2):

            @pl.when(me != side * parts)
            def _():
                extra_arrival(side, c).wait_recv()

    field_sums(half, False)
    for c in range(3):
        last_copy(c).wait_recv()
    field_sums(1 - half, True)

    rows = [
        jnp.sum(sums_ref[i, k], axis=0, keepdims=True) for i in range(2) for k in range(7)
    ] + [jnp.zeros((1, lane), jnp.float32)] * 2
    tile = jnp.sum(jnp.concatenate(rows, axis=0), axis=1, keepdims=True)
    tile_ref[...] = jnp.broadcast_to(tile, tile_ref.shape)
    for n, shift, d in routes:
        swap_copy(n, shift, d, me).start()
    swap_ref[1, me] = tile_ref[...]
    for n, shift, d in routes:
        swap_copy(n, shift, d, lax.rem(me + groups - d, groups)).wait_recv()
    totals = []
    for n in range(3):
        total = swap_ref[n, 0]
        for g in range(1, groups):
            total = total + swap_ref[n, g]
        totals.append(total)

    def entry(n, i, k):
        return totals[n][7 * i + k : 7 * i + k + 1]

    cell_count = float(layer_count * rows_full * columns_full)
    energies = [-0.5 * entry(*at, 0) for at in ((0, 1), (1, 0), (1, 1), (2, 0))]
    distances = [jnp.sqrt(entry(*at, 1) / cell_count) for at in ((0, 1), (1, 0), (1, 1))]
    pulls = []
    for i in range(2):
        weight_next, weight_prior = tangent_weights(energies[i + 1], energies[i + 2], energies[i])
        length_square = (
            weight_next * weight_next * entry(1, i, 2)
            + 2.0 * weight_next * weight_prior * entry(1, i, 3)
            + weight_prior * weight_prior * entry(1, i, 4)
        )
        drive = weight_next * entry(1, i, 5) + weight_prior * entry(1, i, 6)
        size = jnp.sqrt(jnp.maximum(length_square, 0.0) / cell_count + epsilon)
        spring = spring_strength * (distances[i + 1] - distances[i])
        pull = (spring - drive / (cell_count * size)) / size
        pulls.append((pull * weight_next, pull * weight_prior))
    for n, shift, d in routes:
        swap_copy(n, shift, d, me).wait_send()
    peaks = []
    for i in range(2):
        end = first if i == 0 else last
        ahead_pull, behind_pull = [
            jnp.concatenate([jnp.broadcast_to(pull, (row_step, 128))] * (lane // 128), axis=1)
            for pull in pulls[i]
        ]

        def step(z, start, peak):
            rows = pl.ds(start, row_step)
            place = tangent_rows(z, start)
            here = [cells_ref[i, c, z, rows, :] for c in range(3)]
            force = []
            for c in range(3):
                ahead = spec_ref[0, 3 * i + c, place, 0:columns_full]
                behind = spec_ref[0, 3 * i + c, place, columns_full : 2 * columns_full]
                field = field_ref[i, c, z, rows, :]
                force.append(field + ahead_pull * ahead + behind_pull * behind)
            along = dot3(force, here)
            force = [jnp.where(end, 0.0, force[c] - along * here[c]) for c in range(3)]
            for c in range(3):
                field_ref[i, c, z, rows, :] = force[c]
            return (jnp.maximum(peak[0], dot3(force, force)),)

        (peak,) = cell_loop(step, zeros(1))
        peaks.append(jnp.max(peak, axis=0, keepdims=True))
        force_copy(i).start()
    peak = jnp.concatenate(peaks + [jnp.zeros((6, lane), jnp.float32)], axis=0)
    peak = jnp.broadcast_to(jnp.max(peak, axis=1, keepdims=True), (8, 128))
    tile_ref[0:8] = peak
    for d in range(1, groups):
        peak_copy(d, me).start()
    peak_ref[me] = peak
    for d in range(1, groups):
        peak_copy(d, lax.rem(me + groups - d, groups)).wait_recv()
    largest = peak_ref[0]
    for g in range(1, groups):
        largest = jnp.maximum(largest, peak_ref[g])
    small_ref[0:8] = jnp.minimum(step_limit, rotation_limit / (jnp.sqrt(largest) + epsilon))
    small_ref[8:16] = jnp.concatenate(energies[1:3] + [jnp.zeros((6, 128), jnp.float32)], axis=0)

    for i in range(2):
        force_copy(i).wait()
    for d in range(1, groups):
        peak_copy(d, me).wait_send()
    for c in range(3):
        film_copy(c).wait_send()
        last_copy(c).wait_send()
        for kind in range(2):
            for slot in range(parts - 1):
                plane_copy(c, kind, slot).wait_send()
                back_copy(c, kind, slot).wait_send()

    @pl.when(seat == 0)
    def _():
        for c in range(3):
            for step in range(1, groups):
                extra_copy(c, step).wait_send()

    for side in range(2):
        open_side = me != groups - 1 if side == 0 else me != 0

        @pl.when(open_side)
        def _():
            rim_copy(side).wait_send()

        @pl.when(me != side * parts)
        def _():
            pair_copy(side, me).wait_send()

    @pl.when(jnp.logical_not(last))
    def _():
        ahead_copy().wait_send()

    @pl.when(jnp.logical_not(first))
    def _():
        behind_copy().wait_send()


def band_step(magnet, anisotropy, kernel):
    layer_count, row_count, column_count = magnet.shape[2:]
    groups = lax.axis_size("space")
    local_planes = 2 * layer_count // groups
    full_rows = row_count * groups
    slots = groups // 2 - 1
    table_y = parity_table(column_count)
    table_x = parity_table(full_rows)
    square = full_rows == column_count
    tables = [table_limbs(t) for t in (table_y, table_x.T, table_x, table_y.T)][: 2 if square else 4]

    def entry(magnet_ref, kernel_ref, ease_ref, fy_ref, fx_ref, *refs):
        shared = (fy_ref, fx_ref) if square else ()
        scale = -4.0 / padded_cells
        band_kernel(scale, magnet_ref, kernel_ref, ease_ref, fy_ref, fx_ref, *shared, *refs)

    slab = (row_count, column_count)
    film = (layer_count,) + slab
    block = (local_planes, 2) + slab
    anywhere = pl.BlockSpec(memory_space=pl.ANY)
    inside = pl.BlockSpec(memory_space=pltpu.VMEM)
    dots = 6 * local_planes * 4 * full_rows * column_count * 3 * (full_rows + column_count // 2)
    padded_cells = 8 * layer_count * full_rows * column_count
    ease = jnp.broadcast_to(anisotropy[:, None], slab)
    signals = pltpu.SemaphoreType.DMA
    scratch = [
        (2, 3) + film,
        (3,) + film,
        (2, 3) + slab,
        (groups, 3) + slab,
        (2, 3) + slab,
        (3, 2, slots) + block,
        (3, 2, slots) + block,
        (3, groups) + block,
        (local_planes, 6, 2 * full_rows, 2 * column_count),
        (2, 3) + film,
        (3,) + film,
        (3,) + film,
        (3,) + film,
        (2, 2, 3, layer_count, column_count),
        (2, 2, 3, layer_count, column_count),
        slab,
        (2, 7, 8, column_count),
        (16, 128),
        (3, groups, 16, 128),
        (groups, 8, 128),
        (local_planes, 6, full_rows + 8, column_count + 128),
        (2, 2 * full_rows, 2 * column_count),
    ]
    semaphores = [
        (3,),
        (local_planes,),
        (3,),
        (3,),
        (2,),
        (groups,),
        (3, 2, slots),
        (3, 2, slots),
        (3, 2, slots),
        (3, 2, slots),
        (3, groups),
        (2, 3),
        (3,),
        (3,),
        (2,),
        (2,),
        (2,),
        (2,),
        (3, groups),
        (3, groups),
        (groups,),
        (groups,),
        (2,),
    ]
    return pl.pallas_call(
        entry,
        in_specs=[anywhere, anywhere] + [inside] * (1 + len(tables)),
        out_specs=[anywhere, inside],
        out_shape=[
            jax.ShapeDtypeStruct(magnet.shape, jnp.float32),
            jax.ShapeDtypeStruct((16, 128), jnp.float32),
        ],
        scratch_shapes=[pltpu.VMEM(dims, jnp.float32) for dims in scratch]
        + [signals(dims) for dims in semaphores],
        compiler_params=pltpu.CompilerParams(
            vmem_limit_bytes=67043328, collective_id=0, has_side_effects=True
        ),
        cost_estimate=pl.CostEstimate(
            flops=4 * dots, bytes_accessed=4 * magnet.size * 4, transcendentals=0
        ),
        name="band_kernel",
    )(magnet, kernel, ease, *[jnp.asarray(t) for t in tables])


def body(magnet, anisotropy, kernel):
    cell_count = magnet.shape[2] * magnet.shape[3] * lax.axis_size("space") * magnet.shape[4]
    band_force, small = band_step(magnet, anisotropy, kernel)
    move_scale, energy_total = small[0:2, 0], small[8:10, 0]
    stepped = magnet + lift_axes(move_scale) * band_force
    updated = stepped / jnp.sqrt(jnp.sum(stepped * stepped, axis=1, keepdims=True))
    return (updated, band_force, energy_total / cell_count)


def solution(mesh):
    in_specs = (P("image", None, None, "space", None), P("space"), P(None, "space", None, None))
    out_specs = (
        P("image", None, None, "space", None),
        P("image", None, None, "space", None),
        P("image"),
    )
    return jax.shard_map(body, mesh=mesh, in_specs=in_specs, out_specs=out_specs, check_vma=False)
```

```python
import functools
import math

import jax
import jax.numpy as jnp
import numpy as np
from jax import lax
from jax.experimental import pallas as pl
from jax.experimental.pallas import tpu as pltpu
from jax.sharding import PartitionSpec as P

exchange_strength = 0.25
chiral_strength = 0.3
spring_strength = 10.0
step_limit = 1.0
rotation_limit = 0.5
epsilon = 1e-06


def tangent_weights(energy_total, energy_next, energy_prior):
    rise_next = energy_next - energy_total
    rise_prior = energy_total - energy_prior
    upward = (rise_next > 0) & (rise_prior > 0)
    downward = (rise_next < 0) & (rise_prior < 0)
    larger = jnp.maximum(jnp.abs(rise_next), jnp.abs(rise_prior))
    smaller = jnp.minimum(jnp.abs(rise_next), jnp.abs(rise_prior))
    toward_next = energy_next > energy_prior
    weight_next = jnp.where(
        upward, 1.0, jnp.where(downward, 0.0, jnp.where(toward_next, larger, smaller))
    )
    weight_prior = jnp.where(
        upward, 0.0, jnp.where(downward, 1.0, jnp.where(toward_next, smaller, larger))
    )
    return (weight_next, weight_prior)


def split_limbs(values):
    upper = values.astype(jnp.bfloat16)
    return upper, (values - upper.astype(jnp.float32)).astype(jnp.bfloat16)


def table_limbs(table):
    upper = table.astype(np.float32).astype(jnp.bfloat16)
    lower = (table - upper.astype(np.float64)).astype(np.float32).astype(jnp.bfloat16)
    return np.stack([upper, lower])


def parity_table(count):
    position = np.arange(count)[:, None]
    slot = np.arange(count)[None, :]
    turn = np.pi / count
    even_part = np.cos(turn * (position * slot % (2 * count)))
    odd_part = np.sin(turn * (position * slot % (2 * count)))
    odd_part[:, 0] = np.cos(turn * (position[:, 0] * count % (2 * count)))
    return np.concatenate([even_part, odd_part], axis=1)


def half_table(count):
    place = np.arange(count)
    angle = np.pi * (place[:, None] * place[None, :] % (2 * count)) / count
    cosine, sine = np.cos(angle), np.sin(angle)
    cosine[np.abs(cosine) < 1e-12] = 0.0
    sine[np.abs(sine) < 1e-12] = 0.0
    return cosine, sine


def weighted(terms):
    total = None
    for weight, value in terms:
        weight = float(weight)
        if weight == 0.0:
            continue
        if total is None:
            total = value if weight == 1.0 else -value if weight == -1.0 else weight * value
        elif weight == 1.0:
            total = total + value
        elif weight == -1.0:
            total = total - value
        else:
            total = total + weight * value
    return total


def layers_to_spectrum(layers):
    count = len(layers)
    half = count // 2
    cosine, sine = half_table(count)
    sums = {z: layers[z] + layers[count - z] for z in range(1, half)}
    gaps = {z: layers[z] - layers[count - z] for z in range(1, half)}
    spectrum = []
    for k in range(count):
        near, far = (sums, gaps) if k % 2 == 0 else (gaps, sums)
        re = weighted(
            [(1.0, layers[0]), (cosine[half, k], layers[half])]
            + [(cosine[z, k], near[z]) for z in range(1, half)]
        )
        im = weighted(
            [(-sine[half, k], layers[half])] + [(-sine[z, k], far[z]) for z in range(1, half)]
        )
        spectrum.append((re, jnp.zeros_like(re) if im is None else im))
    return spectrum


def spectrum_to_layers(spectrum):
    count = len(spectrum)
    half = count // 2
    cosine, sine = half_table(count)
    layers = [None] * count
    evens, odds = range(2, count, 2), range(1, count, 2)
    layers[0] = weighted([(1.0, spectrum[0][0])] + [(2.0, spectrum[k][0]) for k in range(1, count)])
    layers[half] = weighted(
        [(1.0, spectrum[0][0])]
        + [(2.0 * cosine[half, k], spectrum[k][0]) for k in range(1, count)]
        + [(-2.0 * sine[half, k], spectrum[k][1]) for k in range(1, count)]
    )
    for z in range(1, half):
        even_re = weighted(
            [(1.0, spectrum[0][0])] + [(2.0 * cosine[z, k], spectrum[k][0]) for k in evens]
        )
        odd_re = weighted([(2.0 * cosine[z, k], spectrum[k][0]) for k in odds])
        even_im = weighted([(2.0 * sine[z, k], spectrum[k][1]) for k in evens])
        odd_im = weighted([(2.0 * sine[z, k], spectrum[k][1]) for k in odds])
        layers[z] = (even_re - odd_im) + (odd_re - even_im)
        layers[count - z] = (even_re - odd_im) - (odd_re - even_im)
    return layers


def dot32(left, right):
    return jnp.dot(left, right, preferred_element_type=jnp.float32)


def three_limbs(values, axis):
    upper, lower = split_limbs(values)
    return jnp.concatenate([upper, lower, upper], axis=axis)


def tensor_part(c, spec_ref, kernel_ref, out_ref):
    rows_full, columns_full = out_ref.shape[2] // 2, out_ref.shape[3] // 2
    lane = 128
    sub = 16
    top = lax.broadcasted_iota(jnp.int32, (sub, lane), 0) == 0
    left = lax.broadcasted_iota(jnp.int32, (sub, lane), 1) == 0

    def tile(row_start, first_row, start):
        rows = pl.ds(row_start, sub)
        columns = slice(start, start + lane)
        edge_columns = slice(columns_full, columns_full + lane)
        first_column = start == 0

        def loaded(component):
            body = kernel_ref[component, rows, columns]
            side = kernel_ref[component, rows, edge_columns] if first_column else None
            if not first_row:
                return body, side, None, None
            far = pl.ds(rows_full, 1)
            body_far = kernel_ref[component, far, columns]
            side_far = kernel_ref[component, far, edge_columns] if first_column else None
            return body, side, body_far, side_far

        def pick(parts, odd_x, odd_y):
            body, side, body_far, side_far = parts
            mixed = jnp.where(left, side, body) if odd_y and first_column else body
            if odd_x and first_row:
                far = body_far
                if odd_y and first_column:
                    far = jnp.where(left[:1], side_far, far)
                mixed = jnp.where(top, far, mixed)
            return mixed

        own = loaded(c)
        k_xy = pick(loaded(3), 0, 0) if c < 2 else None
        k_xz = loaded(4) if c != 1 else None
        k_yz = loaded(5) if c != 0 else None

        def place(px, py):
            offset = py * columns_full + start
            return pl.ds(row_start + px * rows_full, sub), slice(offset, offset + lane)

        def spec(px, py, f):
            at_rows, at_columns = place(px, py)
            return spec_ref[f, at_rows, at_columns]

        for px in range(2):
            for py in range(2):
                own_here = pick(own, px, py)
                xz_here = pick(k_xz, 0, py) if c != 1 else None
                yz_here = pick(k_yz, px, 0) if c != 0 else None
                for part in range(2):
                    turn = 1.0 if part else -1.0
                    sx = turn if px else -turn
                    sy = turn if py else -turn
                    other = 1 - part
                    total = own_here * spec(px, py, 2 * c + part)
                    if c < 2:
                        across = k_xy * spec(1 - px, 1 - py, 2 * (1 - c) + part)
                        total = total - across if px == py else total + across
                    if c == 0:
                        third = xz_here * spec(1 - px, py, 4 + other)
                        total = total + third if sx > 0 else total - third
                    elif c == 1:
                        third = yz_here * spec(px, 1 - py, 4 + other)
                        total = total + third if sy > 0 else total - third
                    else:
                        third = xz_here * spec(1 - px, py, other)
                        total = total + third if sx > 0 else total - third
                        third = yz_here * spec(px, 1 - py, 2 + other)
                        total = total + third if sy > 0 else total - third
                    if first_row:
                        total = jnp.where(top, 0.5 * total, total)
                    if first_column:
                        total = jnp.where(left, 0.5 * total, total)
                    upper, lower = split_limbs(total)
                    at_rows, at_columns = place(px, py)
                    out_ref[part, 0, at_rows, at_columns] = upper
                    out_ref[part, 1, at_rows, at_columns] = lower

    for start in range(0, columns_full, lane):
        tile(0, True, start)

    def step(i, carry):
        row_start = pl.multiple_of(i * sub, sub)
        for start in range(0, columns_full, lane):
            tile(row_start, False, start)
        return carry

    lax.fori_loop(1, rows_full // sub, step, 0)


def arc_angle(sine, cosine):
    size = jnp.abs(cosine)
    low, high = jnp.minimum(sine, size), jnp.maximum(sine, size)
    ratio = low / jnp.maximum(high, 1e-37)
    wide = ratio > 0.41421356
    ratio = jnp.where(wide, (ratio - 1.0) / (ratio + 1.0), ratio)
    square = ratio * ratio
    series = ((8.05374449538e-2 * square - 1.38776856032e-1) * square + 1.99777106478e-1) * square
    angle = (series - 3.33329491539e-1) * square * ratio + ratio
    angle = jnp.where(wide, angle + 0.25 * math.pi, angle)
    angle = jnp.where(sine > size, 0.5 * math.pi - angle, angle)
    return jnp.where(cosine < 0.0, math.pi - angle, angle)


def dot3(first, second):
    return first[0] * second[0] + first[1] * second[1] + first[2] * second[2]


def band_kernel(
    scale,
    magnet_ref,
    kernel_ref,
    anisotropy_ref,
    source_tables,
    updated_ref,
    force_ref,
    small_ref,
    tables,
    cells_ref,
    film_ref,
    stage_ref,
    pair_ref,
    extra_ref,
    send_ref,
    back_ref,
    held_ref,
    spec_ref,
    field_ref,
    arrive_ref,
    next_ref,
    prior_ref,
    rim_out_ref,
    rim_ref,
    present_ref,
    ease_ref,
    sums_ref,
    tile_ref,
    swap_ref,
    peak_ref,
    tensor_ref,
    result_ref,
    own_sem,
    tensor_sem,
    film_send,
    film_recv,
    pair_send,
    pair_recv,
    plane_send,
    plane_recv,
    back_send,
    back_recv,
    extra_send,
    extra_recv,
    last_send,
    last_recv,
    image_send,
    image_recv,
    rim_send,
    rim_recv,
    swap_send,
    swap_recv,
    peak_send,
    peak_recv,
    force_sem,
    update_sem,
    table_sem,
):
    fy_ref, fx_ref = tables[:2]
    gx_ref, gy_ref = tables[:2] if len(tables) == 2 else tables[2:]
    groups, local_planes = held_ref.shape[1], held_ref.shape[2]
    slab, columns_full = held_ref.shape[4], held_ref.shape[5]
    layer_count = cells_ref.shape[2]
    rows_full = groups * slab
    parts = groups // 2
    me = lax.axis_index("space")
    half, seat = me // parts, lax.rem(me, parts)
    partner = lax.rem(me + parts, groups)
    flip = (1 - 2 * half).astype(jnp.float32)
    row_step = 8
    images, image = lax.axis_size("image"), lax.axis_index("image")
    first, last = image == 0, image == images - 1
    shifts = (-1, 0, 1)
    routes = [
        (n, shift, d)
        for n, shift in enumerate(shifts)
        for d in range(groups)
        if shift != 0 or d != 0
    ]

    def gate(exists, action):
        if exists is None:
            action()
        else:
            pl.when(exists)(action)

    def receiver(shift):
        return None if shift == 0 else jnp.logical_not(last if shift < 0 else first)

    def sender(shift):
        return None if shift == 0 else jnp.logical_not(first if shift < 0 else last)

    def target_of(shift, d):
        return {"image": lax.rem(image - shift + images, images), "space": lax.rem(me + d, groups)}

    def remote(src, dst, send, recv, target):
        return pltpu.make_async_remote_copy(
            src_ref=src,
            dst_ref=dst,
            send_sem=send,
            recv_sem=recv,
            device_id=target if isinstance(target, dict) else {"space": target},
            device_id_type=pl.DeviceIdType.MESH,
        )

    def row_loop(step):
        def chunk(i, carry):
            step(pl.ds(pl.multiple_of(i * row_step, row_step), row_step))
            return carry

        lax.fori_loop(0, slab // row_step, chunk, 0)

    def own_copy(c):
        return pltpu.make_async_copy(magnet_ref.at[:, c], cells_ref.at[:, c], own_sem.at[c])

    def tensor_copy(q):
        return pltpu.make_async_copy(
            kernel_ref.at[:, q, pl.ds(0, rows_full + 8), pl.ds(0, columns_full + 128)],
            tensor_ref.at[q],
            tensor_sem.at[q],
        )

    def film_copy(c):
        return remote(
            magnet_ref.at[1 - half, c], film_ref.at[c], film_send.at[c], film_recv.at[c], partner
        )

    def pair_copy(side, source):
        return remote(
            stage_ref.at[side],
            pair_ref.at[source],
            pair_send.at[side],
            pair_recv.at[source],
            side * parts,
        )

    def place_of(seat_index, kind):
        return lax.rem((half + kind) * parts + seat_index, groups)

    def plane_copy(c, kind, slot):
        target = lax.rem(seat + 1 + slot, parts)
        return remote(
            send_ref.at[c, kind, slot],
            held_ref.at[c, place_of(seat, kind)],
            plane_send.at[c, kind, slot],
            plane_recv.at[c, kind, parts - 2 - slot],
            half * parts + target,
        )

    def plane_arrival(c, kind, slot):
        source = lax.rem(seat + 1 + slot, parts)
        return remote(
            send_ref.at[c, kind, slot],
            held_ref.at[c, place_of(source, kind)],
            plane_send.at[c, kind, slot],
            plane_recv.at[c, kind, slot],
            half * parts + source,
        )

    def back_copy(c, q, kind, slot):
        target = lax.rem(seat + 1 + slot, parts)
        return remote(
            held_ref.at[c, place_of(target, kind), q],
            back_ref.at[c, kind, parts - 2 - slot, q],
            back_send.at[c, q, kind, slot],
            back_recv.at[c, q, kind, parts - 2 - slot],
            half * parts + target,
        )

    def back_arrival(c, q, kind, slot):
        source = lax.rem(seat + 1 + slot, parts)
        return remote(
            held_ref.at[c, place_of(source, kind), q],
            back_ref.at[c, kind, slot, q],
            back_send.at[c, q, kind, slot],
            back_recv.at[c, q, kind, slot],
            half * parts + source,
        )

    def extra_copy(c, step):
        target = lax.rem(me + step, groups)
        return remote(
            held_ref.at[c, target, 0, 1],
            extra_ref.at[half, c],
            extra_send.at[c, step],
            extra_recv.at[half, c],
            target,
        )

    def extra_arrival(side, c):
        return remote(
            held_ref.at[c, 0, 0, 1],
            extra_ref.at[side, c],
            extra_send.at[c, 0],
            extra_recv.at[side, c],
            side * parts,
        )

    def last_copy(c):
        return remote(
            film_ref.at[c], arrive_ref.at[c], last_send.at[c], last_recv.at[c], partner
        )

    def ahead_copy():
        return remote(
            magnet_ref.at[1],
            prior_ref,
            image_send.at[0],
            image_recv.at[0],
            {"image": lax.rem(image + 1, images)},
        )

    def behind_copy():
        return remote(
            magnet_ref.at[0],
            next_ref,
            image_send.at[1],
            image_recv.at[1],
            {"image": lax.rem(image + images - 1, images)},
        )

    def rim_copy(side):
        return remote(
            rim_out_ref.at[side],
            rim_ref.at[side],
            rim_send.at[side],
            rim_recv.at[side],
            lax.rem(me + (1 if side == 0 else groups - 1), groups),
        )

    def swap_copy(n, shift, d, slot):
        return remote(
            tile_ref, swap_ref.at[n, slot], swap_send.at[n, d], swap_recv.at[n, d], target_of(shift, d)
        )

    def peak_copy(d, slot):
        return remote(
            tile_ref.at[pl.ds(0, 8)],
            peak_ref.at[slot],
            peak_send.at[d],
            peak_recv.at[d],
            lax.rem(me + d, groups),
        )

    def table_copy(n):
        return pltpu.make_async_copy(source_tables[n], tables[n], table_sem.at[n])

    def update_copy(i):
        return pltpu.make_async_copy(cells_ref.at[i], updated_ref.at[i], update_sem.at[i])

    def force_copy(i):
        return pltpu.make_async_copy(field_ref.at[i], force_ref.at[i], force_sem.at[i])

    def transform_layers(c, kind):
        place = place_of(seat, kind)

        def variant(here):
            def step(rows):
                if kind == 0:
                    layers = [cells_ref[half, c, z, rows, :] for z in range(layer_count)]
                else:
                    layers = [film_ref[c, z, rows, :] for z in range(layer_count)]
                layers = [v * flip if z % 2 else v for z, v in enumerate(layers)]
                spectrum = layers_to_spectrum(layers)
                for k in range(layer_count):
                    target, q = k // local_planes, k % local_planes
                    slot = (target - here) % parts - 1
                    for part in range(2):
                        if target == here:
                            held_ref[c, place, q, part, rows, :] = spectrum[k][part]
                        else:
                            send_ref[c, kind, slot, q, part, rows, :] = spectrum[k][part]

            row_loop(step)

        for here in range(parts):
            pl.when(seat == here)(functools.partial(variant, here))
        for slot in range(parts - 1):
            plane_copy(c, kind, slot).start()

    def transform_planes(c, kind):
        place = place_of(seat, kind)

        def variant(here):
            def step(rows):
                spectrum = []
                for k in range(layer_count):
                    source, q = k // local_planes, k % local_planes
                    slot = (source - here) % parts - 1
                    if source == here:
                        spectrum.append(
                            [held_ref[c, place, q, part, rows, :] for part in range(2)]
                        )
                    else:
                        spectrum.append(
                            [back_ref[c, kind, slot, q, part, rows, :] for part in range(2)]
                        )
                for z, value in enumerate(spectrum_to_layers(spectrum)):
                    value = value * (scale * flip if z % 2 else scale)
                    if kind == 0:
                        field_ref[half, c, z, rows, :] = field_ref[half, c, z, rows, :] + value
                    else:
                        film_ref[c, z, rows, :] = value

            row_loop(step)

        for here in range(parts):
            pl.when(seat == here)(functools.partial(variant, here))

    def fill_rims():
        def step(f, carry):
            i, c = f // 3, lax.rem(f, 3)
            for side in range(2):
                row = slab - 1 if side == 0 else 0
                rim_out_ref[side, i, c] = jnp.concatenate(
                    [cells_ref[i, c, z, row : row + 1, :] for z in range(layer_count)], axis=0
                )
            return carry

        lax.fori_loop(0, 6, step, 0)
        row_pos = lax.broadcasted_iota(jnp.int32, (slab, columns_full), 0) + me * slab
        column_pos = lax.broadcasted_iota(jnp.int32, (slab, columns_full), 1)
        faces = [row_pos == 0, row_pos == rows_full - 1]
        faces += [column_pos == 0, column_pos == columns_full - 1]
        present_ref[...] = 6.0 - sum(jnp.where(face, 1.0, 0.0) for face in faces)
        for side in range(2):
            open_side = me != groups - 1 if side == 0 else me != 0

            @pl.when(open_side)
            def _():
                rim_copy(side).start()

            no_source = me == 0 if side == 0 else me == groups - 1

            @pl.when(no_source)
            def _():
                rim_ref[side] = jnp.zeros(rim_ref.shape[1:], jnp.float32)

    def wait_rims():
        for side in range(2):
            has_source = me != 0 if side == 0 else me != groups - 1

            @pl.when(has_source)
            def _():
                rim_copy(side).wait_recv()

    def local_fields(i):
        row_pos = lax.broadcasted_iota(jnp.int32, (slab, columns_full), 0)
        column_pos = lax.broadcasted_iota(jnp.int32, (slab, columns_full), 1)

        def step(z, carry):
            below, above = jnp.maximum(z - 1, 0), jnp.minimum(z + 1, layer_count - 1)
            has_below = (z > 0).astype(jnp.float32)
            has_above = (z < layer_count - 1).astype(jnp.float32)
            present = present_ref[...] - (2.0 - has_below - has_above)
            tilt = []
            for c in range(3):
                cells = cells_ref[i, c, z]
                x_plus = jnp.where(
                    row_pos == slab - 1,
                    rim_ref[1, i, c, pl.ds(z, 1), :],
                    pltpu.roll(cells, slab - 1, 0),
                )
                x_minus = jnp.where(
                    row_pos == 0, rim_ref[0, i, c, pl.ds(z, 1), :], pltpu.roll(cells, 1, 0)
                )
                y_plus = jnp.where(
                    column_pos == columns_full - 1, 0.0, pltpu.roll(cells, columns_full - 1, 1)
                )
                y_minus = jnp.where(column_pos == 0, 0.0, pltpu.roll(cells, 1, 1))
                around = x_plus + x_minus + y_plus + y_minus
                around = around + has_above * cells_ref[i, c, above] + has_below * cells_ref[i, c, below]
                part = exchange_strength * (around - present * cells)
                if c == 0:
                    tilt.append(x_plus - x_minus)
                    field_ref[i, 0, z] = part
                elif c == 1:
                    tilt.append(y_plus - y_minus)
                    field_ref[i, 1, z] = part
                else:
                    ease = ease_ref[...] * cells
                    field_ref[i, 2, z] = part + (ease - chiral_strength * (tilt[0] + tilt[1]))
                    field_ref[i, 0, z] = field_ref[i, 0, z] + chiral_strength * (x_plus - x_minus)
                    field_ref[i, 1, z] = field_ref[i, 1, z] + chiral_strength * (y_plus - y_minus)
            return carry

        lax.fori_loop(0, layer_count, step, 0)

    lane = columns_full

    def cell_loop(step, carry):
        steps = slab // (2 * row_step)

        def chunk(index, carry):
            z = index // steps
            start = pl.multiple_of(lax.rem(index, steps) * 2 * row_step, 2 * row_step)
            for offset in (0, row_step):
                carry = step(z, pl.multiple_of(start + offset, row_step), carry)
            return carry

        return lax.fori_loop(0, layer_count * steps, chunk, carry)

    def zeros(count):
        return tuple(jnp.zeros((row_step, lane), jnp.float32) for _ in range(count))

    def tangent_rows(z, start):
        return pl.ds(pl.multiple_of(z * slab + start, row_step), row_step)

    def neighbour_sums():
        @pl.when(jnp.logical_not(first))
        def _():
            ahead_copy().wait_recv()

        @pl.when(first)
        def _():
            for c in range(3):
                prior_ref[c] = cells_ref[0, c]

        @pl.when(jnp.logical_not(last))
        def _():
            behind_copy().wait_recv()

        @pl.when(last)
        def _():
            for c in range(3):
                next_ref[c] = cells_ref[1, c]

        for i in range(2):

            def step(z, start, carry):
                rows = pl.ds(start, row_step)
                here = [cells_ref[i, c, z, rows, :] for c in range(3)]
                if i == 0:
                    ahead = [cells_ref[1, c, z, rows, :] for c in range(3)]
                    behind = [prior_ref[c, z, rows, :] for c in range(3)]
                else:
                    ahead = [next_ref[c, z, rows, :] for c in range(3)]
                    behind = [cells_ref[0, c, z, rows, :] for c in range(3)]
                normal = [
                    here[1] * ahead[2] - here[2] * ahead[1],
                    here[2] * ahead[0] - here[0] * ahead[2],
                    here[0] * ahead[1] - here[1] * ahead[0],
                ]
                angle = arc_angle(jnp.sqrt(dot3(normal, normal)), dot3(here, ahead))
                ahead = [ahead[c] - here[c] for c in range(3)]
                behind = [here[c] - behind[c] for c in range(3)]
                ahead_on, behind_on = dot3(ahead, here), dot3(behind, here)
                ahead = [ahead[c] - ahead_on * here[c] for c in range(3)]
                behind = [behind[c] - behind_on * here[c] for c in range(3)]
                for c in range(3):
                    place = tangent_rows(z, start)
                    spec_ref[0, 3 * i + c, place, 0:columns_full] = ahead[c]
                    spec_ref[0, 3 * i + c, place, columns_full : 2 * columns_full] = behind[c]
                values = (
                    angle * angle,
                    dot3(ahead, ahead),
                    dot3(ahead, behind),
                    dot3(behind, behind),
                )
                return tuple(total + value for total, value in zip(carry, values))

            totals = cell_loop(step, zeros(4))
            for k in range(4):
                sums_ref[i, k + 1] = totals[k]

    def field_sums(i, c, arrived):
        turn = (2 * i - 1).astype(jnp.float32)

        def step(z, start, carry):
            rows = pl.ds(start, row_step)
            place = tangent_rows(z, start)
            sign = scale * jnp.where(lax.rem(z, 2) == 1, turn, 1.0)
            field = field_ref[i, c, z, rows, :] + sign * extra_ref[1 - i, c, rows, :]
            if arrived:
                field = field + arrive_ref[c, z, rows, :]
            field_ref[i, c, z, rows, :] = field
            values = (
                cells_ref[i, c, z, rows, :] * field,
                field * spec_ref[0, 3 * i + c, place, 0:columns_full],
                field * spec_ref[0, 3 * i + c, place, columns_full : 2 * columns_full],
            )
            return tuple(total + value for total, value in zip(carry, values))

        totals = cell_loop(step, zeros(3))
        for k, slot in enumerate((0, 5, 6)):
            sums_ref[i, slot] = totals[k] if c == 0 else sums_ref[i, slot] + totals[k]

    barrier = pltpu.get_barrier_semaphore()
    for n, shift, d in routes:
        signal = functools.partial(
            pl.semaphore_signal,
            barrier,
            inc=1,
            device_id=target_of(shift, d),
            device_id_type=pl.DeviceIdType.MESH,
        )
        gate(receiver(shift), signal)
    for c in range(3):
        own_copy(c).start()
    for n in range(len(tables)):
        table_copy(n).start()

    def spread(r, carry):
        ease_ref[pl.ds(r, 1), :] = jnp.full((1, columns_full), 2.0 * anisotropy_ref[r])
        return carry

    lax.fori_loop(0, slab, spread, 0)
    ends = first.astype(jnp.int32) + last.astype(jnp.int32)
    pl.semaphore_wait(barrier, len(routes) - groups * ends)
    film_copy(0).start()

    @pl.when(jnp.logical_not(last))
    def _():
        ahead_copy().start()

    @pl.when(jnp.logical_not(first))
    def _():
        behind_copy().start()

    for c in range(3):
        own_copy(c).wait()
    fill_rims()
    for side in range(2):

        def sum_layers(rows):
            for c in range(3):
                layers = [cells_ref[1 - side, c, z, rows, :] for z in range(layer_count)]
                stage_ref[side, c, rows, :] = weighted(
                    [((-1.0) ** (z * side), layers[z]) for z in range(layer_count)]
                )

        row_loop(sum_layers)

        @pl.when(me == side * parts)
        def _():
            pair_ref[me] = stage_ref[side]

        @pl.when(me != side * parts)
        def _():
            pair_copy(side, me).start()

    for c in range(1, 3):
        film_copy(c).start()
    for q in range(local_planes):
        tensor_copy(q).start()

    for c in range(3):
        transform_layers(c, 0)
    for n in range(len(tables)):
        table_copy(n).wait()
    for c in range(3):
        film_copy(c).wait_recv()
        transform_layers(c, 1)
        for kind in range(2):
            for slot in range(parts - 1):
                plane_arrival(c, kind, slot).wait_recv()

        def forward(i, carry):
            q = local_planes - 1 - i

            @pl.when((seat == 0) & (q == 0))
            def _():
                if c == 0:
                    for d in range(1, groups):
                        pair_copy(0, lax.rem(me + d, groups)).wait_recv()
                for g in range(groups):
                    held_ref[c, g, 0, 1] = pair_ref[g, c]

            fy = jnp.concatenate([fy_ref[0], fy_ref[0], fy_ref[1]], axis=0)
            fx = jnp.concatenate([fx_ref[0], fx_ref[0], fx_ref[1]], axis=1)
            cells = jnp.concatenate(
                [held_ref[c, g, q, part] for part in range(2) for g in range(groups)], axis=0
            )
            lines = dot32(three_limbs(cells, 1), fy)
            for part in range(2):
                spec_ref[q, 2 * c + part] = dot32(
                    fx, three_limbs(lines[part * rows_full : (part + 1) * rows_full], 0)
                )
            return carry

        lax.fori_loop(0, local_planes, forward, 0)
        if c == 0:
            wait_rims()
        if c < 2:
            local_fields(c)

    for q in range(local_planes):
        tensor_copy(q).wait()

    for c in range(3):

        def backward(q, carry):
            tensor_part(c, spec_ref.at[q], tensor_ref.at[q], result_ref)
            gx = jnp.concatenate([gx_ref[0], gx_ref[0], gx_ref[1]], axis=1)
            gy = jnp.concatenate([gy_ref[0], gy_ref[0], gy_ref[1]], axis=0)
            for part in range(2):
                upper, lower = result_ref[part, 0], result_ref[part, 1]
                lines = dot32(gx, jnp.concatenate([upper, lower, upper], axis=0))
                cells = dot32(three_limbs(lines, 1), gy)
                for g in range(groups):
                    held_ref[c, g, q, part] = cells[g * slab : (g + 1) * slab]
            for kind in (1, 0):
                for slot in range(parts - 1):
                    back_copy(c, q, kind, slot).start()

            @pl.when((seat == 0) & (q == 0))
            def _():
                extra_ref[half, c] = held_ref[c, me, 0, 1]
                for step in range(1, groups):
                    extra_copy(c, step).start()

            return carry

        lax.fori_loop(0, local_planes, backward, 0)
        for kind in (1, 0):
            for q in range(local_planes):
                for slot in range(parts - 1):
                    back_arrival(c, q, kind, slot).wait_recv()
            transform_planes(c, kind)
            if kind == 1:
                last_copy(c).start()

    neighbour_sums()
    for c in range(3):
        for side in range(2):

            @pl.when(me != side * parts)
            def _():
                extra_arrival(side, c).wait_recv()

        field_sums(half, c, False)
    for c in range(3):
        last_copy(c).wait_recv()
        field_sums(1 - half, c, True)

    rows = [
        jnp.sum(sums_ref[i, k], axis=0, keepdims=True) for i in range(2) for k in range(7)
    ] + [jnp.zeros((1, lane), jnp.float32)] * 2
    tile = jnp.sum(jnp.concatenate(rows, axis=0), axis=1, keepdims=True)
    tile_ref[...] = jnp.broadcast_to(tile, tile_ref.shape)
    for n, shift, d in routes:
        gate(receiver(shift), swap_copy(n, shift, d, me).start)
    swap_ref[1, me] = tile_ref[...]
    for n, end in ((0, first), (2, last)):

        @pl.when(end)
        def _():
            swap_ref[n] = jnp.zeros(swap_ref.shape[1:], jnp.float32)

    for n, shift, d in routes:
        gate(sender(shift), swap_copy(n, shift, d, lax.rem(me + groups - d, groups)).wait_recv)
    totals = []
    for n in range(3):
        total = swap_ref[n, 0]
        for g in range(1, groups):
            total = total + swap_ref[n, g]
        totals.append(total)

    def entry(n, i, k):
        return totals[n][7 * i + k : 7 * i + k + 1]

    cell_count = float(layer_count * rows_full * columns_full)
    energies = [-0.5 * entry(*at, 0) for at in ((0, 1), (1, 0), (1, 1), (2, 0))]
    distances = [jnp.sqrt(entry(*at, 1) / cell_count) for at in ((0, 1), (1, 0), (1, 1))]
    pulls = []
    for i in range(2):
        weight_next, weight_prior = tangent_weights(energies[i + 1], energies[i + 2], energies[i])
        length_square = (
            weight_next * weight_next * entry(1, i, 2)
            + 2.0 * weight_next * weight_prior * entry(1, i, 3)
            + weight_prior * weight_prior * entry(1, i, 4)
        )
        drive = weight_next * entry(1, i, 5) + weight_prior * entry(1, i, 6)
        size = jnp.sqrt(jnp.maximum(length_square, 0.0) / cell_count + epsilon)
        spring = spring_strength * (distances[i + 1] - distances[i])
        pull = (spring - drive / (cell_count * size)) / size
        pulls.append((pull * weight_next, pull * weight_prior))
    for n, shift, d in routes:
        gate(receiver(shift), swap_copy(n, shift, d, me).wait_send)
    peaks = []
    for i in range(2):
        end = first if i == 0 else last
        ahead_pull, behind_pull = [
            jnp.concatenate([jnp.broadcast_to(pull, (row_step, 128))] * (lane // 128), axis=1)
            for pull in pulls[i]
        ]

        def step(z, start, peak):
            rows = pl.ds(start, row_step)
            place = tangent_rows(z, start)
            here = [cells_ref[i, c, z, rows, :] for c in range(3)]
            force = []
            for c in range(3):
                ahead = spec_ref[0, 3 * i + c, place, 0:columns_full]
                behind = spec_ref[0, 3 * i + c, place, columns_full : 2 * columns_full]
                field = field_ref[i, c, z, rows, :]
                force.append(field + ahead_pull * ahead + behind_pull * behind)
            along = dot3(force, here)
            force = [jnp.where(end, 0.0, force[c] - along * here[c]) for c in range(3)]
            for c in range(3):
                field_ref[i, c, z, rows, :] = force[c]
            return (jnp.maximum(peak[0], dot3(force, force)),)

        (peak,) = cell_loop(step, zeros(1))
        peaks.append(jnp.max(peak, axis=0, keepdims=True))
        force_copy(i).start()
    peak = jnp.concatenate(peaks + [jnp.zeros((6, lane), jnp.float32)], axis=0)
    peak = jnp.broadcast_to(jnp.max(peak, axis=1, keepdims=True), (8, 128))
    tile_ref[0:8] = peak
    for d in range(1, groups):
        peak_copy(d, me).start()
    peak_ref[me] = peak
    for d in range(1, groups):
        peak_copy(d, lax.rem(me + groups - d, groups)).wait_recv()
    largest = peak_ref[0]
    for g in range(1, groups):
        largest = jnp.maximum(largest, peak_ref[g])
    moves = jnp.minimum(step_limit, rotation_limit / (jnp.sqrt(largest) + epsilon))
    for i in range(2):
        move = jnp.broadcast_to(moves[i : i + 1], (row_step, 128))
        move = jnp.concatenate([move] * (lane // 128), axis=1)

        def step(z, start, carry):
            rows = pl.ds(start, row_step)
            moved = [
                cells_ref[i, c, z, rows, :] + move * field_ref[i, c, z, rows, :] for c in range(3)
            ]
            inverse = 1.0 / jnp.sqrt(dot3(moved, moved))
            for c in range(3):
                cells_ref[i, c, z, rows, :] = inverse * moved[c]
            return carry

        cell_loop(step, 0)
        update_copy(i).start()
    energy = jnp.concatenate(energies[1:3] + [jnp.zeros((6, 128), jnp.float32)], axis=0)
    small_ref[...] = energy / cell_count
    for i in range(2):
        force_copy(i).wait()
        update_copy(i).wait()
    for d in range(1, groups):
        peak_copy(d, me).wait_send()
    for c in range(3):
        film_copy(c).wait_send()
        last_copy(c).wait_send()
        for kind in range(2):
            for slot in range(parts - 1):
                plane_copy(c, kind, slot).wait_send()
                for q in range(local_planes):
                    back_copy(c, q, kind, slot).wait_send()

    @pl.when(seat == 0)
    def _():
        for c in range(3):
            for step in range(1, groups):
                extra_copy(c, step).wait_send()

    for side in range(2):
        open_side = me != groups - 1 if side == 0 else me != 0

        @pl.when(open_side)
        def _():
            rim_copy(side).wait_send()

        @pl.when(me != side * parts)
        def _():
            pair_copy(side, me).wait_send()

    @pl.when(jnp.logical_not(last))
    def _():
        ahead_copy().wait_send()

    @pl.when(jnp.logical_not(first))
    def _():
        behind_copy().wait_send()


def band_step(magnet, anisotropy, kernel):
    layer_count, row_count, column_count = magnet.shape[2:]
    groups = lax.axis_size("space")
    local_planes = 2 * layer_count // groups
    full_rows = row_count * groups
    slots = groups // 2 - 1
    table_y = parity_table(column_count)
    table_x = parity_table(full_rows)
    square = full_rows == column_count
    tables = [table_limbs(t) for t in (table_y, table_x.T, table_x, table_y.T)][: 2 if square else 4]

    def entry(magnet_ref, kernel_ref, anisotropy_ref, *refs):
        count = len(tables)
        sources, outs = refs[:count], refs[count : count + 3]
        held, rest = refs[count + 3 : 2 * count + 3], refs[2 * count + 3 :]
        scale = -4.0 / padded_cells
        band_kernel(
            scale, magnet_ref, kernel_ref, anisotropy_ref, sources, *outs, held, *rest
        )

    slab = (row_count, column_count)
    film = (layer_count,) + slab
    block = (local_planes, 2) + slab
    anywhere = pl.BlockSpec(memory_space=pl.ANY)
    inside = pl.BlockSpec(memory_space=pltpu.VMEM)
    dots = 6 * local_planes * 4 * full_rows * column_count * 3 * (full_rows + column_count // 2)
    padded_cells = 8 * layer_count * full_rows * column_count
    signals = pltpu.SemaphoreType.DMA
    scratch = [
        (2, 3) + film,
        (3,) + film,
        (2, 3) + slab,
        (groups, 3) + slab,
        (2, 3) + slab,
        (3, 2, slots) + block,
        (3, 2, slots) + block,
        (3, groups) + block,
        (local_planes, 6, 2 * full_rows, 2 * column_count),
        (2, 3) + film,
        (3,) + film,
        (3,) + film,
        (3,) + film,
        (2, 2, 3, layer_count, column_count),
        (2, 2, 3, layer_count, column_count),
        slab,
        slab,
        (2, 7, 8, column_count),
        (16, 128),
        (3, groups, 16, 128),
        (groups, 8, 128),
        (local_planes, 6, full_rows + 8, column_count + 128),
    ]
    semaphores = [
        (3,),
        (local_planes,),
        (3,),
        (3,),
        (2,),
        (groups,),
        (3, 2, slots),
        (3, 2, slots),
        (3, local_planes, 2, slots),
        (3, local_planes, 2, slots),
        (3, groups),
        (2, 3),
        (3,),
        (3,),
        (2,),
        (2,),
        (2,),
        (2,),
        (3, groups),
        (3, groups),
        (groups,),
        (groups,),
        (2,),
        (2,),
        (len(tables),),
    ]
    return pl.pallas_call(
        entry,
        in_specs=[anywhere, anywhere, pl.BlockSpec(memory_space=pltpu.SMEM)]
        + [anywhere] * len(tables),
        out_specs=[anywhere, anywhere, inside],
        out_shape=[
            jax.ShapeDtypeStruct(magnet.shape, jnp.float32),
            jax.ShapeDtypeStruct(magnet.shape, jnp.float32),
            jax.ShapeDtypeStruct((8, 128), jnp.float32),
        ],
        scratch_shapes=[pltpu.VMEM(t.shape, jnp.bfloat16) for t in tables]
        + [pltpu.VMEM(dims, jnp.float32) for dims in scratch]
        + [pltpu.VMEM((2, 2, 2 * full_rows, 2 * column_count), jnp.bfloat16)]
        + [signals(dims) for dims in semaphores],
        compiler_params=pltpu.CompilerParams(
            vmem_limit_bytes=67043328, collective_id=0, has_side_effects=True
        ),
        cost_estimate=pl.CostEstimate(
            flops=4 * dots, bytes_accessed=4 * magnet.size * 4, transcendentals=0
        ),
        name="band_kernel",
    )(magnet, kernel, anisotropy, *[jnp.asarray(t) for t in tables])


def body(magnet, anisotropy, kernel):
    updated, band_force, small = band_step(magnet, anisotropy, kernel)
    return (updated, band_force, small[: magnet.shape[0], 0])


def solution(mesh):
    in_specs = (P("image", None, None, "space", None), P("space"), P(None, "space", None, None))
    out_specs = (
        P("image", None, None, "space", None),
        P("image", None, None, "space", None),
        P("image"),
    )
    return jax.shard_map(body, mesh=mesh, in_specs=in_specs, out_specs=out_specs, check_vma=False)
```

```python
import functools
import math

import jax
import jax.numpy as jnp
import numpy as np
from jax import lax
from jax.experimental import pallas as pl
from jax.experimental.pallas import tpu as pltpu
from jax.sharding import PartitionSpec as P

exchange_strength = 0.25
chiral_strength = 0.3
spring_strength = 10.0
step_limit = 1.0
rotation_limit = 0.5
epsilon = 1e-06


def tangent_weights(energy_total, energy_next, energy_prior):
    rise_next = energy_next - energy_total
    rise_prior = energy_total - energy_prior
    upward = (rise_next > 0) & (rise_prior > 0)
    downward = (rise_next < 0) & (rise_prior < 0)
    larger = jnp.maximum(jnp.abs(rise_next), jnp.abs(rise_prior))
    smaller = jnp.minimum(jnp.abs(rise_next), jnp.abs(rise_prior))
    toward_next = energy_next > energy_prior
    weight_next = jnp.where(
        upward, 1.0, jnp.where(downward, 0.0, jnp.where(toward_next, larger, smaller))
    )
    weight_prior = jnp.where(
        upward, 0.0, jnp.where(downward, 1.0, jnp.where(toward_next, smaller, larger))
    )
    return (weight_next, weight_prior)


def split_limbs(values):
    upper = values.astype(jnp.bfloat16)
    return upper, (values - upper.astype(jnp.float32)).astype(jnp.bfloat16)


def table_limbs(table):
    upper = table.astype(np.float32).astype(jnp.bfloat16)
    lower = (table - upper.astype(np.float64)).astype(np.float32).astype(jnp.bfloat16)
    return np.stack([upper, lower])


def parity_table(count):
    position = np.arange(count)[:, None]
    slot = np.arange(count)[None, :]
    turn = np.pi / count
    even_part = np.cos(turn * (position * slot % (2 * count)))
    odd_part = np.sin(turn * (position * slot % (2 * count)))
    odd_part[:, 0] = np.cos(turn * (position[:, 0] * count % (2 * count)))
    table = np.concatenate([even_part, odd_part], axis=1)
    table[:, [0, count]] *= math.sqrt(0.5)
    return table


def half_table(count):
    place = np.arange(count)
    angle = np.pi * (place[:, None] * place[None, :] % (2 * count)) / count
    cosine, sine = np.cos(angle), np.sin(angle)
    cosine[np.abs(cosine) < 1e-12] = 0.0
    sine[np.abs(sine) < 1e-12] = 0.0
    return cosine, sine


def weighted(terms):
    total = None
    for weight, value in terms:
        weight = float(weight)
        if weight == 0.0:
            continue
        if total is None:
            total = value if weight == 1.0 else -value if weight == -1.0 else weight * value
        elif weight == 1.0:
            total = total + value
        elif weight == -1.0:
            total = total - value
        else:
            total = total + weight * value
    return total


def layers_to_spectrum(layers):
    count = len(layers)
    half = count // 2
    cosine, sine = half_table(count)
    sums = {z: layers[z] + layers[count - z] for z in range(1, half)}
    gaps = {z: layers[z] - layers[count - z] for z in range(1, half)}
    spectrum = []
    for k in range(count):
        near, far = (sums, gaps) if k % 2 == 0 else (gaps, sums)
        re = weighted(
            [(1.0, layers[0]), (cosine[half, k], layers[half])]
            + [(cosine[z, k], near[z]) for z in range(1, half)]
        )
        if k == 0:
            im = weighted(
                [(1.0, layers[0]), ((-1.0) ** half, layers[half])]
                + [((-1.0) ** z, near[z]) for z in range(1, half)]
            )
        else:
            im = weighted(
                [(-sine[half, k], layers[half])] + [(-sine[z, k], far[z]) for z in range(1, half)]
            )
        spectrum.append((re, im))
    return spectrum


def spectrum_to_layers(spectrum):
    count = len(spectrum)
    half = count // 2
    cosine, sine = half_table(count)
    layers = [None] * count
    evens, odds = range(2, count, 2), range(1, count, 2)
    ground = [spectrum[0][0] + spectrum[0][1], spectrum[0][0] - spectrum[0][1]]
    layers[0] = weighted([(1.0, ground[0])] + [(2.0, spectrum[k][0]) for k in range(1, count)])
    layers[half] = weighted(
        [(1.0, ground[half % 2])]
        + [(2.0 * cosine[half, k], spectrum[k][0]) for k in range(1, count)]
        + [(-2.0 * sine[half, k], spectrum[k][1]) for k in range(1, count)]
    )
    for z in range(1, half):
        even_re = weighted(
            [(1.0, ground[z % 2])] + [(2.0 * cosine[z, k], spectrum[k][0]) for k in evens]
        )
        odd_re = weighted([(2.0 * cosine[z, k], spectrum[k][0]) for k in odds])
        even_im = weighted([(2.0 * sine[z, k], spectrum[k][1]) for k in evens])
        odd_im = weighted([(2.0 * sine[z, k], spectrum[k][1]) for k in odds])
        layers[z] = (even_re - odd_im) + (odd_re - even_im)
        layers[count - z] = (even_re - odd_im) - (odd_re - even_im)
    return layers


def dot32(left, right):
    return jnp.dot(left, right, preferred_element_type=jnp.float32)


def three_limbs(values, axis):
    upper, lower = split_limbs(values)
    return jnp.concatenate([upper, lower, upper], axis=axis)


def tensor_part(c, spec_ref, kernel_refs, out_ref):
    rows_full, columns_full = out_ref.shape[2] // 2, out_ref.shape[3] // 2
    lane = 128
    sub = 16
    top = lax.broadcasted_iota(jnp.int32, (sub, lane), 0) == 0
    left = lax.broadcasted_iota(jnp.int32, (sub, lane), 1) == 0

    def tile(row_start, first_row, start):
        rows = pl.ds(row_start, sub)
        columns = slice(start, start + lane)
        edge_columns = slice(columns_full, columns_full + lane)
        first_column = start == 0

        def loaded(component, part=0):
            kernel_ref = kernel_refs[part]
            body = kernel_ref[component, rows, columns]
            side = kernel_ref[component, rows, edge_columns] if first_column else None
            if not first_row:
                return body, side, None, None
            far = pl.ds(rows_full, 1)
            body_far = kernel_ref[component, far, columns]
            side_far = kernel_ref[component, far, edge_columns] if first_column else None
            return body, side, body_far, side_far

        def pick(parts, odd_x, odd_y):
            body, side, body_far, side_far = parts
            mixed = jnp.where(left, side, body) if odd_y and first_column else body
            if odd_x and first_row:
                far = body_far
                if odd_y and first_column:
                    far = jnp.where(left[:1], side_far, far)
                mixed = jnp.where(top, far, mixed)
            return mixed

        own = [loaded(c, part) for part in range(2)]
        k_xy = [pick(loaded(3, part), 0, 0) if c < 2 else None for part in range(2)]
        k_xz = loaded(4) if c != 1 else None
        k_yz = loaded(5) if c != 0 else None

        def place(px, py):
            offset = py * columns_full + start
            return pl.ds(row_start + px * rows_full, sub), slice(offset, offset + lane)

        def spec(px, py, f):
            at_rows, at_columns = place(px, py)
            return spec_ref[f, at_rows, at_columns]

        for px in range(2):
            for py in range(2):
                own_here = [pick(own[part], px, py) for part in range(2)]
                xz_here = pick(k_xz, 0, py) if c != 1 else None
                yz_here = pick(k_yz, px, 0) if c != 0 else None
                for part in range(2):
                    turn = 1.0 if part else -1.0
                    sx = turn if px else -turn
                    sy = turn if py else -turn
                    other = 1 - part
                    total = own_here[part] * spec(px, py, 2 * c + part)
                    if c < 2:
                        across = k_xy[part] * spec(1 - px, 1 - py, 2 * (1 - c) + part)
                        total = total - across if px == py else total + across
                    if c == 0:
                        third = xz_here * spec(1 - px, py, 4 + other)
                        total = total + third if sx > 0 else total - third
                    elif c == 1:
                        third = yz_here * spec(px, 1 - py, 4 + other)
                        total = total + third if sy > 0 else total - third
                    else:
                        third = xz_here * spec(1 - px, py, other)
                        total = total + third if sx > 0 else total - third
                        third = yz_here * spec(px, 1 - py, 2 + other)
                        total = total + third if sy > 0 else total - third
                    upper, lower = split_limbs(total)
                    at_rows, at_columns = place(px, py)
                    out_ref[part, 0, at_rows, at_columns] = upper
                    out_ref[part, 1, at_rows, at_columns] = lower

    for start in range(0, columns_full, lane):
        tile(0, True, start)

    def step(i, carry):
        row_start = pl.multiple_of(i * sub, sub)
        for start in range(0, columns_full, lane):
            tile(row_start, False, start)
        return carry

    lax.fori_loop(1, rows_full // sub, step, 0)


def arc_angle(sine, cosine):
    size = jnp.abs(cosine)
    low, high = jnp.minimum(sine, size), jnp.maximum(sine, size)
    ratio = low / jnp.maximum(high, 1e-37)
    wide = ratio > 0.41421356
    ratio = jnp.where(wide, (ratio - 1.0) / (ratio + 1.0), ratio)
    square = ratio * ratio
    series = ((8.05374449538e-2 * square - 1.38776856032e-1) * square + 1.99777106478e-1) * square
    angle = (series - 3.33329491539e-1) * square * ratio + ratio
    angle = jnp.where(wide, angle + 0.25 * math.pi, angle)
    angle = jnp.where(sine > size, 0.5 * math.pi - angle, angle)
    return jnp.where(cosine < 0.0, math.pi - angle, angle)


def dot3(first, second):
    return first[0] * second[0] + first[1] * second[1] + first[2] * second[2]


def band_kernel(
    scale,
    magnet_ref,
    kernel_ref,
    anisotropy_ref,
    source_tables,
    force_ref,
    small_ref,
    tables,
    cells_ref,
    film_ref,
    edge_out_ref,
    edge_ref,
    send_ref,
    back_ref,
    held_ref,
    spec_ref,
    field_ref,
    arrive_ref,
    next_ref,
    prior_ref,
    rim_out_ref,
    rim_ref,
    present_ref,
    ease_ref,
    sums_ref,
    tile_ref,
    swap_ref,
    peak_ref,
    tensor_ref,
    result_ref,
    own_sem,
    tensor_sem,
    film_send,
    film_recv,
    swap_plane_send,
    swap_plane_recv,
    plane_send,
    plane_recv,
    back_send,
    back_recv,
    last_send,
    last_recv,
    image_send,
    image_recv,
    rim_send,
    rim_recv,
    swap_send,
    swap_recv,
    peak_send,
    peak_recv,
    force_sem,
    table_sem,
):
    fy_ref, fx_ref = tables[:2]
    gx_ref, gy_ref = tables[:2] if len(tables) == 2 else tables[2:]
    groups, local_planes = held_ref.shape[1], held_ref.shape[2]
    slab, columns_full = held_ref.shape[4], held_ref.shape[5]
    layer_count = cells_ref.shape[2]
    rows_full = groups * slab
    parts = groups // 2
    me = lax.axis_index("space")
    half, seat = me // parts, lax.rem(me, parts)
    partner = lax.rem(me + parts, groups)
    flip = (1 - 2 * half).astype(jnp.float32)
    row_step = 8
    images, image = lax.axis_size("image"), lax.axis_index("image")
    first, last = image == 0, image == images - 1
    shifts = (-1, 0, 1)
    routes = [
        (n, shift, d)
        for n, shift in enumerate(shifts)
        for d in range(groups)
        if shift != 0 or d != 0
    ]

    def gate(exists, action):
        if exists is None:
            action()
        else:
            pl.when(exists)(action)

    def receiver(shift):
        return None if shift == 0 else jnp.logical_not(last if shift < 0 else first)

    def sender(shift):
        return None if shift == 0 else jnp.logical_not(first if shift < 0 else last)

    def target_of(shift, d):
        return {"image": lax.rem(image - shift + images, images), "space": lax.rem(me + d, groups)}

    def remote(src, dst, send, recv, target):
        return pltpu.make_async_remote_copy(
            src_ref=src,
            dst_ref=dst,
            send_sem=send,
            recv_sem=recv,
            device_id=target if isinstance(target, dict) else {"space": target},
            device_id_type=pl.DeviceIdType.MESH,
        )

    def row_loop(step):
        def chunk(i, carry):
            step(pl.ds(pl.multiple_of(i * row_step, row_step), row_step))
            return carry

        lax.fori_loop(0, slab // row_step, chunk, 0)

    def own_copy(c):
        return pltpu.make_async_copy(magnet_ref.at[:, c], cells_ref.at[:, c], own_sem.at[c])

    def tensor_copy(q):
        return pltpu.make_async_copy(
            kernel_ref.at[:, q, pl.ds(0, rows_full + 8), pl.ds(0, columns_full + 128)],
            tensor_ref.at[pl.ds(6 * q, 6)],
            tensor_sem.at[q],
        )

    def film_copy(c):
        return remote(
            magnet_ref.at[1 - half, c], film_ref.at[c], film_send.at[c], film_recv.at[c], partner
        )

    def kernel_copies():
        body = (pl.ds(0, rows_full), pl.ds(0, columns_full))
        far = (pl.ds(rows_full, 8), pl.ds(0, columns_full + 128))
        pieces = [
            (kernel_ref.at[pl.ds(0, 4), 0, *body], tensor_ref.at[pl.ds(6 * local_planes, 4), *body]),
            (kernel_ref.at[pl.ds(0, 3), 0, *far], tensor_ref.at[pl.ds(6 * local_planes, 3), *far]),
            (edge_out_ref, edge_ref),
        ]
        return [
            remote(src, dst, swap_plane_send.at[n], swap_plane_recv.at[n], partner)
            for n, (src, dst) in enumerate(pieces)
        ]

    def pack_edges():
        lane_pos = lax.broadcasted_iota(jnp.int32, (row_step, 128), 1)
        columns = pl.ds(columns_full, 128)

        def step(i, carry):
            rows = pl.ds(pl.multiple_of(i * row_step, row_step), row_step)
            edges = [tensor_ref[c, rows, columns] for c in range(3)]
            edge = jnp.where(lane_pos == 1, pltpu.roll(edges[1], 1, 1), edges[0])
            edge_out_ref[rows, :] = jnp.where(lane_pos == 2, pltpu.roll(edges[2], 2, 1), edge)
            return carry

        lax.fori_loop(0, rows_full // row_step, step, 0)

    def unpack_edges():
        columns = pl.ds(columns_full, 128)

        def step(i, carry):
            rows = pl.ds(pl.multiple_of(i * row_step, row_step), row_step)
            edge = edge_ref[rows, :]
            for c in range(3):
                tensor_ref[6 * local_planes + c, rows, columns] = (
                    pltpu.roll(edge, 128 - c, 1) if c else edge
                )
            return carry

        lax.fori_loop(0, rows_full // row_step, step, 0)

    def place_of(seat_index, kind):
        return lax.rem((half + kind) * parts + seat_index, groups)

    def plane_copy(c, kind, slot):
        target = lax.rem(seat + 1 + slot, parts)
        return remote(
            send_ref.at[c, kind, slot],
            held_ref.at[c, place_of(seat, kind)],
            plane_send.at[c, kind, slot],
            plane_recv.at[c, kind, parts - 2 - slot],
            half * parts + target,
        )

    def plane_arrival(c, kind, slot):
        source = lax.rem(seat + 1 + slot, parts)
        return remote(
            send_ref.at[c, kind, slot],
            held_ref.at[c, place_of(source, kind)],
            plane_send.at[c, kind, slot],
            plane_recv.at[c, kind, slot],
            half * parts + source,
        )

    def back_copy(c, q, kind, slot):
        target = lax.rem(seat + 1 + slot, parts)
        return remote(
            held_ref.at[c, place_of(target, kind), q],
            back_ref.at[c, kind, parts - 2 - slot, q],
            back_send.at[c, q, kind, slot],
            back_recv.at[c, q, kind, parts - 2 - slot],
            half * parts + target,
        )

    def back_arrival(c, q, kind, slot):
        source = lax.rem(seat + 1 + slot, parts)
        return remote(
            held_ref.at[c, place_of(source, kind), q],
            back_ref.at[c, kind, slot, q],
            back_send.at[c, q, kind, slot],
            back_recv.at[c, q, kind, slot],
            half * parts + source,
        )

    def last_copy(c):
        return remote(
            film_ref.at[c], arrive_ref.at[c], last_send.at[c], last_recv.at[c], partner
        )

    def ahead_copy():
        return remote(
            magnet_ref.at[1],
            prior_ref,
            image_send.at[0],
            image_recv.at[0],
            {"image": lax.rem(image + 1, images)},
        )

    def behind_copy():
        return remote(
            magnet_ref.at[0],
            next_ref,
            image_send.at[1],
            image_recv.at[1],
            {"image": lax.rem(image + images - 1, images)},
        )

    def rim_copy(side):
        return remote(
            rim_out_ref.at[side],
            rim_ref.at[side],
            rim_send.at[side],
            rim_recv.at[side],
            lax.rem(me + (1 if side == 0 else groups - 1), groups),
        )

    def swap_copy(n, shift, d, slot):
        return remote(
            tile_ref, swap_ref.at[n, slot], swap_send.at[n, d], swap_recv.at[n, d], target_of(shift, d)
        )

    def peak_copy(d, slot):
        return remote(
            tile_ref.at[pl.ds(0, 8)],
            peak_ref.at[slot],
            peak_send.at[d],
            peak_recv.at[d],
            lax.rem(me + d, groups),
        )

    def table_copy(n):
        return pltpu.make_async_copy(source_tables[n], tables[n], table_sem.at[n])

    def force_copy(i):
        return pltpu.make_async_copy(field_ref.at[i], force_ref.at[i], force_sem.at[i])

    def transform_layers(c, kind):
        place = place_of(seat, kind)

        def variant(here):
            def step(rows):
                if kind == 0:
                    layers = [cells_ref[half, c, z, rows, :] for z in range(layer_count)]
                else:
                    layers = [film_ref[c, z, rows, :] for z in range(layer_count)]
                layers = [v * flip if z % 2 else v for z, v in enumerate(layers)]
                spectrum = layers_to_spectrum(layers)
                for k in range(layer_count):
                    target, q = k // local_planes, k % local_planes
                    slot = (target - here) % parts - 1
                    for part in range(2):
                        if target == here:
                            held_ref[c, place, q, part, rows, :] = spectrum[k][part]
                        else:
                            send_ref[c, kind, slot, q, part, rows, :] = spectrum[k][part]

            row_loop(step)

        for here in range(parts):
            pl.when(seat == here)(functools.partial(variant, here))
        for slot in range(parts - 1):
            plane_copy(c, kind, slot).start()

    def transform_planes(c, kind):
        place = place_of(seat, kind)

        def variant(here):
            def step(rows):
                spectrum = []
                for k in range(layer_count):
                    source, q = k // local_planes, k % local_planes
                    slot = (source - here) % parts - 1
                    if source == here:
                        spectrum.append(
                            [held_ref[c, place, q, part, rows, :] for part in range(2)]
                        )
                    else:
                        spectrum.append(
                            [back_ref[c, kind, slot, q, part, rows, :] for part in range(2)]
                        )
                for z, value in enumerate(spectrum_to_layers(spectrum)):
                    value = value * (scale * flip if z % 2 else scale)
                    if kind == 0:
                        field_ref[half, c, z, rows, :] = field_ref[half, c, z, rows, :] + value
                    else:
                        film_ref[c, z, rows, :] = value

            row_loop(step)

        for here in range(parts):
            pl.when(seat == here)(functools.partial(variant, here))

    def fill_rims():
        def step(f, carry):
            i, c = f // 3, lax.rem(f, 3)
            for side in range(2):
                row = slab - 1 if side == 0 else 0
                rim_out_ref[side, i, c] = jnp.concatenate(
                    [cells_ref[i, c, z, row : row + 1, :] for z in range(layer_count)], axis=0
                )
            return carry

        lax.fori_loop(0, 6, step, 0)
        row_pos = lax.broadcasted_iota(jnp.int32, (slab, columns_full), 0) + me * slab
        column_pos = lax.broadcasted_iota(jnp.int32, (slab, columns_full), 1)
        faces = [row_pos == 0, row_pos == rows_full - 1]
        faces += [column_pos == 0, column_pos == columns_full - 1]
        present_ref[...] = 6.0 - sum(jnp.where(face, 1.0, 0.0) for face in faces)
        for side in range(2):
            open_side = me != groups - 1 if side == 0 else me != 0

            @pl.when(open_side)
            def _():
                rim_copy(side).start()

            no_source = me == 0 if side == 0 else me == groups - 1

            @pl.when(no_source)
            def _():
                rim_ref[side] = jnp.zeros(rim_ref.shape[1:], jnp.float32)

    def wait_rims():
        for side in range(2):
            has_source = me != 0 if side == 0 else me != groups - 1

            @pl.when(has_source)
            def _():
                rim_copy(side).wait_recv()

    def local_fields(i):
        row_pos = lax.broadcasted_iota(jnp.int32, (slab, columns_full), 0)
        column_pos = lax.broadcasted_iota(jnp.int32, (slab, columns_full), 1)

        def step(z, carry):
            below, above = jnp.maximum(z - 1, 0), jnp.minimum(z + 1, layer_count - 1)
            has_below = (z > 0).astype(jnp.float32)
            has_above = (z < layer_count - 1).astype(jnp.float32)
            present = present_ref[...] - (2.0 - has_below - has_above)
            tilt = []
            for c in range(3):
                cells = cells_ref[i, c, z]
                x_plus = jnp.where(
                    row_pos == slab - 1,
                    rim_ref[1, i, c, pl.ds(z, 1), :],
                    pltpu.roll(cells, slab - 1, 0),
                )
                x_minus = jnp.where(
                    row_pos == 0, rim_ref[0, i, c, pl.ds(z, 1), :], pltpu.roll(cells, 1, 0)
                )
                y_plus = jnp.where(
                    column_pos == columns_full - 1, 0.0, pltpu.roll(cells, columns_full - 1, 1)
                )
                y_minus = jnp.where(column_pos == 0, 0.0, pltpu.roll(cells, 1, 1))
                around = x_plus + x_minus + y_plus + y_minus
                around = around + has_above * cells_ref[i, c, above] + has_below * cells_ref[i, c, below]
                part = exchange_strength * (around - present * cells)
                if c == 0:
                    tilt.append(x_plus - x_minus)
                    field_ref[i, 0, z] = part
                elif c == 1:
                    tilt.append(y_plus - y_minus)
                    field_ref[i, 1, z] = part
                else:
                    ease = ease_ref[...] * cells
                    field_ref[i, 2, z] = part + (ease - chiral_strength * (tilt[0] + tilt[1]))
                    field_ref[i, 0, z] = field_ref[i, 0, z] + chiral_strength * (x_plus - x_minus)
                    field_ref[i, 1, z] = field_ref[i, 1, z] + chiral_strength * (y_plus - y_minus)
            return carry

        lax.fori_loop(0, layer_count, step, 0)

    lane = columns_full

    def cell_loop(step, carry):
        unrolled = min(4, slab // row_step)
        steps = slab // (unrolled * row_step)

        def chunk(index, carry):
            z = index // steps
            start = lax.rem(index, steps) * unrolled * row_step
            for n in range(unrolled):
                carry = step(z, pl.multiple_of(start + n * row_step, row_step), carry)
            return carry

        return lax.fori_loop(0, layer_count * steps, chunk, carry)

    def zeros(count):
        return tuple(jnp.zeros((row_step, lane), jnp.float32) for _ in range(count))

    def tangent_rows(z, start):
        return pl.ds(pl.multiple_of(z * slab + start, row_step), row_step)

    def neighbour_sums():
        @pl.when(jnp.logical_not(first))
        def _():
            ahead_copy().wait_recv()

        @pl.when(first)
        def _():
            for c in range(3):
                prior_ref[c] = cells_ref[0, c]

        @pl.when(jnp.logical_not(last))
        def _():
            behind_copy().wait_recv()

        @pl.when(last)
        def _():
            for c in range(3):
                next_ref[c] = cells_ref[1, c]

        for i in range(2):

            def step(z, start, carry):
                rows = pl.ds(start, row_step)
                here = [cells_ref[i, c, z, rows, :] for c in range(3)]
                if i == 0:
                    ahead = [cells_ref[1, c, z, rows, :] for c in range(3)]
                    behind = [prior_ref[c, z, rows, :] for c in range(3)]
                else:
                    ahead = [next_ref[c, z, rows, :] for c in range(3)]
                    behind = [cells_ref[0, c, z, rows, :] for c in range(3)]
                normal = [
                    here[1] * ahead[2] - here[2] * ahead[1],
                    here[2] * ahead[0] - here[0] * ahead[2],
                    here[0] * ahead[1] - here[1] * ahead[0],
                ]
                angle = arc_angle(jnp.sqrt(dot3(normal, normal)), dot3(here, ahead))
                ahead = [ahead[c] - here[c] for c in range(3)]
                behind = [here[c] - behind[c] for c in range(3)]
                ahead_on, behind_on = dot3(ahead, here), dot3(behind, here)
                ahead = [ahead[c] - ahead_on * here[c] for c in range(3)]
                behind = [behind[c] - behind_on * here[c] for c in range(3)]
                for c in range(3):
                    place = tangent_rows(z, start)
                    spec_ref[0, 3 * i + c, place, 0:columns_full] = ahead[c]
                    spec_ref[0, 3 * i + c, place, columns_full : 2 * columns_full] = behind[c]
                values = (
                    angle * angle,
                    dot3(ahead, ahead),
                    dot3(ahead, behind),
                    dot3(behind, behind),
                )
                return tuple(total + value for total, value in zip(carry, values))

            totals = cell_loop(step, zeros(4))
            for k in range(4):
                sums_ref[i, k + 1] = totals[k]

    def field_sums(i, c, arrived):
        def step(z, start, carry):
            rows = pl.ds(start, row_step)
            place = tangent_rows(z, start)
            field = field_ref[i, c, z, rows, :]
            if arrived:
                field = field + arrive_ref[c, z, rows, :]
                field_ref[i, c, z, rows, :] = field
            values = (
                cells_ref[i, c, z, rows, :] * field,
                field * spec_ref[0, 3 * i + c, place, 0:columns_full],
                field * spec_ref[0, 3 * i + c, place, columns_full : 2 * columns_full],
            )
            return tuple(total + value for total, value in zip(carry, values))

        totals = cell_loop(step, zeros(3))
        for k, slot in enumerate((0, 5, 6)):
            sums_ref[i, slot] = totals[k] if c == 0 else sums_ref[i, slot] + totals[k]

    barrier = pltpu.get_barrier_semaphore()
    for n, shift, d in routes:
        signal = functools.partial(
            pl.semaphore_signal,
            barrier,
            inc=1,
            device_id=target_of(shift, d),
            device_id_type=pl.DeviceIdType.MESH,
        )
        gate(receiver(shift), signal)
    for c in range(3):
        own_copy(c).start()
    for n in range(len(tables)):
        table_copy(n).start()

    def spread(r, carry):
        ease_ref[pl.ds(r, 1), :] = jnp.full((1, columns_full), 2.0 * anisotropy_ref[r])
        return carry

    lax.fori_loop(0, slab, spread, 0)
    ends = first.astype(jnp.int32) + last.astype(jnp.int32)
    pl.semaphore_wait(barrier, len(routes) - groups * ends)
    film_copy(0).start()

    @pl.when(jnp.logical_not(last))
    def _():
        ahead_copy().start()

    @pl.when(jnp.logical_not(first))
    def _():
        behind_copy().start()

    for c in range(3):
        own_copy(c).wait()
    fill_rims()
    for c in range(1, 3):
        film_copy(c).start()

    @pl.when(seat == 0)
    def _():
        for copy in kernel_copies()[:2]:
            copy.start()

    for q in range(local_planes):
        tensor_copy(q).start()

    for c in range(3):
        transform_layers(c, 0)
    for n in range(len(tables)):
        table_copy(n).wait()
    tensor_copy(0).wait()

    @pl.when(seat == 0)
    def _():
        pack_edges()
        kernel_copies()[2].start()

    for c in range(3):
        film_copy(c).wait_recv()
        transform_layers(c, 1)
        for kind in range(2):
            for slot in range(parts - 1):
                plane_arrival(c, kind, slot).wait_recv()

        def forward(i, carry):
            q = i
            fy = jnp.concatenate([fy_ref[0], fy_ref[0], fy_ref[1]], axis=0)
            fx = jnp.concatenate([fx_ref[0], fx_ref[0], fx_ref[1]], axis=1)
            cells = jnp.concatenate(
                [held_ref[c, g, q, part] for part in range(2) for g in range(groups)], axis=0
            )
            lines = dot32(three_limbs(cells, 1), fy)
            for part in range(2):
                spec_ref[q, 2 * c + part] = dot32(
                    fx, three_limbs(lines[part * rows_full : (part + 1) * rows_full], 0)
                )
            return carry

        lax.fori_loop(0, local_planes, forward, 0)
        if c == 0:
            wait_rims()
        if c < 2:
            local_fields(c)

    for q in range(1, local_planes):
        tensor_copy(q).wait()

    for c in range(3):

        def backward(i, carry):
            q = local_planes - 1 - i
            twin = (seat == 0) & (q == 0)
            if c == 0:

                @pl.when(twin)
                def _():
                    for copy in kernel_copies():
                        copy.wait_recv()
                    unpack_edges()

            second = jnp.where(twin, local_planes, q)
            kernels = (tensor_ref.at[pl.ds(6 * q, 6)], tensor_ref.at[pl.ds(6 * second, 4)])
            tensor_part(c, spec_ref.at[q], kernels, result_ref)
            gx = jnp.concatenate([gx_ref[0], gx_ref[0], gx_ref[1]], axis=1)
            gy = jnp.concatenate([gy_ref[0], gy_ref[0], gy_ref[1]], axis=0)
            for part in range(2):
                upper, lower = result_ref[part, 0], result_ref[part, 1]
                lines = dot32(gx, jnp.concatenate([upper, lower, upper], axis=0))
                cells = dot32(three_limbs(lines, 1), gy)
                for g in range(groups):
                    held_ref[c, g, q, part] = cells[g * slab : (g + 1) * slab]
            for kind in (1, 0):
                for slot in range(parts - 1):
                    back_copy(c, q, kind, slot).start()

            return carry

        lax.fori_loop(0, local_planes, backward, 0)
        for kind in (1, 0):
            for q in range(local_planes):
                for slot in range(parts - 1):
                    back_arrival(c, q, kind, slot).wait_recv()
            transform_planes(c, kind)
            if kind == 1:
                last_copy(c).start()

    neighbour_sums()
    for c in range(3):
        field_sums(half, c, False)
    for c in range(3):
        last_copy(c).wait_recv()
        field_sums(1 - half, c, True)

    rows = [
        jnp.sum(sums_ref[i, k], axis=0, keepdims=True) for i in range(2) for k in range(7)
    ] + [jnp.zeros((1, lane), jnp.float32)] * 2
    tile = jnp.sum(jnp.concatenate(rows, axis=0), axis=1, keepdims=True)
    tile_ref[...] = jnp.broadcast_to(tile, tile_ref.shape)
    for n, shift, d in routes:
        gate(receiver(shift), swap_copy(n, shift, d, me).start)
    swap_ref[1, me] = tile_ref[...]
    for n, end in ((0, first), (2, last)):

        @pl.when(end)
        def _():
            swap_ref[n] = jnp.zeros(swap_ref.shape[1:], jnp.float32)

    for n, shift, d in routes:
        gate(sender(shift), swap_copy(n, shift, d, lax.rem(me + groups - d, groups)).wait_recv)
    totals = []
    for n in range(3):
        total = swap_ref[n, 0]
        for g in range(1, groups):
            total = total + swap_ref[n, g]
        totals.append(total)

    def entry(n, i, k):
        return totals[n][7 * i + k : 7 * i + k + 1]

    cell_count = float(layer_count * rows_full * columns_full)
    energies = [-0.5 * entry(*at, 0) for at in ((0, 1), (1, 0), (1, 1), (2, 0))]
    distances = [jnp.sqrt(entry(*at, 1) / cell_count) for at in ((0, 1), (1, 0), (1, 1))]
    pulls = []
    for i in range(2):
        weight_next, weight_prior = tangent_weights(energies[i + 1], energies[i + 2], energies[i])
        length_square = (
            weight_next * weight_next * entry(1, i, 2)
            + 2.0 * weight_next * weight_prior * entry(1, i, 3)
            + weight_prior * weight_prior * entry(1, i, 4)
        )
        drive = weight_next * entry(1, i, 5) + weight_prior * entry(1, i, 6)
        size = jnp.sqrt(jnp.maximum(length_square, 0.0) / cell_count + epsilon)
        spring = spring_strength * (distances[i + 1] - distances[i])
        pull = (spring - drive / (cell_count * size)) / size
        pulls.append((pull * weight_next, pull * weight_prior))
    for n, shift, d in routes:
        gate(receiver(shift), swap_copy(n, shift, d, me).wait_send)
    peaks = []
    for i in range(2):
        end = first if i == 0 else last
        ahead_pull, behind_pull = [
            jnp.concatenate([jnp.broadcast_to(pull, (row_step, 128))] * (lane // 128), axis=1)
            for pull in pulls[i]
        ]

        def step(z, start, peak):
            rows = pl.ds(start, row_step)
            place = tangent_rows(z, start)
            here = [cells_ref[i, c, z, rows, :] for c in range(3)]
            force = []
            for c in range(3):
                ahead = spec_ref[0, 3 * i + c, place, 0:columns_full]
                behind = spec_ref[0, 3 * i + c, place, columns_full : 2 * columns_full]
                field = field_ref[i, c, z, rows, :]
                force.append(field + ahead_pull * ahead + behind_pull * behind)
            along = dot3(force, here)
            force = [jnp.where(end, 0.0, force[c] - along * here[c]) for c in range(3)]
            for c in range(3):
                field_ref[i, c, z, rows, :] = force[c]
            return (jnp.maximum(peak[0], dot3(force, force)),)

        (peak,) = cell_loop(step, zeros(1))
        peaks.append(jnp.max(peak, axis=0, keepdims=True))
        force_copy(i).start()
    peak = jnp.concatenate(peaks + [jnp.zeros((6, lane), jnp.float32)], axis=0)
    peak = jnp.broadcast_to(jnp.max(peak, axis=1, keepdims=True), (8, 128))
    tile_ref[0:8] = peak
    for d in range(1, groups):
        peak_copy(d, me).start()
    peak_ref[me] = peak
    for d in range(1, groups):
        peak_copy(d, lax.rem(me + groups - d, groups)).wait_recv()
    largest = peak_ref[0]
    for g in range(1, groups):
        largest = jnp.maximum(largest, peak_ref[g])
    moves = jnp.minimum(step_limit, rotation_limit / (jnp.sqrt(largest) + epsilon))
    energy = jnp.concatenate(energies[1:3], axis=0) / cell_count
    small_ref[...] = jnp.concatenate([moves[0:2], energy, jnp.zeros((4, 128), jnp.float32)], axis=0)
    for i in range(2):
        force_copy(i).wait()
    for d in range(1, groups):
        peak_copy(d, me).wait_send()
    for c in range(3):
        film_copy(c).wait_send()
        last_copy(c).wait_send()
        for kind in range(2):
            for slot in range(parts - 1):
                plane_copy(c, kind, slot).wait_send()
                for q in range(local_planes):
                    back_copy(c, q, kind, slot).wait_send()

    @pl.when(seat == 0)
    def _():
        for copy in kernel_copies():
            copy.wait_send()

    for side in range(2):
        open_side = me != groups - 1 if side == 0 else me != 0

        @pl.when(open_side)
        def _():
            rim_copy(side).wait_send()

    @pl.when(jnp.logical_not(last))
    def _():
        ahead_copy().wait_send()

    @pl.when(jnp.logical_not(first))
    def _():
        behind_copy().wait_send()


def band_step(magnet, anisotropy, kernel):
    layer_count, row_count, column_count = magnet.shape[2:]
    groups = lax.axis_size("space")
    local_planes = 2 * layer_count // groups
    full_rows = row_count * groups
    slots = groups // 2 - 1
    table_y = parity_table(column_count)
    table_x = parity_table(full_rows)
    square = full_rows == column_count
    tables = [table_limbs(t) for t in (table_y, table_x.T, table_x, table_y.T)][: 2 if square else 4]

    def entry(magnet_ref, kernel_ref, anisotropy_ref, *refs):
        count = len(tables)
        sources, outs = refs[:count], refs[count : count + 2]
        held, rest = refs[count + 2 : 2 * count + 2], refs[2 * count + 2 :]
        scale = -4.0 / padded_cells
        band_kernel(
            scale, magnet_ref, kernel_ref, anisotropy_ref, sources, *outs, held, *rest
        )

    slab = (row_count, column_count)
    film = (layer_count,) + slab
    block = (local_planes, 2) + slab
    anywhere = pl.BlockSpec(memory_space=pl.ANY)
    inside = pl.BlockSpec(memory_space=pltpu.VMEM)
    dots = 6 * local_planes * 4 * full_rows * column_count * 3 * (full_rows + column_count // 2)
    padded_cells = 8 * layer_count * full_rows * column_count
    signals = pltpu.SemaphoreType.DMA
    scratch = [
        (2, 3) + film,
        (3,) + film,
        (full_rows, 128),
        (full_rows, 128),
        (3, 2, slots) + block,
        (3, 2, slots) + block,
        (3, groups) + block,
        (local_planes, 6, 2 * full_rows, 2 * column_count),
        (2, 3) + film,
        (3,) + film,
        (3,) + film,
        (3,) + film,
        (2, 2, 3, layer_count, column_count),
        (2, 2, 3, layer_count, column_count),
        slab,
        slab,
        (2, 7, 8, column_count),
        (16, 128),
        (3, groups, 16, 128),
        (groups, 8, 128),
        (6 * local_planes + 4, full_rows + 8, column_count + 128),
    ]
    semaphores = [
        (3,),
        (local_planes,),
        (3,),
        (3,),
        (3,),
        (3,),
        (3, 2, slots),
        (3, 2, slots),
        (3, local_planes, 2, slots),
        (3, local_planes, 2, slots),
        (3,),
        (3,),
        (2,),
        (2,),
        (2,),
        (2,),
        (3, groups),
        (3, groups),
        (groups,),
        (groups,),
        (2,),
        (len(tables),),
    ]
    return pl.pallas_call(
        entry,
        in_specs=[anywhere, anywhere, pl.BlockSpec(memory_space=pltpu.SMEM)]
        + [anywhere] * len(tables),
        out_specs=[anywhere, inside],
        out_shape=[
            jax.ShapeDtypeStruct(magnet.shape, jnp.float32),
            jax.ShapeDtypeStruct((8, 128), jnp.float32),
        ],
        scratch_shapes=[pltpu.VMEM(t.shape, jnp.bfloat16) for t in tables]
        + [pltpu.VMEM(dims, jnp.float32) for dims in scratch]
        + [pltpu.VMEM((2, 2, 2 * full_rows, 2 * column_count), jnp.bfloat16)]
        + [signals(dims) for dims in semaphores],
        compiler_params=pltpu.CompilerParams(
            vmem_limit_bytes=67043328, collective_id=0, has_side_effects=True
        ),
        cost_estimate=pl.CostEstimate(
            flops=4 * dots, bytes_accessed=4 * magnet.size * 4, transcendentals=0
        ),
        name="band_kernel",
    )(magnet, kernel, anisotropy, *[jnp.asarray(t) for t in tables])


def move_kernel(small_ref, magnet_ref, force_ref, updated_ref, out_ref, energy_ref):
    i = pl.program_id(0)
    layers, slab, columns = magnet_ref.shape[2:]

    @pl.when((i == 0) & (pl.program_id(1) == 0))
    def _():
        for n in range(2):
            energy_ref[n] = jnp.max(small_ref[n + 2 : n + 3, :])

    row_step = 8
    move = jnp.broadcast_to(small_ref[pl.ds(i, 1), :], (row_step, 128))
    move = jnp.concatenate([move] * (columns // 128), axis=1)
    unrolled = min(4, slab // row_step)

    def chunk(index, carry):
        for z in range(layers):
            for n in range(unrolled):
                start = (index * unrolled + n) * row_step
                rows = pl.ds(pl.multiple_of(start, row_step), row_step)
                force = [force_ref[0, c, z, rows, :] for c in range(3)]
                moved = [magnet_ref[0, c, z, rows, :] + move * force[c] for c in range(3)]
                inverse = lax.rsqrt(dot3(moved, moved))
                for c in range(3):
                    updated_ref[0, c, z, rows, :] = inverse * moved[c]
                    out_ref[0, c, z, rows, :] = force[c]
        return carry

    lax.fori_loop(0, slab // (unrolled * row_step), chunk, 0)


def move_images(magnet, force, small):
    images, _, layer_count, row_count, column_count = magnet.shape
    layers = max(1, layer_count // 4)
    block = pl.BlockSpec(
        (1, 3, layers, row_count, column_count), lambda i, k: (i, 0, k, 0, 0)
    )
    return pl.pallas_call(
        move_kernel,
        grid=(images, layer_count // layers),
        in_specs=[pl.BlockSpec((8, 128), lambda i, k: (0, 0)), block, block],
        out_specs=[block, block, pl.BlockSpec(memory_space=pltpu.SMEM)],
        out_shape=[
            jax.ShapeDtypeStruct(magnet.shape, jnp.float32),
            jax.ShapeDtypeStruct(magnet.shape, jnp.float32),
            jax.ShapeDtypeStruct((images,), jnp.float32),
        ],
        name="move_kernel",
    )(small, magnet, force)


def body(magnet, anisotropy, kernel):
    force, small = band_step(magnet, anisotropy, kernel)
    return move_images(magnet, force, small)


def solution(mesh):
    in_specs = (P("image", None, None, "space", None), P("space"), P(None, "space", None, None))
    out_specs = (
        P("image", None, None, "space", None),
        P("image", None, None, "space", None),
        P("image"),
    )
    return jax.shard_map(body, mesh=mesh, in_specs=in_specs, out_specs=out_specs, check_vma=False)
```

```python
import functools
import math

import jax
import jax.numpy as jnp
import numpy as np
from jax import lax
from jax.experimental import pallas as pl
from jax.experimental.pallas import tpu as pltpu
from jax.sharding import PartitionSpec as P

exchange_strength = 0.25
chiral_strength = 0.3
spring_strength = 10.0
step_limit = 1.0
rotation_limit = 0.5
epsilon = 1e-06


def tangent_weights(energy_total, energy_next, energy_prior):
    rise_next = energy_next - energy_total
    rise_prior = energy_total - energy_prior
    upward = (rise_next > 0) & (rise_prior > 0)
    downward = (rise_next < 0) & (rise_prior < 0)
    larger = jnp.maximum(jnp.abs(rise_next), jnp.abs(rise_prior))
    smaller = jnp.minimum(jnp.abs(rise_next), jnp.abs(rise_prior))
    toward_next = energy_next > energy_prior
    weight_next = jnp.where(
        upward, 1.0, jnp.where(downward, 0.0, jnp.where(toward_next, larger, smaller))
    )
    weight_prior = jnp.where(
        upward, 0.0, jnp.where(downward, 1.0, jnp.where(toward_next, smaller, larger))
    )
    return (weight_next, weight_prior)


def split_limbs(values):
    upper = values.astype(jnp.bfloat16)
    return upper, (values - upper.astype(jnp.float32)).astype(jnp.bfloat16)


def table_limbs(table):
    upper = table.astype(np.float32).astype(jnp.bfloat16)
    lower = (table - upper.astype(np.float64)).astype(np.float32).astype(jnp.bfloat16)
    return np.stack([upper, lower])


def parity_table(count):
    position = np.arange(count)[:, None]
    slot = np.arange(count)[None, :]
    turn = np.pi / count
    even_part = np.cos(turn * (position * slot % (2 * count)))
    odd_part = np.sin(turn * (position * slot % (2 * count)))
    odd_part[:, 0] = np.cos(turn * (position[:, 0] * count % (2 * count)))
    table = np.concatenate([even_part, odd_part], axis=1)
    table[:, [0, count]] *= math.sqrt(0.5)
    return table


def half_table(count):
    place = np.arange(count)
    angle = np.pi * (place[:, None] * place[None, :] % (2 * count)) / count
    cosine, sine = np.cos(angle), np.sin(angle)
    cosine[np.abs(cosine) < 1e-12] = 0.0
    sine[np.abs(sine) < 1e-12] = 0.0
    return cosine, sine


def weighted(terms):
    total = None
    for weight, value in terms:
        weight = float(weight)
        if weight == 0.0:
            continue
        if total is None:
            total = value if weight == 1.0 else -value if weight == -1.0 else weight * value
        elif weight == 1.0:
            total = total + value
        elif weight == -1.0:
            total = total - value
        else:
            total = total + weight * value
    return total


def layers_to_spectrum(layers):
    count = len(layers)
    half = count // 2
    cosine, sine = half_table(count)
    sums = {z: layers[z] + layers[count - z] for z in range(1, half)}
    gaps = {z: layers[z] - layers[count - z] for z in range(1, half)}
    spectrum = []
    for k in range(count):
        near, far = (sums, gaps) if k % 2 == 0 else (gaps, sums)
        re = weighted(
            [(1.0, layers[0]), (cosine[half, k], layers[half])]
            + [(cosine[z, k], near[z]) for z in range(1, half)]
        )
        if k == 0:
            im = weighted(
                [(1.0, layers[0]), ((-1.0) ** half, layers[half])]
                + [((-1.0) ** z, near[z]) for z in range(1, half)]
            )
        else:
            im = weighted(
                [(-sine[half, k], layers[half])] + [(-sine[z, k], far[z]) for z in range(1, half)]
            )
        spectrum.append((re, im))
    return spectrum


def spectrum_to_layers(spectrum):
    count = len(spectrum)
    half = count // 2
    cosine, sine = half_table(count)
    layers = [None] * count
    evens, odds = range(2, count, 2), range(1, count, 2)
    ground = [spectrum[0][0] + spectrum[0][1], spectrum[0][0] - spectrum[0][1]]
    layers[0] = weighted([(1.0, ground[0])] + [(2.0, spectrum[k][0]) for k in range(1, count)])
    layers[half] = weighted(
        [(1.0, ground[half % 2])]
        + [(2.0 * cosine[half, k], spectrum[k][0]) for k in range(1, count)]
        + [(-2.0 * sine[half, k], spectrum[k][1]) for k in range(1, count)]
    )
    for z in range(1, half):
        even_re = weighted(
            [(1.0, ground[z % 2])] + [(2.0 * cosine[z, k], spectrum[k][0]) for k in evens]
        )
        odd_re = weighted([(2.0 * cosine[z, k], spectrum[k][0]) for k in odds])
        even_im = weighted([(2.0 * sine[z, k], spectrum[k][1]) for k in evens])
        odd_im = weighted([(2.0 * sine[z, k], spectrum[k][1]) for k in odds])
        layers[z] = (even_re - odd_im) + (odd_re - even_im)
        layers[count - z] = (even_re - odd_im) - (odd_re - even_im)
    return layers


def dot32(left, right):
    return jnp.dot(left, right, preferred_element_type=jnp.float32)


def three_limbs(values, axis):
    upper, lower = split_limbs(values)
    return jnp.concatenate([upper, lower, upper], axis=axis)


def tensor_part(c, spec_ref, kernel_refs, out_ref):
    rows_full, columns_full = out_ref.shape[1] // 2, out_ref.shape[2] // 2
    lane = 128
    sub = 8
    top = lax.broadcasted_iota(jnp.int32, (sub, lane), 0) == 0
    left = lax.broadcasted_iota(jnp.int32, (sub, lane), 1) == 0

    def tile(row_start, first_row, start):
        rows = pl.ds(row_start, sub)
        columns = slice(start, start + lane)
        edge_columns = slice(columns_full, columns_full + lane)
        first_column = start == 0

        def loaded(component, part=0):
            kernel_ref = kernel_refs[part]
            body = kernel_ref[component, rows, columns]
            side = kernel_ref[component, rows, edge_columns] if first_column else None
            if not first_row:
                return body, side, None, None
            far = pl.ds(rows_full, 1)
            body_far = kernel_ref[component, far, columns]
            side_far = kernel_ref[component, far, edge_columns] if first_column else None
            return body, side, body_far, side_far

        def pick(parts, odd_x, odd_y):
            body, side, body_far, side_far = parts
            mixed = jnp.where(left, side, body) if odd_y and first_column else body
            if odd_x and first_row:
                far = body_far
                if odd_y and first_column:
                    far = jnp.where(left[:1], side_far, far)
                mixed = jnp.where(top, far, mixed)
            return mixed

        own = [loaded(c, part) for part in range(2)]
        k_xy = [pick(loaded(3, part), 0, 0) if c < 2 else None for part in range(2)]
        k_xz = loaded(4) if c != 1 else None
        k_yz = loaded(5) if c != 0 else None

        def place(px, py):
            offset = py * columns_full + start
            return pl.ds(row_start + px * rows_full, sub), slice(offset, offset + lane)

        def spec(px, py, f):
            at_rows, at_columns = place(px, py)
            return spec_ref[f, at_rows, at_columns]

        for px in range(2):
            for py in range(2):
                own_here = [pick(own[part], px, py) for part in range(2)]
                xz_here = pick(k_xz, 0, py) if c != 1 else None
                yz_here = pick(k_yz, px, 0) if c != 0 else None
                for part in range(2):
                    turn = 1.0 if part else -1.0
                    sx = turn if px else -turn
                    sy = turn if py else -turn
                    other = 1 - part
                    total = own_here[part] * spec(px, py, 2 * c + part)
                    if c < 2:
                        across = k_xy[part] * spec(1 - px, 1 - py, 2 * (1 - c) + part)
                        total = total - across if px == py else total + across
                    if c == 0:
                        third = xz_here * spec(1 - px, py, 4 + other)
                        total = total + third if sx > 0 else total - third
                    elif c == 1:
                        third = yz_here * spec(px, 1 - py, 4 + other)
                        total = total + third if sy > 0 else total - third
                    else:
                        third = xz_here * spec(1 - px, py, other)
                        total = total + third if sx > 0 else total - third
                        third = yz_here * spec(px, 1 - py, 2 + other)
                        total = total + third if sy > 0 else total - third
                    at_rows, at_columns = place(px, py)
                    out_ref[part, at_rows, at_columns] = total

    for start in range(0, columns_full, lane):
        tile(0, True, start)

    unrolled = 3
    peeled = (rows_full // sub - 1) % unrolled + 1
    for n in range(1, peeled):
        for start in range(0, columns_full, lane):
            tile(n * sub, False, start)

    def step(i, carry):
        for n in range(unrolled):
            row_start = pl.multiple_of((unrolled * i + n + peeled) * sub, sub)
            for start in range(0, columns_full, lane):
                tile(row_start, False, start)
        return carry

    lax.fori_loop(0, (rows_full // sub - peeled) // unrolled, step, 0)


def arc_angle(sine, cosine):
    size = jnp.abs(cosine)
    low, high = jnp.minimum(sine, size), jnp.maximum(sine, size)
    ratio = low / jnp.maximum(high, 1e-37)
    wide = ratio > 0.41421356
    ratio = jnp.where(wide, (ratio - 1.0) / (ratio + 1.0), ratio)
    square = ratio * ratio
    series = ((8.05374449538e-2 * square - 1.38776856032e-1) * square + 1.99777106478e-1) * square
    angle = (series - 3.33329491539e-1) * square * ratio + ratio
    angle = jnp.where(wide, angle + 0.25 * math.pi, angle)
    angle = jnp.where(sine > size, 0.5 * math.pi - angle, angle)
    return jnp.where(cosine < 0.0, math.pi - angle, angle)


def dot3(first, second):
    return first[0] * second[0] + first[1] * second[1] + first[2] * second[2]


def band_kernel(
    scale,
    magnet_ref,
    kernel_ref,
    anisotropy_ref,
    source_tables,
    force_ref,
    small_ref,
    tables,
    cells_ref,
    film_ref,
    edge_out_ref,
    edge_ref,
    send_ref,
    back_ref,
    held_ref,
    spec_ref,
    field_ref,
    arrive_ref,
    next_ref,
    prior_ref,
    rim_out_ref,
    rim_ref,
    present_ref,
    ease_ref,
    sums_ref,
    tile_ref,
    swap_ref,
    peak_ref,
    tensor_ref,
    result_ref,
    own_sem,
    tensor_sem,
    film_send,
    film_recv,
    twin_send,
    twin_recv,
    plane_send,
    plane_recv,
    back_send,
    back_recv,
    last_send,
    last_recv,
    image_send,
    image_recv,
    rim_send,
    rim_recv,
    swap_send,
    swap_recv,
    peak_send,
    peak_recv,
    force_sem,
    table_sem,
):
    fy_ref, fx_ref = tables[:2]
    gx_ref, gy_ref = tables[:2] if len(tables) == 2 else tables[2:]
    groups, local_planes = held_ref.shape[1], held_ref.shape[2]
    slab, columns_full = held_ref.shape[4], held_ref.shape[5]
    layer_count = cells_ref.shape[2]
    rows_full = groups * slab
    parts = groups // 2
    me = lax.axis_index("space")
    half, seat = me // parts, lax.rem(me, parts)
    partner = lax.rem(me + parts, groups)
    flip = (1 - 2 * half).astype(jnp.float32)
    row_step = 8
    images, image = lax.axis_size("image"), lax.axis_index("image")
    first, last = image == 0, image == images - 1
    shifts = (-1, 0, 1)
    routes = [
        (n, shift, d)
        for n, shift in enumerate(shifts)
        for d in range(groups)
        if shift != 0 or d != 0
    ]

    def gate(exists, action):
        if exists is None:
            action()
        else:
            pl.when(exists)(action)

    def receiver(shift):
        return None if shift == 0 else jnp.logical_not(last if shift < 0 else first)

    def sender(shift):
        return None if shift == 0 else jnp.logical_not(first if shift < 0 else last)

    def target_of(shift, d):
        return {"image": lax.rem(image - shift + images, images), "space": lax.rem(me + d, groups)}

    def remote(src, dst, send, recv, target):
        return pltpu.make_async_remote_copy(
            src_ref=src,
            dst_ref=dst,
            send_sem=send,
            recv_sem=recv,
            device_id=target if isinstance(target, dict) else {"space": target},
            device_id_type=pl.DeviceIdType.MESH,
        )

    def row_loop(step):
        def chunk(i, carry):
            step(pl.ds(pl.multiple_of(i * row_step, row_step), row_step))
            return carry

        lax.fori_loop(0, slab // row_step, chunk, 0)

    def own_copy(c):
        return pltpu.make_async_copy(magnet_ref.at[:, c], cells_ref.at[:, c], own_sem.at[c])

    def tensor_copy(q):
        return pltpu.make_async_copy(
            kernel_ref.at[:, q, pl.ds(0, rows_full + 8), pl.ds(0, columns_full + 128)],
            tensor_ref.at[pl.ds(6 * q, 6)],
            tensor_sem.at[q],
        )

    def film_copy(c):
        return remote(
            magnet_ref.at[1 - half, c], film_ref.at[c], film_send.at[c], film_recv.at[c], partner
        )

    def kernel_copies():
        body = (pl.ds(0, rows_full), pl.ds(0, columns_full))
        far = (pl.ds(rows_full, 8), pl.ds(0, columns_full + 128))
        twin = 6 * local_planes
        pieces = [(tensor_ref.at[n, *body], tensor_ref.at[twin + n, *body]) for n in (0, 3)]
        pieces += [
            (edge_out_ref, edge_ref),
            (tensor_ref.at[pl.ds(0, 3), *far], tensor_ref.at[pl.ds(twin, 3), *far]),
        ]
        pieces += [(tensor_ref.at[n, *body], tensor_ref.at[twin + n, *body]) for n in (1, 2)]
        return [
            remote(src, dst, twin_send.at[n], twin_recv.at[n], partner)
            for n, (src, dst) in enumerate(pieces)
        ]

    def pack_edges():
        rows, columns = pl.ds(0, rows_full), pl.ds(columns_full, 128)
        lane_pos = lax.broadcasted_iota(jnp.int32, (rows_full, 128), 1)
        edge = tensor_ref[0, rows, columns]
        for c in (1, 2):
            edge = jnp.where(lane_pos == c, pltpu.roll(tensor_ref[c, rows, columns], c, 1), edge)
        edge_out_ref[...] = edge

    def unpack_edges():
        rows, columns = pl.ds(0, rows_full), pl.ds(columns_full, 128)
        edge = edge_ref[...]
        for c in range(3):
            tensor_ref[6 * local_planes + c, rows, columns] = pltpu.roll(edge, 128 - c, 1) if c else edge

    def place_of(seat_index, kind):
        return lax.rem((half + kind) * parts + seat_index, groups)

    def plane_copy(c, kind, slot):
        target = lax.rem(seat + 1 + slot, parts)
        return remote(
            send_ref.at[c, kind, slot],
            held_ref.at[c, place_of(seat, kind)],
            plane_send.at[c, kind, slot],
            plane_recv.at[c, kind, parts - 2 - slot],
            half * parts + target,
        )

    def plane_arrival(c, kind, slot):
        source = lax.rem(seat + 1 + slot, parts)
        return remote(
            send_ref.at[c, kind, slot],
            held_ref.at[c, place_of(source, kind)],
            plane_send.at[c, kind, slot],
            plane_recv.at[c, kind, slot],
            half * parts + source,
        )

    def back_copy(c, q, kind, slot):
        target = lax.rem(seat + 1 + slot, parts)
        return remote(
            held_ref.at[c, place_of(target, kind), q],
            back_ref.at[c, kind, parts - 2 - slot, q],
            back_send.at[c, q, kind, slot],
            back_recv.at[c, q, kind, parts - 2 - slot],
            half * parts + target,
        )

    def back_arrival(c, q, kind, slot):
        source = lax.rem(seat + 1 + slot, parts)
        return remote(
            held_ref.at[c, place_of(source, kind), q],
            back_ref.at[c, kind, slot, q],
            back_send.at[c, q, kind, slot],
            back_recv.at[c, q, kind, slot],
            half * parts + source,
        )

    def last_copy(c):
        return remote(
            film_ref.at[c], arrive_ref.at[c], last_send.at[c], last_recv.at[c], partner
        )

    def ahead_copy():
        return remote(
            magnet_ref.at[1],
            prior_ref,
            image_send.at[0],
            image_recv.at[0],
            {"image": lax.rem(image + 1, images)},
        )

    def behind_copy():
        return remote(
            magnet_ref.at[0],
            next_ref,
            image_send.at[1],
            image_recv.at[1],
            {"image": lax.rem(image + images - 1, images)},
        )

    def rim_copy(side):
        return remote(
            rim_out_ref.at[side],
            rim_ref.at[side],
            rim_send.at[side],
            rim_recv.at[side],
            lax.rem(me + (1 if side == 0 else groups - 1), groups),
        )

    def swap_copy(n, shift, d, slot):
        return remote(
            tile_ref, swap_ref.at[n, slot], swap_send.at[n, d], swap_recv.at[n, d], target_of(shift, d)
        )

    def peak_copy(d, slot):
        return remote(
            tile_ref.at[pl.ds(0, 8)],
            peak_ref.at[slot],
            peak_send.at[d],
            peak_recv.at[d],
            lax.rem(me + d, groups),
        )

    def table_copy(n):
        return pltpu.make_async_copy(source_tables[n], tables[n], table_sem.at[n])

    def force_copy(i):
        return pltpu.make_async_copy(field_ref.at[i], force_ref.at[i], force_sem.at[i])

    def transform_layers(c, kind):
        place = place_of(seat, kind)

        def variant(here):
            def step(rows):
                if kind == 0:
                    layers = [cells_ref[half, c, z, rows, :] for z in range(layer_count)]
                else:
                    layers = [film_ref[c, z, rows, :] for z in range(layer_count)]
                layers = [v * flip if z % 2 else v for z, v in enumerate(layers)]
                spectrum = layers_to_spectrum(layers)
                for k in range(layer_count):
                    target, q = k // local_planes, k % local_planes
                    slot = (target - here) % parts - 1
                    for part in range(2):
                        if target == here:
                            held_ref[c, place, q, part, rows, :] = spectrum[k][part]
                        else:
                            send_ref[c, kind, slot, q, part, rows, :] = spectrum[k][part]

            row_loop(step)

        for here in range(parts):
            pl.when(seat == here)(functools.partial(variant, here))
        for slot in range(parts - 1):
            plane_copy(c, kind, slot).start()

    def transform_planes(c, kind):
        place = place_of(seat, kind)

        def variant(here):
            def step(rows):
                spectrum = []
                for k in range(layer_count):
                    source, q = k // local_planes, k % local_planes
                    slot = (source - here) % parts - 1
                    if source == here:
                        spectrum.append(
                            [held_ref[c, place, q, part, rows, :] for part in range(2)]
                        )
                    else:
                        spectrum.append(
                            [back_ref[c, kind, slot, q, part, rows, :] for part in range(2)]
                        )
                for z, value in enumerate(spectrum_to_layers(spectrum)):
                    value = value * (scale * flip if z % 2 else scale)
                    if kind == 0:
                        field_ref[half, c, z, rows, :] = field_ref[half, c, z, rows, :] + value
                    else:
                        film_ref[c, z, rows, :] = value

            row_loop(step)

        for here in range(parts):
            pl.when(seat == here)(functools.partial(variant, here))

    def fill_rims():
        def step(f, carry):
            i, c = f // 3, lax.rem(f, 3)
            for side in range(2):
                row = slab - 1 if side == 0 else 0
                rim_out_ref[side, i, c] = jnp.concatenate(
                    [cells_ref[i, c, z, row : row + 1, :] for z in range(layer_count)], axis=0
                )
            return carry

        lax.fori_loop(0, 6, step, 0)
        row_pos = lax.broadcasted_iota(jnp.int32, (slab, columns_full), 0) + me * slab
        column_pos = lax.broadcasted_iota(jnp.int32, (slab, columns_full), 1)
        faces = [row_pos == 0, row_pos == rows_full - 1]
        faces += [column_pos == 0, column_pos == columns_full - 1]
        present_ref[...] = 6.0 - sum(jnp.where(face, 1.0, 0.0) for face in faces)
        for side in range(2):
            open_side = me != groups - 1 if side == 0 else me != 0

            @pl.when(open_side)
            def _():
                rim_copy(side).start()

            no_source = me == 0 if side == 0 else me == groups - 1

            @pl.when(no_source)
            def _():
                rim_ref[side] = jnp.zeros(rim_ref.shape[1:], jnp.float32)

    def wait_rims():
        for side in range(2):
            has_source = me != 0 if side == 0 else me != groups - 1

            @pl.when(has_source)
            def _():
                rim_copy(side).wait_recv()

    def local_fields(i):
        row_pos = lax.broadcasted_iota(jnp.int32, (slab, columns_full), 0)
        column_pos = lax.broadcasted_iota(jnp.int32, (slab, columns_full), 1)

        def step(z, carry):
            below, above = jnp.maximum(z - 1, 0), jnp.minimum(z + 1, layer_count - 1)
            has_below = (z > 0).astype(jnp.float32)
            has_above = (z < layer_count - 1).astype(jnp.float32)
            present = present_ref[...] - (2.0 - has_below - has_above)
            tilt = []
            for c in range(3):
                cells = cells_ref[i, c, z]
                x_plus = jnp.where(
                    row_pos == slab - 1,
                    rim_ref[1, i, c, pl.ds(z, 1), :],
                    pltpu.roll(cells, slab - 1, 0),
                )
                x_minus = jnp.where(
                    row_pos == 0, rim_ref[0, i, c, pl.ds(z, 1), :], pltpu.roll(cells, 1, 0)
                )
                y_plus = jnp.where(
                    column_pos == columns_full - 1, 0.0, pltpu.roll(cells, columns_full - 1, 1)
                )
                y_minus = jnp.where(column_pos == 0, 0.0, pltpu.roll(cells, 1, 1))
                around = x_plus + x_minus + y_plus + y_minus
                around = around + has_above * cells_ref[i, c, above] + has_below * cells_ref[i, c, below]
                part = exchange_strength * (around - present * cells)
                if c == 0:
                    tilt.append(x_plus - x_minus)
                    field_ref[i, 0, z] = part
                elif c == 1:
                    tilt.append(y_plus - y_minus)
                    field_ref[i, 1, z] = part
                else:
                    ease = ease_ref[...] * cells
                    field_ref[i, 2, z] = part + (ease - chiral_strength * (tilt[0] + tilt[1]))
                    field_ref[i, 0, z] = field_ref[i, 0, z] + chiral_strength * (x_plus - x_minus)
                    field_ref[i, 1, z] = field_ref[i, 1, z] + chiral_strength * (y_plus - y_minus)
            return carry

        lax.fori_loop(0, layer_count, step, 0)

    lane = columns_full

    def cell_loop(step, carry):
        unrolled = min(4, slab // row_step)
        steps = slab // (unrolled * row_step)

        def chunk(index, carry):
            z = index // steps
            start = lax.rem(index, steps) * unrolled * row_step
            for n in range(unrolled):
                carry = step(z, pl.multiple_of(start + n * row_step, row_step), carry)
            return carry

        return lax.fori_loop(0, layer_count * steps, chunk, carry)

    def zeros(count):
        return tuple(jnp.zeros((row_step, lane), jnp.float32) for _ in range(count))

    def tangent_rows(z, start):
        return pl.ds(pl.multiple_of(z * slab + start, row_step), row_step)

    def neighbour_sums():
        @pl.when(jnp.logical_not(first))
        def _():
            ahead_copy().wait_recv()

        @pl.when(first)
        def _():
            for c in range(3):
                prior_ref[c] = cells_ref[0, c]

        @pl.when(jnp.logical_not(last))
        def _():
            behind_copy().wait_recv()

        @pl.when(last)
        def _():
            for c in range(3):
                next_ref[c] = cells_ref[1, c]

        for i in range(2):

            def step(z, start, carry):
                rows = pl.ds(start, row_step)
                here = [cells_ref[i, c, z, rows, :] for c in range(3)]
                if i == 0:
                    ahead = [cells_ref[1, c, z, rows, :] for c in range(3)]
                    behind = [prior_ref[c, z, rows, :] for c in range(3)]
                else:
                    ahead = [next_ref[c, z, rows, :] for c in range(3)]
                    behind = [cells_ref[0, c, z, rows, :] for c in range(3)]
                normal = [
                    here[1] * ahead[2] - here[2] * ahead[1],
                    here[2] * ahead[0] - here[0] * ahead[2],
                    here[0] * ahead[1] - here[1] * ahead[0],
                ]
                angle = arc_angle(jnp.sqrt(dot3(normal, normal)), dot3(here, ahead))
                ahead = [ahead[c] - here[c] for c in range(3)]
                behind = [here[c] - behind[c] for c in range(3)]
                ahead_on, behind_on = dot3(ahead, here), dot3(behind, here)
                ahead = [ahead[c] - ahead_on * here[c] for c in range(3)]
                behind = [behind[c] - behind_on * here[c] for c in range(3)]
                for c in range(3):
                    place = tangent_rows(z, start)
                    spec_ref[0, 3 * i + c, place, 0:columns_full] = ahead[c]
                    spec_ref[0, 3 * i + c, place, columns_full : 2 * columns_full] = behind[c]
                values = (
                    angle * angle,
                    dot3(ahead, ahead),
                    dot3(ahead, behind),
                    dot3(behind, behind),
                )
                return tuple(total + value for total, value in zip(carry, values))

            totals = cell_loop(step, zeros(4))
            for k in range(4):
                sums_ref[i, k + 1] = totals[k]

    def field_sums(i, c, arrived):
        def step(z, start, carry):
            rows = pl.ds(start, row_step)
            place = tangent_rows(z, start)
            field = field_ref[i, c, z, rows, :]
            if arrived:
                field = field + arrive_ref[c, z, rows, :]
                field_ref[i, c, z, rows, :] = field
            values = (
                cells_ref[i, c, z, rows, :] * field,
                field * spec_ref[0, 3 * i + c, place, 0:columns_full],
                field * spec_ref[0, 3 * i + c, place, columns_full : 2 * columns_full],
            )
            return tuple(total + value for total, value in zip(carry, values))

        totals = cell_loop(step, zeros(3))
        for k, slot in enumerate((0, 5, 6)):
            sums_ref[i, slot] = totals[k] if c == 0 else sums_ref[i, slot] + totals[k]

    barrier = pltpu.get_barrier_semaphore()
    for n, shift, d in routes:
        signal = functools.partial(
            pl.semaphore_signal,
            barrier,
            inc=1,
            device_id=target_of(shift, d),
            device_id_type=pl.DeviceIdType.MESH,
        )
        gate(receiver(shift), signal)
    for c in range(3):
        own_copy(c).start()
    for n in range(len(tables)):
        table_copy(n).start()

    def spread(r, carry):
        ease_ref[pl.ds(r, 1), :] = jnp.full((1, columns_full), 2.0 * anisotropy_ref[r])
        return carry

    lax.fori_loop(0, slab, spread, 0)
    ends = first.astype(jnp.int32) + last.astype(jnp.int32)
    pl.semaphore_wait(barrier, len(routes) - groups * ends)
    film_copy(0).start()

    @pl.when(jnp.logical_not(last))
    def _():
        ahead_copy().start()

    @pl.when(jnp.logical_not(first))
    def _():
        behind_copy().start()

    for c in range(3):
        own_copy(c).wait()
    fill_rims()
    for c in range(1, 3):
        film_copy(c).start()

    for q in range(local_planes):
        tensor_copy(q).start()

    for c in range(3):
        transform_layers(c, 0)
    for n in range(len(tables)):
        table_copy(n).wait()
    tensor_copy(0).wait()

    @pl.when(seat == 0)
    def _():
        pack_edges()
        for copy in kernel_copies():
            copy.start()

    for c in range(3):
        film_copy(c).wait_recv()
        transform_layers(c, 1)
        for kind in range(2):
            for slot in range(parts - 1):
                plane_arrival(c, kind, slot).wait_recv()

        def forward(i, carry):
            q = i
            fy = jnp.concatenate([fy_ref[0], fy_ref[0], fy_ref[1]], axis=0)
            fx = jnp.concatenate([fx_ref[0], fx_ref[0], fx_ref[1]], axis=1)
            cells = jnp.concatenate(
                [held_ref[c, g, q, part] for part in range(2) for g in range(groups)], axis=0
            )
            lines = dot32(three_limbs(cells, 1), fy)
            for part in range(2):
                spec_ref[q, 2 * c + part] = dot32(
                    fx, three_limbs(lines[part * rows_full : (part + 1) * rows_full], 0)
                )
            return carry

        lax.fori_loop(0, local_planes, forward, 0)
        if c == 0:
            wait_rims()
        if c < 2:
            local_fields(c)

    for q in range(1, local_planes):
        tensor_copy(q).wait()

    for c in range(3):

        def backward(i, carry):
            q = local_planes - 1 - i
            twin = (seat == 0) & (q == 0)

            @pl.when(twin)
            def _():
                for copy in kernel_copies()[:4] if c == 0 else kernel_copies()[c + 3 : c + 4]:
                    copy.wait_recv()
                if c == 0:
                    unpack_edges()

            second = jnp.where(twin, local_planes, q)
            kernels = (tensor_ref.at[pl.ds(6 * q, 6)], tensor_ref.at[pl.ds(6 * second, 4)])
            tensor_part(c, spec_ref.at[q], kernels, result_ref)
            gx = jnp.concatenate([gx_ref[0], gx_ref[0], gx_ref[1]], axis=1)
            gy = jnp.concatenate([gy_ref[0], gy_ref[0], gy_ref[1]], axis=0)
            for part in range(2):
                lines = dot32(gx, three_limbs(result_ref[part], 0))
                cells = dot32(three_limbs(lines, 1), gy)
                for g in range(groups):
                    held_ref[c, g, q, part] = cells[g * slab : (g + 1) * slab]
            for kind in (1, 0):
                for slot in range(parts - 1):
                    back_copy(c, q, kind, slot).start()

            return carry

        lax.fori_loop(0, local_planes, backward, 0)
        for kind in (1, 0):
            for q in range(local_planes):
                for slot in range(parts - 1):
                    back_arrival(c, q, kind, slot).wait_recv()
            transform_planes(c, kind)
            if kind == 1:
                last_copy(c).start()

    neighbour_sums()
    for c in range(3):
        field_sums(half, c, False)
    for c in range(3):
        last_copy(c).wait_recv()
        field_sums(1 - half, c, True)

    rows = [
        jnp.sum(sums_ref[i, k], axis=0, keepdims=True) for i in range(2) for k in range(7)
    ] + [jnp.zeros((1, lane), jnp.float32)] * 2
    tile = jnp.sum(jnp.concatenate(rows, axis=0), axis=1, keepdims=True)
    tile_ref[...] = jnp.broadcast_to(tile, tile_ref.shape)
    for n, shift, d in routes:
        gate(receiver(shift), swap_copy(n, shift, d, me).start)
    swap_ref[1, me] = tile_ref[...]
    for n, end in ((0, first), (2, last)):

        @pl.when(end)
        def _():
            swap_ref[n] = jnp.zeros(swap_ref.shape[1:], jnp.float32)

    for n, shift, d in routes:
        gate(sender(shift), swap_copy(n, shift, d, lax.rem(me + groups - d, groups)).wait_recv)
    totals = []
    for n in range(3):
        total = swap_ref[n, 0]
        for g in range(1, groups):
            total = total + swap_ref[n, g]
        totals.append(total)

    def entry(n, i, k):
        return totals[n][7 * i + k : 7 * i + k + 1]

    cell_count = float(layer_count * rows_full * columns_full)
    energies = [-0.5 * entry(*at, 0) for at in ((0, 1), (1, 0), (1, 1), (2, 0))]
    distances = [jnp.sqrt(entry(*at, 1) / cell_count) for at in ((0, 1), (1, 0), (1, 1))]
    pulls = []
    for i in range(2):
        weight_next, weight_prior = tangent_weights(energies[i + 1], energies[i + 2], energies[i])
        length_square = (
            weight_next * weight_next * entry(1, i, 2)
            + 2.0 * weight_next * weight_prior * entry(1, i, 3)
            + weight_prior * weight_prior * entry(1, i, 4)
        )
        drive = weight_next * entry(1, i, 5) + weight_prior * entry(1, i, 6)
        size = jnp.sqrt(jnp.maximum(length_square, 0.0) / cell_count + epsilon)
        spring = spring_strength * (distances[i + 1] - distances[i])
        pull = (spring - drive / (cell_count * size)) / size
        pulls.append((pull * weight_next, pull * weight_prior))
    for n, shift, d in routes:
        gate(receiver(shift), swap_copy(n, shift, d, me).wait_send)
    peaks = []
    for i in range(2):
        end = first if i == 0 else last
        ahead_pull, behind_pull = [
            jnp.concatenate([jnp.broadcast_to(pull, (row_step, 128))] * (lane // 128), axis=1)
            for pull in pulls[i]
        ]

        def step(z, start, peak):
            rows = pl.ds(start, row_step)
            place = tangent_rows(z, start)
            here = [cells_ref[i, c, z, rows, :] for c in range(3)]
            force = []
            for c in range(3):
                ahead = spec_ref[0, 3 * i + c, place, 0:columns_full]
                behind = spec_ref[0, 3 * i + c, place, columns_full : 2 * columns_full]
                field = field_ref[i, c, z, rows, :]
                force.append(field + ahead_pull * ahead + behind_pull * behind)
            along = dot3(force, here)
            force = [jnp.where(end, 0.0, force[c] - along * here[c]) for c in range(3)]
            for c in range(3):
                field_ref[i, c, z, rows, :] = force[c]
            return (jnp.maximum(peak[0], dot3(force, force)),)

        (peak,) = cell_loop(step, zeros(1))
        peaks.append(jnp.max(peak, axis=0, keepdims=True))
        force_copy(i).start()
    peak = jnp.concatenate(peaks + [jnp.zeros((6, lane), jnp.float32)], axis=0)
    peak = jnp.broadcast_to(jnp.max(peak, axis=1, keepdims=True), (8, 128))
    tile_ref[0:8] = peak
    for d in range(1, groups):
        peak_copy(d, me).start()
    peak_ref[me] = peak
    for d in range(1, groups):
        peak_copy(d, lax.rem(me + groups - d, groups)).wait_recv()
    largest = peak_ref[0]
    for g in range(1, groups):
        largest = jnp.maximum(largest, peak_ref[g])
    moves = jnp.minimum(step_limit, rotation_limit / (jnp.sqrt(largest) + epsilon))
    energy = jnp.concatenate(energies[1:3], axis=0) / cell_count
    small_ref[...] = jnp.concatenate([moves[0:2], energy, jnp.zeros((4, 128), jnp.float32)], axis=0)
    for i in range(2):
        force_copy(i).wait()
    for d in range(1, groups):
        peak_copy(d, me).wait_send()
    for c in range(3):
        film_copy(c).wait_send()
        last_copy(c).wait_send()
        for kind in range(2):
            for slot in range(parts - 1):
                plane_copy(c, kind, slot).wait_send()
                for q in range(local_planes):
                    back_copy(c, q, kind, slot).wait_send()

    @pl.when(seat == 0)
    def _():
        for copy in kernel_copies():
            copy.wait_send()

    for side in range(2):
        open_side = me != groups - 1 if side == 0 else me != 0

        @pl.when(open_side)
        def _():
            rim_copy(side).wait_send()

    @pl.when(jnp.logical_not(last))
    def _():
        ahead_copy().wait_send()

    @pl.when(jnp.logical_not(first))
    def _():
        behind_copy().wait_send()


def band_step(magnet, anisotropy, kernel):
    layer_count, row_count, column_count = magnet.shape[2:]
    groups = lax.axis_size("space")
    local_planes = 2 * layer_count // groups
    full_rows = row_count * groups
    slots = groups // 2 - 1
    table_y = parity_table(column_count)
    table_x = parity_table(full_rows)
    square = full_rows == column_count
    tables = [table_limbs(t) for t in (table_y, table_x.T, table_x, table_y.T)][: 2 if square else 4]

    def entry(magnet_ref, kernel_ref, anisotropy_ref, *refs):
        count = len(tables)
        sources, outs = refs[:count], refs[count : count + 2]
        held, rest = refs[count + 2 : 2 * count + 2], refs[2 * count + 2 :]
        scale = -4.0 / padded_cells
        band_kernel(
            scale, magnet_ref, kernel_ref, anisotropy_ref, sources, *outs, held, *rest
        )

    slab = (row_count, column_count)
    film = (layer_count,) + slab
    block = (local_planes, 2) + slab
    anywhere = pl.BlockSpec(memory_space=pl.ANY)
    inside = pl.BlockSpec(memory_space=pltpu.VMEM)
    dots = 6 * local_planes * 4 * full_rows * column_count * 3 * (full_rows + column_count // 2)
    padded_cells = 8 * layer_count * full_rows * column_count
    signals = pltpu.SemaphoreType.DMA
    scratch = [
        (2, 3) + film,
        (3,) + film,
        (full_rows, 128),
        (full_rows, 128),
        (3, 2, slots) + block,
        (3, 2, slots) + block,
        (3, groups) + block,
        (local_planes, 6, 2 * full_rows, 2 * column_count),
        (2, 3) + film,
        (3,) + film,
        (3,) + film,
        (3,) + film,
        (2, 2, 3, layer_count, column_count),
        (2, 2, 3, layer_count, column_count),
        slab,
        slab,
        (2, 7, 8, column_count),
        (16, 128),
        (3, groups, 16, 128),
        (groups, 8, 128),
        (6 * local_planes + 4, full_rows + 8, column_count + 128),
    ]
    semaphores = [
        (3,),
        (local_planes,),
        (3,),
        (3,),
        (6,),
        (6,),
        (3, 2, slots),
        (3, 2, slots),
        (3, local_planes, 2, slots),
        (3, local_planes, 2, slots),
        (3,),
        (3,),
        (2,),
        (2,),
        (2,),
        (2,),
        (3, groups),
        (3, groups),
        (groups,),
        (groups,),
        (2,),
        (len(tables),),
    ]
    return pl.pallas_call(
        entry,
        in_specs=[anywhere, anywhere, pl.BlockSpec(memory_space=pltpu.SMEM)]
        + [anywhere] * len(tables),
        out_specs=[anywhere, inside],
        out_shape=[
            jax.ShapeDtypeStruct(magnet.shape, jnp.float32),
            jax.ShapeDtypeStruct((8, 128), jnp.float32),
        ],
        scratch_shapes=[pltpu.VMEM(t.shape, jnp.bfloat16) for t in tables]
        + [pltpu.VMEM(dims, jnp.float32) for dims in scratch]
        + [pltpu.VMEM((2, 2 * full_rows, 2 * column_count), jnp.float32)]
        + [signals(dims) for dims in semaphores],
        compiler_params=pltpu.CompilerParams(
            vmem_limit_bytes=67043328, collective_id=0, has_side_effects=True
        ),
        cost_estimate=pl.CostEstimate(
            flops=4 * dots, bytes_accessed=4 * magnet.size * 4, transcendentals=0
        ),
        name="band_kernel",
    )(magnet, kernel, anisotropy, *[jnp.asarray(t) for t in tables])


def move_kernel(
    small_ref,
    magnet_ref,
    force_ref,
    updated_ref,
    out_ref,
    energy_ref,
    cells_ref,
    held_ref,
    magnet_sem,
    force_sem,
    updated_sem,
    out_sem,
):
    images, _, layer_count, slab, columns = magnet_ref.shape
    pieces = magnet_sem.shape[1]
    layers = layer_count // pieces

    def copy(src, dst, sem, i, k):
        part = pl.ds(k * layers, layers)
        return pltpu.make_async_copy(src.at[i, :, part], dst.at[i, :, part], sem.at[i, k])

    places = [(i, k) for i in range(images) for k in range(pieces)]
    ahead = 4

    def load(i, k):
        copy(force_ref, held_ref, force_sem, i, k).start()
        copy(magnet_ref, cells_ref, magnet_sem, i, k).start()

    for i, k in places[:ahead]:
        load(i, k)
    for n in range(images):
        energy_ref[n] = jnp.max(small_ref[n + 2 : n + 3, :])
    row_step = 8
    unrolled = min(4, slab // row_step)
    steps = slab // (unrolled * row_step)
    for index, (i, k) in enumerate(places):
        move = jnp.broadcast_to(small_ref[i : i + 1, :], (row_step, 128))
        move = jnp.concatenate([move] * (columns // 128), axis=1)
        copy(force_ref, held_ref, force_sem, i, k).wait()
        copy(held_ref, out_ref, out_sem, i, k).start()
        copy(magnet_ref, cells_ref, magnet_sem, i, k).wait()
        for place in places[index + ahead : index + ahead + 1]:
            load(*place)

        def chunk(index, carry):
            z = k * layers + index // steps
            for n in range(unrolled):
                start = (lax.rem(index, steps) * unrolled + n) * row_step
                rows = pl.ds(pl.multiple_of(start, row_step), row_step)
                moved = [
                    cells_ref[i, c, z, rows, :] + move * held_ref[i, c, z, rows, :]
                    for c in range(3)
                ]
                inverse = lax.rsqrt(dot3(moved, moved))
                for c in range(3):
                    cells_ref[i, c, z, rows, :] = inverse * moved[c]
            return carry

        lax.fori_loop(0, layers * steps, chunk, 0)
        copy(cells_ref, updated_ref, updated_sem, i, k).start()
    for i, k in places:
        copy(held_ref, out_ref, out_sem, i, k).wait()
        copy(cells_ref, updated_ref, updated_sem, i, k).wait()


def move_images(magnet, force, small):
    images, _, layer_count = magnet.shape[:3]
    pieces = math.gcd(layer_count, 2)
    anywhere = pl.BlockSpec(memory_space=pl.ANY)
    return pl.pallas_call(
        move_kernel,
        in_specs=[pl.BlockSpec(memory_space=pltpu.VMEM), anywhere, anywhere],
        out_specs=[anywhere, anywhere, pl.BlockSpec(memory_space=pltpu.SMEM)],
        out_shape=[
            jax.ShapeDtypeStruct(magnet.shape, jnp.float32),
            jax.ShapeDtypeStruct(magnet.shape, jnp.float32),
            jax.ShapeDtypeStruct((images,), jnp.float32),
        ],
        scratch_shapes=[pltpu.VMEM(magnet.shape, jnp.float32)] * 2
        + [pltpu.SemaphoreType.DMA((images, pieces))] * 4,
        name="move_kernel",
    )(small, magnet, force)


def body(magnet, anisotropy, kernel):
    force, small = band_step(magnet, anisotropy, kernel)
    return move_images(magnet, force, small)


def solution(mesh):
    in_specs = (P("image", None, None, "space", None), P("space"), P(None, "space", None, None))
    out_specs = (
        P("image", None, None, "space", None),
        P("image", None, None, "space", None),
        P("image"),
    )
    return jax.shard_map(body, mesh=mesh, in_specs=in_specs, out_specs=out_specs, check_vma=False)
```

```python
import functools
import math

import jax
import jax.numpy as jnp
import numpy as np
from jax import lax
from jax.experimental import pallas as pl
from jax.experimental.pallas import tpu as pltpu
from jax.sharding import PartitionSpec as P

exchange_strength = 0.25
chiral_strength = 0.3
spring_strength = 10.0
step_limit = 1.0
rotation_limit = 0.5
epsilon = 1e-06


def tangent_weights(energy_total, energy_next, energy_prior):
    rise_next = energy_next - energy_total
    rise_prior = energy_total - energy_prior
    upward = (rise_next > 0) & (rise_prior > 0)
    downward = (rise_next < 0) & (rise_prior < 0)
    larger = jnp.maximum(jnp.abs(rise_next), jnp.abs(rise_prior))
    smaller = jnp.minimum(jnp.abs(rise_next), jnp.abs(rise_prior))
    toward_next = energy_next > energy_prior
    weight_next = jnp.where(
        upward, 1.0, jnp.where(downward, 0.0, jnp.where(toward_next, larger, smaller))
    )
    weight_prior = jnp.where(
        upward, 0.0, jnp.where(downward, 1.0, jnp.where(toward_next, smaller, larger))
    )
    return (weight_next, weight_prior)


def split_limbs(values):
    upper = values.astype(jnp.bfloat16)
    return upper, (values - upper.astype(jnp.float32)).astype(jnp.bfloat16)


def table_limbs(table):
    upper = table.astype(np.float32).astype(jnp.bfloat16)
    lower = (table - upper.astype(np.float64)).astype(np.float32).astype(jnp.bfloat16)
    return np.stack([upper, lower])


def parity_table(count):
    position = np.arange(count)[:, None]
    slot = np.arange(count)[None, :]
    turn = np.pi / count
    even_part = np.cos(turn * (position * slot % (2 * count)))
    odd_part = np.sin(turn * (position * slot % (2 * count)))
    odd_part[:, 0] = np.cos(turn * (position[:, 0] * count % (2 * count)))
    table = np.concatenate([even_part, odd_part], axis=1)
    table[:, [0, count]] *= math.sqrt(0.5)
    return table


def half_table(count):
    place = np.arange(count)
    angle = np.pi * (place[:, None] * place[None, :] % (2 * count)) / count
    cosine, sine = np.cos(angle), np.sin(angle)
    cosine[np.abs(cosine) < 1e-12] = 0.0
    sine[np.abs(sine) < 1e-12] = 0.0
    return cosine, sine


def weighted(terms):
    total = None
    for weight, value in terms:
        weight = float(weight)
        if weight == 0.0:
            continue
        if total is None:
            total = value if weight == 1.0 else -value if weight == -1.0 else weight * value
        elif weight == 1.0:
            total = total + value
        elif weight == -1.0:
            total = total - value
        else:
            total = total + weight * value
    return total


def layers_to_spectrum(layers):
    count = len(layers)
    half = count // 2
    cosine, sine = half_table(count)
    sums = {z: layers[z] + layers[count - z] for z in range(1, half)}
    gaps = {z: layers[z] - layers[count - z] for z in range(1, half)}
    spectrum = []
    for k in range(count):
        near, far = (sums, gaps) if k % 2 == 0 else (gaps, sums)
        re = weighted(
            [(1.0, layers[0]), (cosine[half, k], layers[half])]
            + [(cosine[z, k], near[z]) for z in range(1, half)]
        )
        if k == 0:
            im = weighted(
                [(1.0, layers[0]), ((-1.0) ** half, layers[half])]
                + [((-1.0) ** z, near[z]) for z in range(1, half)]
            )
        else:
            im = weighted(
                [(-sine[half, k], layers[half])] + [(-sine[z, k], far[z]) for z in range(1, half)]
            )
        spectrum.append((re, im))
    return spectrum


def spectrum_to_layers(spectrum):
    count = len(spectrum)
    half = count // 2
    cosine, sine = half_table(count)
    layers = [None] * count
    evens, odds = range(2, count, 2), range(1, count, 2)
    ground = [spectrum[0][0] + spectrum[0][1], spectrum[0][0] - spectrum[0][1]]
    layers[0] = weighted([(1.0, ground[0])] + [(2.0, spectrum[k][0]) for k in range(1, count)])
    layers[half] = weighted(
        [(1.0, ground[half % 2])]
        + [(2.0 * cosine[half, k], spectrum[k][0]) for k in range(1, count)]
        + [(-2.0 * sine[half, k], spectrum[k][1]) for k in range(1, count)]
    )
    for z in range(1, half):
        even_re = weighted(
            [(1.0, ground[z % 2])] + [(2.0 * cosine[z, k], spectrum[k][0]) for k in evens]
        )
        odd_re = weighted([(2.0 * cosine[z, k], spectrum[k][0]) for k in odds])
        even_im = weighted([(2.0 * sine[z, k], spectrum[k][1]) for k in evens])
        odd_im = weighted([(2.0 * sine[z, k], spectrum[k][1]) for k in odds])
        layers[z] = (even_re - odd_im) + (odd_re - even_im)
        layers[count - z] = (even_re - odd_im) - (odd_re - even_im)
    return layers


def dot32(left, right):
    return jnp.dot(left, right, preferred_element_type=jnp.float32)


def three_limbs(values, axis):
    upper, lower = split_limbs(values)
    return jnp.concatenate([upper, lower, upper], axis=axis)


def tensor_part(c, spec_ref, kernel_refs, out_ref):
    rows_full, columns_full = out_ref.shape[1] // 2, out_ref.shape[2] // 2
    lane = 128
    sub = 8
    top = lax.broadcasted_iota(jnp.int32, (sub, lane), 0) == 0
    left = lax.broadcasted_iota(jnp.int32, (sub, lane), 1) == 0

    def tile(row_start, first_row, start):
        rows = pl.ds(row_start, sub)
        columns = slice(start, start + lane)
        edge_columns = slice(columns_full, columns_full + lane)
        first_column = start == 0

        def loaded(component, part=0):
            kernel_ref = kernel_refs[part]
            body = kernel_ref[component, rows, columns]
            side = kernel_ref[component, rows, edge_columns] if first_column else None
            if not first_row:
                return body, side, None, None
            far = pl.ds(rows_full, 1)
            body_far = kernel_ref[component, far, columns]
            side_far = kernel_ref[component, far, edge_columns] if first_column else None
            return body, side, body_far, side_far

        def pick(parts, odd_x, odd_y):
            body, side, body_far, side_far = parts
            mixed = jnp.where(left, side, body) if odd_y and first_column else body
            if odd_x and first_row:
                far = body_far
                if odd_y and first_column:
                    far = jnp.where(left[:1], side_far, far)
                mixed = jnp.where(top, far, mixed)
            return mixed

        own = [loaded(c, part) for part in range(2)]
        k_xy = [pick(loaded(3, part), 0, 0) if c < 2 else None for part in range(2)]
        k_xz = loaded(4) if c != 1 else None
        k_yz = loaded(5) if c != 0 else None

        def place(px, py):
            offset = py * columns_full + start
            return pl.ds(row_start + px * rows_full, sub), slice(offset, offset + lane)

        def spec(px, py, f):
            at_rows, at_columns = place(px, py)
            return spec_ref[f, at_rows, at_columns]

        for px in range(2):
            for py in range(2):
                own_here = [pick(own[part], px, py) for part in range(2)]
                xz_here = pick(k_xz, 0, py) if c != 1 else None
                yz_here = pick(k_yz, px, 0) if c != 0 else None
                for part in range(2):
                    turn = 1.0 if part else -1.0
                    sx = turn if px else -turn
                    sy = turn if py else -turn
                    other = 1 - part
                    total = own_here[part] * spec(px, py, 2 * c + part)
                    if c < 2:
                        across = k_xy[part] * spec(1 - px, 1 - py, 2 * (1 - c) + part)
                        total = total - across if px == py else total + across
                    if c == 0:
                        third = xz_here * spec(1 - px, py, 4 + other)
                        total = total + third if sx > 0 else total - third
                    elif c == 1:
                        third = yz_here * spec(px, 1 - py, 4 + other)
                        total = total + third if sy > 0 else total - third
                    else:
                        third = xz_here * spec(1 - px, py, other)
                        total = total + third if sx > 0 else total - third
                        third = yz_here * spec(px, 1 - py, 2 + other)
                        total = total + third if sy > 0 else total - third
                    at_rows, at_columns = place(px, py)
                    out_ref[part, at_rows, at_columns] = total

    for start in range(0, columns_full, lane):
        tile(0, True, start)

    unrolled = 3
    peeled = (rows_full // sub - 1) % unrolled + 1
    for n in range(1, peeled):
        for start in range(0, columns_full, lane):
            tile(n * sub, False, start)

    def step(i, carry):
        for n in range(unrolled):
            row_start = pl.multiple_of((unrolled * i + n + peeled) * sub, sub)
            for start in range(0, columns_full, lane):
                tile(row_start, False, start)
        return carry

    lax.fori_loop(0, (rows_full // sub - peeled) // unrolled, step, 0)


def arc_angle(sine, cosine):
    size = jnp.abs(cosine)
    low, high = jnp.minimum(sine, size), jnp.maximum(sine, size)
    ratio = low / jnp.maximum(high, 1e-37)
    wide = ratio > 0.41421356
    ratio = jnp.where(wide, (ratio - 1.0) / (ratio + 1.0), ratio)
    square = ratio * ratio
    series = ((8.05374449538e-2 * square - 1.38776856032e-1) * square + 1.99777106478e-1) * square
    angle = (series - 3.33329491539e-1) * square * ratio + ratio
    angle = jnp.where(wide, angle + 0.25 * math.pi, angle)
    angle = jnp.where(sine > size, 0.5 * math.pi - angle, angle)
    return jnp.where(cosine < 0.0, math.pi - angle, angle)


def dot3(first, second):
    return first[0] * second[0] + first[1] * second[1] + first[2] * second[2]


def band_kernel(
    scale,
    magnet_ref,
    kernel_ref,
    anisotropy_ref,
    source_tables,
    field_ref,
    small_ref,
    tables,
    cells_ref,
    film_ref,
    edge_out_ref,
    edge_ref,
    send_ref,
    back_ref,
    held_ref,
    spec_ref,
    arrive_ref,
    next_ref,
    prior_ref,
    rim_out_ref,
    rim_ref,
    present_ref,
    ease_ref,
    sums_ref,
    tile_ref,
    swap_ref,
    peak_ref,
    tensor_ref,
    result_ref,
    own_sem,
    tensor_sem,
    film_send,
    film_recv,
    twin_send,
    twin_recv,
    plane_send,
    plane_recv,
    back_send,
    back_recv,
    last_send,
    last_recv,
    image_send,
    image_recv,
    rim_send,
    rim_recv,
    swap_send,
    swap_recv,
    peak_send,
    peak_recv,
    table_sem,
):
    fy_ref, fx_ref = tables[:2]
    gx_ref, gy_ref = tables[:2] if len(tables) == 2 else tables[2:]
    groups, local_planes = held_ref.shape[1], held_ref.shape[2]
    slab, columns_full = held_ref.shape[4], held_ref.shape[5]
    layer_count = cells_ref.shape[2]
    rows_full = groups * slab
    parts = groups // 2
    me = lax.axis_index("space")
    half, seat = me // parts, lax.rem(me, parts)
    partner = lax.rem(me + parts, groups)
    flip = (1 - 2 * half).astype(jnp.float32)
    row_step = 8
    images, image = lax.axis_size("image"), lax.axis_index("image")
    first, last = image == 0, image == images - 1
    shifts = (-1, 0, 1)
    routes = [
        (n, shift, d)
        for n, shift in enumerate(shifts)
        for d in range(groups)
        if shift != 0 or d != 0
    ]

    def gate(exists, action):
        if exists is None:
            action()
        else:
            pl.when(exists)(action)

    def receiver(shift):
        return None if shift == 0 else jnp.logical_not(last if shift < 0 else first)

    def sender(shift):
        return None if shift == 0 else jnp.logical_not(first if shift < 0 else last)

    def target_of(shift, d):
        return {"image": lax.rem(image - shift + images, images), "space": lax.rem(me + d, groups)}

    def remote(src, dst, send, recv, target):
        return pltpu.make_async_remote_copy(
            src_ref=src,
            dst_ref=dst,
            send_sem=send,
            recv_sem=recv,
            device_id=target if isinstance(target, dict) else {"space": target},
            device_id_type=pl.DeviceIdType.MESH,
        )

    def row_loop(step):
        def chunk(i, carry):
            step(pl.ds(pl.multiple_of(i * row_step, row_step), row_step))
            return carry

        lax.fori_loop(0, slab // row_step, chunk, 0)

    def own_copy(c):
        return pltpu.make_async_copy(magnet_ref.at[:, c], cells_ref.at[:, c], own_sem.at[c])

    def tensor_copy(q):
        return pltpu.make_async_copy(
            kernel_ref.at[:, q, pl.ds(0, rows_full + 8), pl.ds(0, columns_full + 128)],
            tensor_ref.at[pl.ds(6 * q, 6)],
            tensor_sem.at[q],
        )

    def film_copy(c):
        return remote(
            magnet_ref.at[1 - half, c], film_ref.at[c], film_send.at[c], film_recv.at[c], partner
        )

    def kernel_copies():
        body = (pl.ds(0, rows_full), pl.ds(0, columns_full))
        far = (pl.ds(rows_full, 8), pl.ds(0, columns_full + 128))
        twin = 6 * local_planes
        pieces = [(tensor_ref.at[n, *body], tensor_ref.at[twin + n, *body]) for n in (0, 3)]
        pieces += [
            (edge_out_ref, edge_ref),
            (tensor_ref.at[pl.ds(0, 3), *far], tensor_ref.at[pl.ds(twin, 3), *far]),
        ]
        pieces += [(tensor_ref.at[n, *body], tensor_ref.at[twin + n, *body]) for n in (1, 2)]
        return [
            remote(src, dst, twin_send.at[n], twin_recv.at[n], partner)
            for n, (src, dst) in enumerate(pieces)
        ]

    def pack_edges():
        rows, columns = pl.ds(0, rows_full), pl.ds(columns_full, 128)
        lane_pos = lax.broadcasted_iota(jnp.int32, (rows_full, 128), 1)
        edge = tensor_ref[0, rows, columns]
        for c in (1, 2):
            edge = jnp.where(lane_pos == c, pltpu.roll(tensor_ref[c, rows, columns], c, 1), edge)
        edge_out_ref[...] = edge

    def unpack_edges():
        rows, columns = pl.ds(0, rows_full), pl.ds(columns_full, 128)
        edge = edge_ref[...]
        for c in range(3):
            tensor_ref[6 * local_planes + c, rows, columns] = pltpu.roll(edge, 128 - c, 1) if c else edge

    def place_of(seat_index, kind):
        return lax.rem((half + kind) * parts + seat_index, groups)

    def plane_copy(c, kind, slot):
        target = lax.rem(seat + 1 + slot, parts)
        return remote(
            send_ref.at[3 if kind else c, slot],
            held_ref.at[c, place_of(seat, kind)],
            plane_send.at[c, kind, slot],
            plane_recv.at[c, kind, parts - 2 - slot],
            half * parts + target,
        )

    def plane_arrival(c, kind, slot):
        source = lax.rem(seat + 1 + slot, parts)
        return remote(
            send_ref.at[3 if kind else c, slot],
            held_ref.at[c, place_of(source, kind)],
            plane_send.at[c, kind, slot],
            plane_recv.at[c, kind, slot],
            half * parts + source,
        )

    def back_copy(c, q, kind, slot):
        target = lax.rem(seat + 1 + slot, parts)
        return remote(
            held_ref.at[c, place_of(target, kind), q],
            back_ref.at[c, kind, parts - 2 - slot, q],
            back_send.at[c, q, kind, slot],
            back_recv.at[c, q, kind, parts - 2 - slot],
            half * parts + target,
        )

    def back_arrival(c, q, kind, slot):
        source = lax.rem(seat + 1 + slot, parts)
        return remote(
            held_ref.at[c, place_of(source, kind), q],
            back_ref.at[c, kind, slot, q],
            back_send.at[c, q, kind, slot],
            back_recv.at[c, q, kind, slot],
            half * parts + source,
        )

    def last_copy(c):
        return remote(
            film_ref.at[c], arrive_ref.at[c], last_send.at[c], last_recv.at[c], partner
        )

    def ahead_copy():
        return remote(
            magnet_ref.at[1],
            prior_ref,
            image_send.at[0],
            image_recv.at[0],
            {"image": lax.rem(image + 1, images)},
        )

    def behind_copy():
        return remote(
            magnet_ref.at[0],
            next_ref,
            image_send.at[1],
            image_recv.at[1],
            {"image": lax.rem(image + images - 1, images)},
        )

    def rim_copy(side):
        return remote(
            rim_out_ref.at[side],
            rim_ref.at[side],
            rim_send.at[side],
            rim_recv.at[side],
            lax.rem(me + (1 if side == 0 else groups - 1), groups),
        )

    def swap_copy(n, shift, d, slot):
        return remote(
            tile_ref, swap_ref.at[n, slot], swap_send.at[n, d], swap_recv.at[n, d], target_of(shift, d)
        )

    def peak_copy(d, slot):
        return remote(
            tile_ref.at[pl.ds(0, 8)],
            peak_ref.at[slot],
            peak_send.at[d],
            peak_recv.at[d],
            lax.rem(me + d, groups),
        )

    def table_copy(n):
        return pltpu.make_async_copy(source_tables[n], tables[n], table_sem.at[n])

    def kernel_copies():
        body = (pl.ds(0, rows_full), pl.ds(0, columns_full))
        far = (pl.ds(rows_full, 8), pl.ds(0, columns_full + 128))
        twin = 6 * local_planes
        pieces = [(tensor_ref.at[n, *body], tensor_ref.at[twin + n, *body]) for n in (0, 3)]
        pieces += [
            (edge_out_ref, edge_ref),
            (tensor_ref.at[pl.ds(0, 3), *far], tensor_ref.at[pl.ds(twin, 3), *far]),
        ]
        pieces += [(tensor_ref.at[n, *body], tensor_ref.at[twin + n, *body]) for n in (1, 2)]
        return [
            remote(src, dst, twin_send.at[n], twin_recv.at[n], partner)
            for n, (src, dst) in enumerate(pieces)
        ]

    def pack_edges():
        rows, columns = pl.ds(0, rows_full), pl.ds(columns_full, 128)
        lane_pos = lax.broadcasted_iota(jnp.int32, (rows_full, 128), 1)
        edge = tensor_ref[0, rows, columns]
        for c in (1, 2):
            edge = jnp.where(lane_pos == c, pltpu.roll(tensor_ref[c, rows, columns], c, 1), edge)
        edge_out_ref[...] = edge

    def unpack_edges():
        rows, columns = pl.ds(0, rows_full), pl.ds(columns_full, 128)
        edge = edge_ref[...]
        for c in range(3):
            tensor_ref[6 * local_planes + c, rows, columns] = pltpu.roll(edge, 128 - c, 1) if c else edge

    def last_copy(c):
        return remote(
            film_ref.at[c], arrive_ref.at[c], last_send.at[c], last_recv.at[c], partner
        )

    def ahead_copy():
        return remote(
            magnet_ref.at[1],
            prior_ref,
            image_send.at[0],
            image_recv.at[0],
            {"image": lax.rem(image + 1, images)},
        )

    def behind_copy():
        return remote(
            magnet_ref.at[0],
            next_ref,
            image_send.at[1],
            image_recv.at[1],
            {"image": lax.rem(image + images - 1, images)},
        )

    def rim_copy(side):
        return remote(
            rim_out_ref.at[side],
            rim_ref.at[side],
            rim_send.at[side],
            rim_recv.at[side],
            lax.rem(me + (1 if side == 0 else groups - 1), groups),
        )

    def swap_copy(n, shift, d, slot):
        return remote(
            tile_ref, swap_ref.at[n, slot], swap_send.at[n, d], swap_recv.at[n, d], target_of(shift, d)
        )

    def peak_copy(d, slot):
        return remote(
            tile_ref.at[pl.ds(0, 8)],
            peak_ref.at[slot],
            peak_send.at[d],
            peak_recv.at[d],
            lax.rem(me + d, groups),
        )

    def table_copy(n):
        return pltpu.make_async_copy(source_tables[n], tables[n], table_sem.at[n])

    def force_copy(i):
        return pltpu.make_async_copy(field_ref.at[i], force_ref.at[i], force_sem.at[i])

    def transform_layers(c, kind):
        place = place_of(seat, kind)

        def variant(here):
            def step(rows):
                if kind == 0:
                    layers = [cells_ref[half, c, z, rows, :] for z in range(layer_count)]
                else:
                    layers = [film_ref[c, z, rows, :] for z in range(layer_count)]
                layers = [v * flip if z % 2 else v for z, v in enumerate(layers)]
                spectrum = layers_to_spectrum(layers)
                for k in range(layer_count):
                    target, q = k // local_planes, k % local_planes
                    slot = (target - here) % parts - 1
                    for part in range(2):
                        if target == here:
                            held_ref[c, place, q, part, rows, :] = spectrum[k][part]
                        else:
                            send_ref[3 if kind else c, slot, q, part, rows, :] = spectrum[k][part]

            row_loop(step)

        for here in range(parts):
            pl.when(seat == here)(functools.partial(variant, here))
        for slot in range(parts - 1):
            plane_copy(c, kind, slot).start()

    def transform_planes(c, kind):
        place = place_of(seat, kind)

        def variant(here):
            def step(rows):
                spectrum = []
                for k in range(layer_count):
                    source, q = k // local_planes, k % local_planes
                    slot = (source - here) % parts - 1
                    if source == here:
                        spectrum.append(
                            [held_ref[c, place, q, part, rows, :] for part in range(2)]
                        )
                    else:
                        spectrum.append(
                            [back_ref[c, kind, slot, q, part, rows, :] for part in range(2)]
                        )
                for z, value in enumerate(spectrum_to_layers(spectrum)):
                    value = value * (scale * flip if z % 2 else scale)
                    if kind == 0:
                        field_ref[half, c, z, rows, :] = field_ref[half, c, z, rows, :] + value
                    else:
                        film_ref[c, z, rows, :] = value

            row_loop(step)

        for here in range(parts):
            pl.when(seat == here)(functools.partial(variant, here))

    def fill_rims():
        def step(f, carry):
            i, c = f // 3, lax.rem(f, 3)
            for side in range(2):
                row = slab - 1 if side == 0 else 0
                rim_out_ref[side, i, c] = jnp.concatenate(
                    [cells_ref[i, c, z, row : row + 1, :] for z in range(layer_count)], axis=0
                )
            return carry

        lax.fori_loop(0, 6, step, 0)
        row_pos = lax.broadcasted_iota(jnp.int32, (slab, columns_full), 0) + me * slab
        column_pos = lax.broadcasted_iota(jnp.int32, (slab, columns_full), 1)
        faces = [row_pos == 0, row_pos == rows_full - 1]
        faces += [column_pos == 0, column_pos == columns_full - 1]
        present_ref[...] = 6.0 - sum(jnp.where(face, 1.0, 0.0) for face in faces)
        for side in range(2):
            open_side = me != groups - 1 if side == 0 else me != 0

            @pl.when(open_side)
            def _():
                rim_copy(side).start()

            no_source = me == 0 if side == 0 else me == groups - 1

            @pl.when(no_source)
            def _():
                rim_ref[side] = jnp.zeros(rim_ref.shape[1:], jnp.float32)

    def wait_rims():
        for side in range(2):
            has_source = me != 0 if side == 0 else me != groups - 1

            @pl.when(has_source)
            def _():
                rim_copy(side).wait_recv()

    def local_fields(i):
        row_pos = lax.broadcasted_iota(jnp.int32, (slab, columns_full), 0)
        column_pos = lax.broadcasted_iota(jnp.int32, (slab, columns_full), 1)

        def step(z, carry):
            below, above = jnp.maximum(z - 1, 0), jnp.minimum(z + 1, layer_count - 1)
            has_below = (z > 0).astype(jnp.float32)
            has_above = (z < layer_count - 1).astype(jnp.float32)
            present = present_ref[...] - (2.0 - has_below - has_above)
            tilt = []
            for c in range(3):
                cells = cells_ref[i, c, z]
                x_plus = jnp.where(
                    row_pos == slab - 1,
                    rim_ref[1, i, c, pl.ds(z, 1), :],
                    pltpu.roll(cells, slab - 1, 0),
                )
                x_minus = jnp.where(
                    row_pos == 0, rim_ref[0, i, c, pl.ds(z, 1), :], pltpu.roll(cells, 1, 0)
                )
                y_plus = jnp.where(
                    column_pos == columns_full - 1, 0.0, pltpu.roll(cells, columns_full - 1, 1)
                )
                y_minus = jnp.where(column_pos == 0, 0.0, pltpu.roll(cells, 1, 1))
                around = x_plus + x_minus + y_plus + y_minus
                around = around + has_above * cells_ref[i, c, above] + has_below * cells_ref[i, c, below]
                part = exchange_strength * (around - present * cells)
                if c == 0:
                    tilt.append(x_plus - x_minus)
                    field_ref[i, 0, z] = part
                elif c == 1:
                    tilt.append(y_plus - y_minus)
                    field_ref[i, 1, z] = part
                else:
                    ease = ease_ref[...] * cells
                    field_ref[i, 2, z] = part + (ease - chiral_strength * (tilt[0] + tilt[1]))
                    field_ref[i, 0, z] = field_ref[i, 0, z] + chiral_strength * (x_plus - x_minus)
                    field_ref[i, 1, z] = field_ref[i, 1, z] + chiral_strength * (y_plus - y_minus)
            return carry

        lax.fori_loop(0, layer_count, step, 0)

    lane = columns_full

    def cell_loop(step, carry):
        unrolled = min(4, slab // row_step)
        steps = slab // (unrolled * row_step)

        def chunk(index, carry):
            z = index // steps
            start = lax.rem(index, steps) * unrolled * row_step
            for n in range(unrolled):
                carry = step(z, pl.multiple_of(start + n * row_step, row_step), carry)
            return carry

        return lax.fori_loop(0, layer_count * steps, chunk, carry)

    def zeros(count):
        return tuple(jnp.zeros((row_step, lane), jnp.float32) for _ in range(count))

    def tangent_rows(z, start):
        return pl.ds(pl.multiple_of(z * slab + start, row_step), row_step)

    def neighbour_sums():
        @pl.when(jnp.logical_not(first))
        def _():
            ahead_copy().wait_recv()

        @pl.when(first)
        def _():
            for c in range(3):
                prior_ref[c] = cells_ref[0, c]

        @pl.when(jnp.logical_not(last))
        def _():
            behind_copy().wait_recv()

        @pl.when(last)
        def _():
            for c in range(3):
                next_ref[c] = cells_ref[1, c]

        for i in range(2):

            def step(z, start, carry):
                rows = pl.ds(start, row_step)
                here = [cells_ref[i, c, z, rows, :] for c in range(3)]
                if i == 0:
                    ahead = [cells_ref[1, c, z, rows, :] for c in range(3)]
                    behind = [prior_ref[c, z, rows, :] for c in range(3)]
                else:
                    ahead = [next_ref[c, z, rows, :] for c in range(3)]
                    behind = [cells_ref[0, c, z, rows, :] for c in range(3)]
                normal = [
                    here[1] * ahead[2] - here[2] * ahead[1],
                    here[2] * ahead[0] - here[0] * ahead[2],
                    here[0] * ahead[1] - here[1] * ahead[0],
                ]
                angle = arc_angle(jnp.sqrt(dot3(normal, normal)), dot3(here, ahead))
                ahead = [ahead[c] - here[c] for c in range(3)]
                behind = [here[c] - behind[c] for c in range(3)]
                ahead_on, behind_on = dot3(ahead, here), dot3(behind, here)
                ahead = [ahead[c] - ahead_on * here[c] for c in range(3)]
                behind = [behind[c] - behind_on * here[c] for c in range(3)]
                for c in range(3):
                    place = tangent_rows(z, start)
                    spec_ref[0, 3 * i + c, place, 0:columns_full] = ahead[c]
                    spec_ref[0, 3 * i + c, place, columns_full : 2 * columns_full] = behind[c]
                values = (
                    angle * angle,
                    dot3(ahead, ahead),
                    dot3(ahead, behind),
                    dot3(behind, behind),
                )
                return tuple(total + value for total, value in zip(carry, values))

            totals = cell_loop(step, zeros(4))
            for k in range(4):
                sums_ref[i, k + 1] = totals[k]

    def field_sums(i, c, arrived):
        def step(z, start, carry):
            rows = pl.ds(start, row_step)
            place = tangent_rows(z, start)
            field = field_ref[i, c, z, rows, :]
            if arrived:
                field = field + arrive_ref[c, z, rows, :]
                field_ref[i, c, z, rows, :] = field
            values = (
                cells_ref[i, c, z, rows, :] * field,
                field * spec_ref[0, 3 * i + c, place, 0:columns_full],
                field * spec_ref[0, 3 * i + c, place, columns_full : 2 * columns_full],
            )
            return tuple(total + value for total, value in zip(carry, values))

        totals = cell_loop(step, zeros(3))
        for k, slot in enumerate((0, 5, 6)):
            sums_ref[i, slot] = totals[k] if c == 0 else sums_ref[i, slot] + totals[k]

    barrier = pltpu.get_barrier_semaphore()
    for n, shift, d in routes:
        signal = functools.partial(
            pl.semaphore_signal,
            barrier,
            inc=1,
            device_id=target_of(shift, d),
            device_id_type=pl.DeviceIdType.MESH,
        )
        gate(receiver(shift), signal)
    for c in range(3):
        own_copy(c).start()
    for n in range(len(tables)):
        table_copy(n).start()

    def spread(r, carry):
        ease_ref[pl.ds(r, 1), :] = jnp.full((1, columns_full), 2.0 * anisotropy_ref[r])
        return carry

    lax.fori_loop(0, slab, spread, 0)
    ends = first.astype(jnp.int32) + last.astype(jnp.int32)
    pl.semaphore_wait(barrier, len(routes) - groups * ends)
    film_copy(0).start()

    @pl.when(jnp.logical_not(last))
    def _():
        ahead_copy().start()

    @pl.when(jnp.logical_not(first))
    def _():
        behind_copy().start()

    for c in range(3):
        own_copy(c).wait()
    fill_rims()
    for c in range(1, 3):
        film_copy(c).start()

    for q in range(local_planes):
        tensor_copy(q).start()

    for c in range(3):
        transform_layers(c, 0)
    for n in range(len(tables)):
        table_copy(n).wait()
    tensor_copy(0).wait()

    @pl.when(seat == 0)
    def _():
        pack_edges()
        for copy in kernel_copies():
            copy.start()

    for c in range(3):
        film_copy(c).wait_recv()
        if c > 0:
            for slot in range(parts - 1):
                plane_copy(c - 1, 1, slot).wait_send()
        transform_layers(c, 1)
        for kind in range(2):
            for slot in range(parts - 1):
                plane_arrival(c, kind, slot).wait_recv()

        def forward(i, carry):
            q = i
            fy = jnp.concatenate([fy_ref[0], fy_ref[0], fy_ref[1]], axis=0)
            fx = jnp.concatenate([fx_ref[0], fx_ref[0], fx_ref[1]], axis=1)
            cells = jnp.concatenate(
                [held_ref[c, g, q, part] for part in range(2) for g in range(groups)], axis=0
            )
            lines = dot32(three_limbs(cells, 1), fy)
            for part in range(2):
                spec_ref[q, 2 * c + part] = dot32(
                    fx, three_limbs(lines[part * rows_full : (part + 1) * rows_full], 0)
                )
            return carry

        lax.fori_loop(0, local_planes, forward, 0)
        if c == 0:
            wait_rims()
        if c < 2:
            local_fields(c)

    for q in range(1, local_planes):
        tensor_copy(q).wait()

    for c in range(3):

        def backward(i, carry):
            q = local_planes - 1 - i
            twin = (seat == 0) & (q == 0)

            @pl.when(twin)
            def _():
                for copy in kernel_copies()[:4] if c == 0 else kernel_copies()[c + 3 : c + 4]:
                    copy.wait_recv()
                if c == 0:
                    unpack_edges()

            second = jnp.where(twin, local_planes, q)
            kernels = (tensor_ref.at[pl.ds(6 * q, 6)], tensor_ref.at[pl.ds(6 * second, 4)])
            tensor_part(c, spec_ref.at[q], kernels, result_ref)
            gx = jnp.concatenate([gx_ref[0], gx_ref[0], gx_ref[1]], axis=1)
            gy = jnp.concatenate([gy_ref[0], gy_ref[0], gy_ref[1]], axis=0)
            lines = [dot32(gx, three_limbs(result_ref[part], 0)) for part in range(2)]
            cells = dot32(three_limbs(jnp.concatenate(lines, axis=0), 1), gy)
            for part in range(2):
                for g in range(groups):
                    start = part * rows_full + g * slab
                    held_ref[c, g, q, part] = cells[start : start + slab]
            for kind in (1, 0):
                for slot in range(parts - 1):
                    back_copy(c, q, kind, slot).start()

            return carry

        lax.fori_loop(0, local_planes, backward, 0)
        for kind in (1, 0):
            for q in range(local_planes):
                for slot in range(parts - 1):
                    back_arrival(c, q, kind, slot).wait_recv()
            transform_planes(c, kind)
            if kind == 1:
                last_copy(c).start()

    neighbour_sums()
    for c in range(3):
        field_sums(half, c, False)
    for c in range(3):
        last_copy(c).wait_recv()
        field_sums(1 - half, c, True)

    rows = [
        jnp.sum(sums_ref[i, k], axis=0, keepdims=True) for i in range(2) for k in range(7)
    ] + [jnp.zeros((1, lane), jnp.float32)] * 2
    tile = jnp.sum(jnp.concatenate(rows, axis=0), axis=1, keepdims=True)
    tile_ref[...] = jnp.broadcast_to(tile, tile_ref.shape)
    for n, shift, d in routes:
        gate(receiver(shift), swap_copy(n, shift, d, me).start)
    swap_ref[1, me] = tile_ref[...]
    for n, end in ((0, first), (2, last)):

        @pl.when(end)
        def _():
            swap_ref[n] = jnp.zeros(swap_ref.shape[1:], jnp.float32)

    for n, shift, d in routes:
        gate(sender(shift), swap_copy(n, shift, d, lax.rem(me + groups - d, groups)).wait_recv)
    totals = []
    for n in range(3):
        total = swap_ref[n, 0]
        for g in range(1, groups):
            total = total + swap_ref[n, g]
        totals.append(total)

    def entry(n, i, k):
        return totals[n][7 * i + k : 7 * i + k + 1]

    cell_count = float(layer_count * rows_full * columns_full)
    energies = [-0.5 * entry(*at, 0) for at in ((0, 1), (1, 0), (1, 1), (2, 0))]
    distances = [jnp.sqrt(entry(*at, 1) / cell_count) for at in ((0, 1), (1, 0), (1, 1))]
    pulls = []
    for i in range(2):
        weight_next, weight_prior = tangent_weights(energies[i + 1], energies[i + 2], energies[i])
        length_square = (
            weight_next * weight_next * entry(1, i, 2)
            + 2.0 * weight_next * weight_prior * entry(1, i, 3)
            + weight_prior * weight_prior * entry(1, i, 4)
        )
        drive = weight_next * entry(1, i, 5) + weight_prior * entry(1, i, 6)
        size = jnp.sqrt(jnp.maximum(length_square, 0.0) / cell_count + epsilon)
        spring = spring_strength * (distances[i + 1] - distances[i])
        pull = (spring - drive / (cell_count * size)) / size
        pulls.append((pull * weight_next, pull * weight_prior))
    for n, shift, d in routes:
        gate(receiver(shift), swap_copy(n, shift, d, me).wait_send)
    peaks = []
    for i in range(2):
        end = first if i == 0 else last
        ahead_pull, behind_pull = [
            jnp.concatenate([jnp.broadcast_to(pull, (row_step, 128))] * (lane // 128), axis=1)
            for pull in pulls[i]
        ]

        def step(z, start, peak):
            rows = pl.ds(start, row_step)
            place = tangent_rows(z, start)
            here = [cells_ref[i, c, z, rows, :] for c in range(3)]
            force = []
            for c in range(3):
                ahead = spec_ref[0, 3 * i + c, place, 0:columns_full]
                behind = spec_ref[0, 3 * i + c, place, columns_full : 2 * columns_full]
                field = field_ref[i, c, z, rows, :]
                force.append(field + ahead_pull * ahead + behind_pull * behind)
            along = dot3(force, here)
            force = [jnp.where(end, 0.0, force[c] - along * here[c]) for c in range(3)]
            for c in range(3):
                field_ref[i, c, z, rows, :] = force[c]
            return (jnp.maximum(peak[0], dot3(force, force)),)

        (peak,) = cell_loop(step, zeros(1))
        peaks.append(jnp.max(peak, axis=0, keepdims=True))
    peak = jnp.concatenate(peaks + [jnp.zeros((6, lane), jnp.float32)], axis=0)
    peak = jnp.broadcast_to(jnp.max(peak, axis=1, keepdims=True), (8, 128))
    tile_ref[0:8] = peak
    for d in range(1, groups):
        peak_copy(d, me).start()
    peak_ref[me] = peak
    for d in range(1, groups):
        peak_copy(d, lax.rem(me + groups - d, groups)).wait_recv()
    largest = peak_ref[0]
    for g in range(1, groups):
        largest = jnp.maximum(largest, peak_ref[g])
    moves = jnp.minimum(step_limit, rotation_limit / (jnp.sqrt(largest) + epsilon))
    energy = jnp.concatenate(energies[1:3], axis=0) / cell_count
    small_ref[...] = jnp.concatenate([moves[0:2], energy, jnp.zeros((4, 128), jnp.float32)], axis=0)
    for d in range(1, groups):
        peak_copy(d, me).wait_send()
    for c in range(3):
        film_copy(c).wait_send()
        last_copy(c).wait_send()
        for kind in range(2):
            for slot in range(parts - 1):
                if kind == 0 or c == 2:
                    plane_copy(c, kind, slot).wait_send()
                for q in range(local_planes):
                    back_copy(c, q, kind, slot).wait_send()

    @pl.when(seat == 0)
    def _():
        for copy in kernel_copies():
            copy.wait_send()

    for side in range(2):
        open_side = me != groups - 1 if side == 0 else me != 0

        @pl.when(open_side)
        def _():
            rim_copy(side).wait_send()

    @pl.when(jnp.logical_not(last))
    def _():
        ahead_copy().wait_send()

    @pl.when(jnp.logical_not(first))
    def _():
        behind_copy().wait_send()


def band_step(magnet, anisotropy, kernel):
    layer_count, row_count, column_count = magnet.shape[2:]
    groups = lax.axis_size("space")
    local_planes = 2 * layer_count // groups
    full_rows = row_count * groups
    slots = groups // 2 - 1
    table_y = parity_table(column_count)
    table_x = parity_table(full_rows)
    square = full_rows == column_count
    tables = [table_limbs(t) for t in (table_y, table_x.T, table_x, table_y.T)][: 2 if square else 4]

    def entry(magnet_ref, kernel_ref, anisotropy_ref, *refs):
        count = len(tables)
        sources, outs = refs[:count], refs[count : count + 2]
        held, rest = refs[count + 2 : 2 * count + 2], refs[2 * count + 2 :]
        scale = -4.0 / padded_cells
        band_kernel(
            scale, magnet_ref, kernel_ref, anisotropy_ref, sources, *outs, held, *rest
        )

    slab = (row_count, column_count)
    film = (layer_count,) + slab
    block = (local_planes, 2) + slab
    anywhere = pl.BlockSpec(memory_space=pl.ANY)
    inside = pl.BlockSpec(memory_space=pltpu.VMEM)
    dots = 6 * local_planes * 4 * full_rows * column_count * 3 * (full_rows + column_count // 2)
    padded_cells = 8 * layer_count * full_rows * column_count
    signals = pltpu.SemaphoreType.DMA
    scratch = [
        (2, 3) + film,
        (3,) + film,
        (full_rows, 128),
        (full_rows, 128),
        (4, slots) + block,
        (3, 2, slots) + block,
        (3, groups) + block,
        (local_planes, 6, 2 * full_rows, 2 * column_count),
        (3,) + film,
        (3,) + film,
        (3,) + film,
        (2, 2, 3, layer_count, column_count),
        (2, 2, 3, layer_count, column_count),
        slab,
        slab,
        (2, 7, 8, column_count),
        (16, 128),
        (3, groups, 16, 128),
        (groups, 8, 128),
        (6 * local_planes + 4, full_rows + 8, column_count + 128),
    ]
    semaphores = [
        (3,),
        (local_planes,),
        (3,),
        (3,),
        (6,),
        (6,),
        (3, 2, slots),
        (3, 2, slots),
        (3, local_planes, 2, slots),
        (3, local_planes, 2, slots),
        (3,),
        (3,),
        (2,),
        (2,),
        (2,),
        (2,),
        (3, groups),
        (3, groups),
        (groups,),
        (groups,),
        (len(tables),),
    ]
    return pl.pallas_call(
        entry,
        in_specs=[anywhere, anywhere, pl.BlockSpec(memory_space=pltpu.SMEM)]
        + [anywhere] * len(tables),
        out_specs=[inside, inside],
        out_shape=[
            pltpu.VMEM(magnet.shape, jnp.float32),
            jax.ShapeDtypeStruct((8, 128), jnp.float32),
        ],
        scratch_shapes=[pltpu.VMEM(t.shape, jnp.bfloat16) for t in tables]
        + [pltpu.VMEM(dims, jnp.float32) for dims in scratch]
        + [pltpu.VMEM((2, 2 * full_rows, 2 * column_count), jnp.float32)]
        + [signals(dims) for dims in semaphores],
        compiler_params=pltpu.CompilerParams(
            vmem_limit_bytes=67043328 - 4 * magnet.size, collective_id=0, has_side_effects=True
        ),
        cost_estimate=pl.CostEstimate(
            flops=4 * dots, bytes_accessed=4 * magnet.size * 4, transcendentals=0
        ),
        name="band_kernel",
    )(magnet, kernel, anisotropy, *[jnp.asarray(t) for t in tables])


def move_kernel(
    small_ref,
    magnet_ref,
    force_ref,
    updated_ref,
    out_ref,
    energy_ref,
    cells_ref,
    cells_sem,
    updated_sem,
    out_sem,
):
    images, _, layer_count, slab, columns = cells_ref.shape
    pieces = updated_sem.shape[1]
    layers = layer_count // pieces

    def piece_copy(src, dst, sem, i, k):
        part = pl.ds(k * layers, layers)
        return pltpu.make_async_copy(src.at[i, :, part], dst.at[i, :, part], sem.at[i, k])

    def out_copy(i):
        return pltpu.make_async_copy(force_ref.at[i], out_ref.at[i], out_sem.at[i])

    places = [(i, k) for i in range(images) for k in range(pieces)]
    for i, k in places:
        piece_copy(magnet_ref, cells_ref, cells_sem, i, k).start()
    for i in range(images):
        out_copy(i).start()
    for n in range(images):
        energy_ref[n] = jnp.max(small_ref[n + 2 : n + 3, :])
    row_step = 8
    unrolled = min(4, slab // row_step)
    steps = slab // (unrolled * row_step)
    for i, k in places:
        move = jnp.broadcast_to(small_ref[i : i + 1, :], (row_step, 128))
        move = jnp.concatenate([move] * (columns // 128), axis=1)

        piece_copy(magnet_ref, cells_ref, cells_sem, i, k).wait()

        def chunk(index, carry):
            z = k * layers + index // steps
            for n in range(unrolled):
                start = (lax.rem(index, steps) * unrolled + n) * row_step
                rows = pl.ds(pl.multiple_of(start, row_step), row_step)
                moved = [
                    cells_ref[i, c, z, rows, :] + move * force_ref[i, c, z, rows, :]
                    for c in range(3)
                ]
                inverse = lax.rsqrt(dot3(moved, moved))
                for c in range(3):
                    cells_ref[i, c, z, rows, :] = inverse * moved[c]
            return carry

        lax.fori_loop(0, layers * steps, chunk, 0)
        piece_copy(cells_ref, updated_ref, updated_sem, i, k).start()
    for i in range(images):
        out_copy(i).wait()
    for i, k in places:
        piece_copy(cells_ref, updated_ref, updated_sem, i, k).wait()


def move_images(magnet, force, small):
    images, _, layer_count = magnet.shape[:3]
    pieces = math.gcd(layer_count, 4)
    inside = pl.BlockSpec(memory_space=pltpu.VMEM)
    anywhere = pl.BlockSpec(memory_space=pl.ANY)
    return pl.pallas_call(
        move_kernel,
        in_specs=[inside, anywhere, inside],
        out_specs=[anywhere, anywhere, pl.BlockSpec(memory_space=pltpu.SMEM)],
        out_shape=[
            jax.ShapeDtypeStruct(magnet.shape, jnp.float32),
            jax.ShapeDtypeStruct(magnet.shape, jnp.float32),
            jax.ShapeDtypeStruct((images,), jnp.float32),
        ],
        scratch_shapes=[
            pltpu.VMEM(magnet.shape, jnp.float32),
            pltpu.SemaphoreType.DMA((images, pieces)),
            pltpu.SemaphoreType.DMA((images, pieces)),
            pltpu.SemaphoreType.DMA((images,)),
        ],
        name="move_kernel",
    )(small, magnet, pltpu.with_memory_space_constraint(force, pltpu.VMEM))


def body(magnet, anisotropy, kernel):
    force, small = band_step(magnet, anisotropy, kernel)
    return move_images(magnet, force, small)


def solution(mesh):
    in_specs = (P("image", None, None, "space", None), P("space"), P(None, "space", None, None))
    out_specs = (
        P("image", None, None, "space", None),
        P("image", None, None, "space", None),
        P("image"),
    )
    return jax.shard_map(body, mesh=mesh, in_specs=in_specs, out_specs=out_specs, check_vma=False)
```

```python
import functools
import math

import jax
import jax.numpy as jnp
import numpy as np
from jax import lax
from jax.experimental import pallas as pl
from jax.experimental.pallas import tpu as pltpu
from jax.sharding import PartitionSpec as P

exchange_strength = 0.25
chiral_strength = 0.3
spring_strength = 10.0
step_limit = 1.0
rotation_limit = 0.5
epsilon = 1e-06


def tangent_weights(energy_total, energy_next, energy_prior):
    rise_next = energy_next - energy_total
    rise_prior = energy_total - energy_prior
    upward = (rise_next > 0) & (rise_prior > 0)
    downward = (rise_next < 0) & (rise_prior < 0)
    larger = jnp.maximum(jnp.abs(rise_next), jnp.abs(rise_prior))
    smaller = jnp.minimum(jnp.abs(rise_next), jnp.abs(rise_prior))
    toward_next = energy_next > energy_prior
    weight_next = jnp.where(
        upward, 1.0, jnp.where(downward, 0.0, jnp.where(toward_next, larger, smaller))
    )
    weight_prior = jnp.where(
        upward, 0.0, jnp.where(downward, 1.0, jnp.where(toward_next, smaller, larger))
    )
    return (weight_next, weight_prior)


def split_limbs(values):
    upper = values.astype(jnp.bfloat16)
    return upper, (values - upper.astype(jnp.float32)).astype(jnp.bfloat16)


def table_limbs(table):
    upper = table.astype(np.float32).astype(jnp.bfloat16)
    lower = (table - upper.astype(np.float64)).astype(np.float32).astype(jnp.bfloat16)
    return np.stack([upper, lower])


def parity_table(count):
    position = np.arange(count)[:, None]
    slot = np.arange(count)[None, :]
    turn = np.pi / count
    even_part = np.cos(turn * (position * slot % (2 * count)))
    odd_part = np.sin(turn * (position * slot % (2 * count)))
    odd_part[:, 0] = np.cos(turn * (position[:, 0] * count % (2 * count)))
    table = np.concatenate([even_part, odd_part], axis=1)
    table[:, [0, count]] *= math.sqrt(0.5)
    return table


def half_table(count):
    place = np.arange(count)
    angle = np.pi * (place[:, None] * place[None, :] % (2 * count)) / count
    cosine, sine = np.cos(angle), np.sin(angle)
    cosine[np.abs(cosine) < 1e-12] = 0.0
    sine[np.abs(sine) < 1e-12] = 0.0
    return cosine, sine


def weighted(terms):
    total = None
    for weight, value in terms:
        weight = float(weight)
        if weight == 0.0:
            continue
        if total is None:
            total = value if weight == 1.0 else -value if weight == -1.0 else weight * value
        elif weight == 1.0:
            total = total + value
        elif weight == -1.0:
            total = total - value
        else:
            total = total + weight * value
    return total


def layers_to_spectrum(layers):
    count = len(layers)
    half = count // 2
    cosine, sine = half_table(count)
    sums = {z: layers[z] + layers[count - z] for z in range(1, half)}
    gaps = {z: layers[z] - layers[count - z] for z in range(1, half)}
    spectrum = []
    for k in range(count):
        near, far = (sums, gaps) if k % 2 == 0 else (gaps, sums)
        re = weighted(
            [(1.0, layers[0]), (cosine[half, k], layers[half])]
            + [(cosine[z, k], near[z]) for z in range(1, half)]
        )
        if k == 0:
            im = weighted(
                [(1.0, layers[0]), ((-1.0) ** half, layers[half])]
                + [((-1.0) ** z, near[z]) for z in range(1, half)]
            )
        else:
            im = weighted(
                [(-sine[half, k], layers[half])] + [(-sine[z, k], far[z]) for z in range(1, half)]
            )
        spectrum.append((re, im))
    return spectrum


def spectrum_to_layers(spectrum):
    count = len(spectrum)
    half = count // 2
    cosine, sine = half_table(count)
    layers = [None] * count
    evens, odds = range(2, count, 2), range(1, count, 2)
    ground = [spectrum[0][0] + spectrum[0][1], spectrum[0][0] - spectrum[0][1]]
    layers[0] = weighted([(1.0, ground[0])] + [(2.0, spectrum[k][0]) for k in range(1, count)])
    layers[half] = weighted(
        [(1.0, ground[half % 2])]
        + [(2.0 * cosine[half, k], spectrum[k][0]) for k in range(1, count)]
        + [(-2.0 * sine[half, k], spectrum[k][1]) for k in range(1, count)]
    )
    for z in range(1, half):
        even_re = weighted(
            [(1.0, ground[z % 2])] + [(2.0 * cosine[z, k], spectrum[k][0]) for k in evens]
        )
        odd_re = weighted([(2.0 * cosine[z, k], spectrum[k][0]) for k in odds])
        even_im = weighted([(2.0 * sine[z, k], spectrum[k][1]) for k in evens])
        odd_im = weighted([(2.0 * sine[z, k], spectrum[k][1]) for k in odds])
        layers[z] = (even_re - odd_im) + (odd_re - even_im)
        layers[count - z] = (even_re - odd_im) - (odd_re - even_im)
    return layers


def dot32(left, right):
    return jnp.dot(left, right, preferred_element_type=jnp.float32)


def three_limbs(values, axis):
    upper, lower = split_limbs(values)
    return jnp.concatenate([upper, lower, upper], axis=axis)


def tensor_part(c, spec_ref, kernel_refs, out_ref):
    rows_full, columns_full = out_ref.shape[1] // 2, out_ref.shape[2] // 2
    lane = 128
    sub = 8
    top = lax.broadcasted_iota(jnp.int32, (sub, lane), 0) == 0
    left = lax.broadcasted_iota(jnp.int32, (sub, lane), 1) == 0

    def tile(row_start, first_row, start):
        rows = pl.ds(row_start, sub)
        columns = slice(start, start + lane)
        edge_columns = slice(columns_full, columns_full + lane)
        first_column = start == 0

        def loaded(component, part=0):
            kernel_ref = kernel_refs[part]
            body = kernel_ref[component, rows, columns]
            side = kernel_ref[component, rows, edge_columns] if first_column else None
            if not first_row:
                return body, side, None, None
            far = pl.ds(rows_full, 1)
            body_far = kernel_ref[component, far, columns]
            side_far = kernel_ref[component, far, edge_columns] if first_column else None
            return body, side, body_far, side_far

        def pick(parts, odd_x, odd_y):
            body, side, body_far, side_far = parts
            mixed = jnp.where(left, side, body) if odd_y and first_column else body
            if odd_x and first_row:
                far = body_far
                if odd_y and first_column:
                    far = jnp.where(left[:1], side_far, far)
                mixed = jnp.where(top, far, mixed)
            return mixed

        own = [loaded(c, part) for part in range(2)]
        k_xy = [pick(loaded(3, part), 0, 0) if c < 2 else None for part in range(2)]
        k_xz = loaded(4) if c != 1 else None
        k_yz = loaded(5) if c != 0 else None

        def place(px, py):
            offset = py * columns_full + start
            return pl.ds(row_start + px * rows_full, sub), slice(offset, offset + lane)

        def spec(px, py, f):
            at_rows, at_columns = place(px, py)
            return spec_ref[f, at_rows, at_columns]

        for px in range(2):
            for py in range(2):
                own_here = [pick(own[part], px, py) for part in range(2)]
                xz_here = pick(k_xz, 0, py) if c != 1 else None
                yz_here = pick(k_yz, px, 0) if c != 0 else None
                for part in range(2):
                    turn = 1.0 if part else -1.0
                    sx = turn if px else -turn
                    sy = turn if py else -turn
                    other = 1 - part
                    total = own_here[part] * spec(px, py, 2 * c + part)
                    if c < 2:
                        across = k_xy[part] * spec(1 - px, 1 - py, 2 * (1 - c) + part)
                        total = total - across if px == py else total + across
                    if c == 0:
                        third = xz_here * spec(1 - px, py, 4 + other)
                        total = total + third if sx > 0 else total - third
                    elif c == 1:
                        third = yz_here * spec(px, 1 - py, 4 + other)
                        total = total + third if sy > 0 else total - third
                    else:
                        third = xz_here * spec(1 - px, py, other)
                        total = total + third if sx > 0 else total - third
                        third = yz_here * spec(px, 1 - py, 2 + other)
                        total = total + third if sy > 0 else total - third
                    at_rows, at_columns = place(px, py)
                    out_ref[part, at_rows, at_columns] = total

    for start in range(0, columns_full, lane):
        tile(0, True, start)

    unrolled = 3
    peeled = (rows_full // sub - 1) % unrolled + 1
    for n in range(1, peeled):
        for start in range(0, columns_full, lane):
            tile(n * sub, False, start)

    def step(i, carry):
        for n in range(unrolled):
            row_start = pl.multiple_of((unrolled * i + n + peeled) * sub, sub)
            for start in range(0, columns_full, lane):
                tile(row_start, False, start)
        return carry

    lax.fori_loop(0, (rows_full // sub - peeled) // unrolled, step, 0)


def arc_angle(sine, cosine):
    size = jnp.abs(cosine)
    low, high = jnp.minimum(sine, size), jnp.maximum(sine, size)
    ratio = low / jnp.maximum(high, 1e-37)
    wide = ratio > 0.41421356
    ratio = jnp.where(wide, (ratio - 1.0) / (ratio + 1.0), ratio)
    square = ratio * ratio
    series = ((8.05374449538e-2 * square - 1.38776856032e-1) * square + 1.99777106478e-1) * square
    angle = (series - 3.33329491539e-1) * square * ratio + ratio
    angle = jnp.where(wide, angle + 0.25 * math.pi, angle)
    angle = jnp.where(sine > size, 0.5 * math.pi - angle, angle)
    return jnp.where(cosine < 0.0, math.pi - angle, angle)


def dot3(first, second):
    return first[0] * second[0] + first[1] * second[1] + first[2] * second[2]


def band_kernel(
    scale,
    magnet_ref,
    kernel_ref,
    anisotropy_ref,
    source_tables,
    field_ref,
    small_ref,
    tables,
    cells_ref,
    film_ref,
    edge_out_ref,
    edge_ref,
    send_ref,
    back_ref,
    held_ref,
    spec_ref,
    arrive_ref,
    next_ref,
    prior_ref,
    rim_out_ref,
    rim_ref,
    tile_ref,
    swap_ref,
    peak_ref,
    tensor_ref,
    result_ref,
    own_sem,
    tensor_sem,
    film_send,
    film_recv,
    twin_send,
    twin_recv,
    plane_send,
    plane_recv,
    back_send,
    back_recv,
    last_send,
    last_recv,
    image_send,
    image_recv,
    rim_send,
    rim_recv,
    swap_send,
    swap_recv,
    peak_send,
    peak_recv,
    table_sem,
):
    fy_ref, fx_ref = tables[:2]
    present_ref, ease_ref = [back_ref.at[0, 0, 0, 0, n] for n in range(2)]
    gx_ref, gy_ref = tables[:2] if len(tables) == 2 else tables[2:]
    groups, local_planes = held_ref.shape[1], held_ref.shape[2]
    slab, columns_full = held_ref.shape[4], held_ref.shape[5]
    layer_count = cells_ref.shape[2]
    rows_full = groups * slab
    parts = groups // 2
    me = lax.axis_index("space")
    half, seat = me // parts, lax.rem(me, parts)
    partner = lax.rem(me + parts, groups)
    flip = (1 - 2 * half).astype(jnp.float32)
    row_step = 8
    images, image = lax.axis_size("image"), lax.axis_index("image")
    first, last = image == 0, image == images - 1
    shifts = (-1, 0, 1)
    routes = [
        (n, shift, d)
        for n, shift in enumerate(shifts)
        for d in range(groups)
        if shift != 0 or d != 0
    ]

    def gate(exists, action):
        if exists is None:
            action()
        else:
            pl.when(exists)(action)

    def receiver(shift):
        return None if shift == 0 else jnp.logical_not(last if shift < 0 else first)

    def sender(shift):
        return None if shift == 0 else jnp.logical_not(first if shift < 0 else last)

    def target_of(shift, d):
        return {"image": lax.rem(image - shift + images, images), "space": lax.rem(me + d, groups)}

    def remote(src, dst, send, recv, target):
        return pltpu.make_async_remote_copy(
            src_ref=src,
            dst_ref=dst,
            send_sem=send,
            recv_sem=recv,
            device_id=target if isinstance(target, dict) else {"space": target},
            device_id_type=pl.DeviceIdType.MESH,
        )

    def row_loop(step):
        def chunk(i, carry):
            step(pl.ds(pl.multiple_of(i * row_step, row_step), row_step))
            return carry

        lax.fori_loop(0, slab // row_step, chunk, 0)

    def own_copy(c):
        return pltpu.make_async_copy(magnet_ref.at[:, c], cells_ref.at[:, c], own_sem.at[c])

    def tensor_copy(q):
        return pltpu.make_async_copy(
            kernel_ref.at[:, q, pl.ds(0, rows_full + 8), pl.ds(0, columns_full + 128)],
            tensor_ref.at[pl.ds(6 * q, 6)],
            tensor_sem.at[q],
        )

    def film_copy(c):
        return remote(
            magnet_ref.at[1 - half, c], film_ref.at[c], film_send.at[c], film_recv.at[c], partner
        )

    def place_of(seat_index, kind):
        return lax.rem((half + kind) * parts + seat_index, groups)

    def plane_copy(c, kind, slot):
        target = lax.rem(seat + 1 + slot, parts)
        return remote(
            send_ref.at[3 if kind else c, slot],
            held_ref.at[c, place_of(seat, kind)],
            plane_send.at[c, kind, slot],
            plane_recv.at[c, kind, parts - 2 - slot],
            half * parts + target,
        )

    def plane_arrival(c, kind, slot):
        source = lax.rem(seat + 1 + slot, parts)
        return remote(
            send_ref.at[3 if kind else c, slot],
            held_ref.at[c, place_of(source, kind)],
            plane_send.at[c, kind, slot],
            plane_recv.at[c, kind, slot],
            half * parts + source,
        )

    def back_copy(c, q, kind, slot):
        target = lax.rem(seat + 1 + slot, parts)
        return remote(
            held_ref.at[c, place_of(target, kind), q],
            back_ref.at[c, kind, parts - 2 - slot, q],
            back_send.at[c, q, kind, slot],
            back_recv.at[c, q, kind, parts - 2 - slot],
            half * parts + target,
        )

    def back_arrival(c, q, kind, slot):
        source = lax.rem(seat + 1 + slot, parts)
        return remote(
            held_ref.at[c, place_of(source, kind), q],
            back_ref.at[c, kind, slot, q],
            back_send.at[c, q, kind, slot],
            back_recv.at[c, q, kind, slot],
            half * parts + source,
        )

    def last_copy(c):
        return remote(
            film_ref.at[c], arrive_ref.at[c], last_send.at[c], last_recv.at[c], partner
        )

    def ahead_copy():
        return remote(
            magnet_ref.at[1],
            prior_ref,
            image_send.at[0],
            image_recv.at[0],
            {"image": lax.rem(image + 1, images)},
        )

    def behind_copy():
        return remote(
            magnet_ref.at[0],
            next_ref,
            image_send.at[1],
            image_recv.at[1],
            {"image": lax.rem(image + images - 1, images)},
        )

    def rim_copy(side):
        return remote(
            rim_out_ref.at[side],
            rim_ref.at[side],
            rim_send.at[side],
            rim_recv.at[side],
            lax.rem(me + (1 if side == 0 else groups - 1), groups),
        )

    def swap_copy(n, shift, d, slot):
        return remote(
            tile_ref, swap_ref.at[n, slot], swap_send.at[n, d], swap_recv.at[n, d], target_of(shift, d)
        )

    def peak_copy(d, slot):
        return remote(
            tile_ref.at[pl.ds(0, 8)],
            peak_ref.at[slot],
            peak_send.at[d],
            peak_recv.at[d],
            lax.rem(me + d, groups),
        )

    def table_copy(n):
        return pltpu.make_async_copy(source_tables[n], tables[n], table_sem.at[n])

    def kernel_copies():
        body = (pl.ds(0, rows_full), pl.ds(0, columns_full))
        far = (pl.ds(rows_full, 8), pl.ds(0, columns_full + 128))
        twin = 6 * local_planes
        pieces = [(tensor_ref.at[n, *body], tensor_ref.at[twin + n, *body]) for n in (0, 3)]
        pieces += [
            (edge_out_ref, edge_ref),
            (tensor_ref.at[pl.ds(0, 3), *far], tensor_ref.at[pl.ds(twin, 3), *far]),
        ]
        pieces += [(tensor_ref.at[n, *body], tensor_ref.at[twin + n, *body]) for n in (1, 2)]
        return [
            remote(src, dst, twin_send.at[n], twin_recv.at[n], partner)
            for n, (src, dst) in enumerate(pieces)
        ]

    def pack_edges():
        rows, columns = pl.ds(0, rows_full), pl.ds(columns_full, 128)
        lane_pos = lax.broadcasted_iota(jnp.int32, (rows_full, 128), 1)
        edge = tensor_ref[0, rows, columns]
        for c in (1, 2):
            edge = jnp.where(lane_pos == c, pltpu.roll(tensor_ref[c, rows, columns], c, 1), edge)
        edge_out_ref[...] = edge

    def unpack_edges():
        rows, columns = pl.ds(0, rows_full), pl.ds(columns_full, 128)
        edge = edge_ref[...]
        for c in range(3):
            tensor_ref[6 * local_planes + c, rows, columns] = pltpu.roll(edge, 128 - c, 1) if c else edge

    def transform_layers(c, kind):
        place = place_of(seat, kind)

        def variant(here):
            def step(rows):
                if kind == 0:
                    layers = [cells_ref[half, c, z, rows, :] for z in range(layer_count)]
                else:
                    layers = [film_ref[c, z, rows, :] for z in range(layer_count)]
                layers = [v * flip if z % 2 else v for z, v in enumerate(layers)]
                spectrum = layers_to_spectrum(layers)
                for k in range(layer_count):
                    target, q = k // local_planes, k % local_planes
                    slot = (target - here) % parts - 1
                    for part in range(2):
                        if target == here:
                            held_ref[c, place, q, part, rows, :] = spectrum[k][part]
                        else:
                            send_ref[3 if kind else c, slot, q, part, rows, :] = spectrum[k][part]

            row_loop(step)

        for here in range(parts):
            pl.when(seat == here)(functools.partial(variant, here))
        for slot in range(parts - 1):
            plane_copy(c, kind, slot).start()

    def transform_planes(c, kind):
        place = place_of(seat, kind)

        def variant(here):
            def step(rows):
                spectrum = []
                for k in range(layer_count):
                    source, q = k // local_planes, k % local_planes
                    slot = (source - here) % parts - 1
                    if source == here:
                        spectrum.append(
                            [held_ref[c, place, q, part, rows, :] for part in range(2)]
                        )
                    else:
                        spectrum.append(
                            [back_ref[c, kind, slot, q, part, rows, :] for part in range(2)]
                        )
                for z, value in enumerate(spectrum_to_layers(spectrum)):
                    value = value * (scale * flip if z % 2 else scale)
                    if kind == 0:
                        field_ref[half, c, z, rows, :] = field_ref[half, c, z, rows, :] + value
                    else:
                        film_ref[c, z, rows, :] = value

            row_loop(step)

        for here in range(parts):
            pl.when(seat == here)(functools.partial(variant, here))

    def fill_rims():
        def step(f, carry):
            i, c = f // 3, lax.rem(f, 3)
            for side in range(2):
                row = slab - 1 if side == 0 else 0
                rim_out_ref[side, i, c] = jnp.concatenate(
                    [cells_ref[i, c, z, row : row + 1, :] for z in range(layer_count)], axis=0
                )
            return carry

        lax.fori_loop(0, 6, step, 0)
        row_pos = lax.broadcasted_iota(jnp.int32, (slab, columns_full), 0) + me * slab
        column_pos = lax.broadcasted_iota(jnp.int32, (slab, columns_full), 1)
        faces = [row_pos == 0, row_pos == rows_full - 1]
        faces += [column_pos == 0, column_pos == columns_full - 1]
        present_ref[...] = 6.0 - sum(jnp.where(face, 1.0, 0.0) for face in faces)
        for side in range(2):
            open_side = me != groups - 1 if side == 0 else me != 0

            @pl.when(open_side)
            def _():
                rim_copy(side).start()

            no_source = me == 0 if side == 0 else me == groups - 1

            @pl.when(no_source)
            def _():
                rim_ref[side] = jnp.zeros(rim_ref.shape[1:], jnp.float32)

    def wait_rims():
        for side in range(2):
            has_source = me != 0 if side == 0 else me != groups - 1

            @pl.when(has_source)
            def _():
                rim_copy(side).wait_recv()

    def local_fields(i):
        row_pos = lax.broadcasted_iota(jnp.int32, (slab, columns_full), 0)
        column_pos = lax.broadcasted_iota(jnp.int32, (slab, columns_full), 1)

        def step(z, carry):
            below, above = jnp.maximum(z - 1, 0), jnp.minimum(z + 1, layer_count - 1)
            has_below = (z > 0).astype(jnp.float32)
            has_above = (z < layer_count - 1).astype(jnp.float32)
            present = present_ref[...] - (2.0 - has_below - has_above)
            tilt = []
            for c in range(3):
                cells = cells_ref[i, c, z]
                x_plus = jnp.where(
                    row_pos == slab - 1,
                    rim_ref[1, i, c, pl.ds(z, 1), :],
                    pltpu.roll(cells, slab - 1, 0),
                )
                x_minus = jnp.where(
                    row_pos == 0, rim_ref[0, i, c, pl.ds(z, 1), :], pltpu.roll(cells, 1, 0)
                )
                y_plus = jnp.where(
                    column_pos == columns_full - 1, 0.0, pltpu.roll(cells, columns_full - 1, 1)
                )
                y_minus = jnp.where(column_pos == 0, 0.0, pltpu.roll(cells, 1, 1))
                around = x_plus + x_minus + y_plus + y_minus
                around = around + has_above * cells_ref[i, c, above] + has_below * cells_ref[i, c, below]
                part = exchange_strength * (around - present * cells)
                if c == 0:
                    tilt.append(x_plus - x_minus)
                    field_ref[i, 0, z] = part
                elif c == 1:
                    tilt.append(y_plus - y_minus)
                    field_ref[i, 1, z] = part
                else:
                    ease = ease_ref[...] * cells
                    field_ref[i, 2, z] = part + (ease - chiral_strength * (tilt[0] + tilt[1]))
                    field_ref[i, 0, z] = field_ref[i, 0, z] + chiral_strength * (x_plus - x_minus)
                    field_ref[i, 1, z] = field_ref[i, 1, z] + chiral_strength * (y_plus - y_minus)
            return carry

        lax.fori_loop(0, layer_count, step, 0)

    lane = columns_full

    def cell_loop(step, carry):
        unrolled = min(4, slab // row_step)
        steps = slab // (unrolled * row_step)

        def chunk(index, carry):
            z = index // steps
            start = lax.rem(index, steps) * unrolled * row_step
            for n in range(unrolled):
                carry = step(z, pl.multiple_of(start + n * row_step, row_step), carry)
            return carry

        return lax.fori_loop(0, layer_count * steps, chunk, carry)

    def get_sum(i, k):
        return result_ref[i, row_step * k : row_step * (k + 1), 0:lane]

    def put_sum(i, k, value):
        result_ref[i, row_step * k : row_step * (k + 1), 0:lane] = value

    def zeros(count):
        return tuple(jnp.zeros((row_step, lane), jnp.float32) for _ in range(count))

    def tangent_rows(z, start):
        return pl.ds(pl.multiple_of(z * slab + start, row_step), row_step)

    def neighbour_sums():
        @pl.when(jnp.logical_not(first))
        def _():
            ahead_copy().wait_recv()

        @pl.when(first)
        def _():
            for c in range(3):
                prior_ref[c] = cells_ref[0, c]

        @pl.when(jnp.logical_not(last))
        def _():
            behind_copy().wait_recv()

        @pl.when(last)
        def _():
            for c in range(3):
                next_ref[c] = cells_ref[1, c]

        for i in range(2):

            def step(z, start, carry):
                rows = pl.ds(start, row_step)
                here = [cells_ref[i, c, z, rows, :] for c in range(3)]
                if i == 0:
                    ahead = [cells_ref[1, c, z, rows, :] for c in range(3)]
                    behind = [prior_ref[c, z, rows, :] for c in range(3)]
                else:
                    ahead = [next_ref[c, z, rows, :] for c in range(3)]
                    behind = [cells_ref[0, c, z, rows, :] for c in range(3)]
                normal = [
                    here[1] * ahead[2] - here[2] * ahead[1],
                    here[2] * ahead[0] - here[0] * ahead[2],
                    here[0] * ahead[1] - here[1] * ahead[0],
                ]
                angle = arc_angle(jnp.sqrt(dot3(normal, normal)), dot3(here, ahead))
                ahead = [ahead[c] - here[c] for c in range(3)]
                behind = [here[c] - behind[c] for c in range(3)]
                ahead_on, behind_on = dot3(ahead, here), dot3(behind, here)
                ahead = [ahead[c] - ahead_on * here[c] for c in range(3)]
                behind = [behind[c] - behind_on * here[c] for c in range(3)]
                for c in range(3):
                    place = tangent_rows(z, start)
                    spec_ref[0, 3 * i + c, place, 0:columns_full] = ahead[c]
                    spec_ref[0, 3 * i + c, place, columns_full : 2 * columns_full] = behind[c]
                values = (
                    angle * angle,
                    dot3(ahead, ahead),
                    dot3(ahead, behind),
                    dot3(behind, behind),
                )
                return tuple(total + value for total, value in zip(carry, values))

            totals = cell_loop(step, zeros(4))
            for k in range(4):
                put_sum(i, k + 1, totals[k])

    def field_sums(i, c, arrived):
        def step(z, start, carry):
            rows = pl.ds(start, row_step)
            place = tangent_rows(z, start)
            field = field_ref[i, c, z, rows, :]
            if arrived:
                field = field + arrive_ref[c, z, rows, :]
                field_ref[i, c, z, rows, :] = field
            values = (
                cells_ref[i, c, z, rows, :] * field,
                field * spec_ref[0, 3 * i + c, place, 0:columns_full],
                field * spec_ref[0, 3 * i + c, place, columns_full : 2 * columns_full],
            )
            return tuple(total + value for total, value in zip(carry, values))

        totals = cell_loop(step, zeros(3))
        for k, slot in enumerate((0, 5, 6)):
            put_sum(i, slot, totals[k] if c == 0 else get_sum(i, slot) + totals[k])

    barrier = pltpu.get_barrier_semaphore()
    for n, shift, d in routes:
        signal = functools.partial(
            pl.semaphore_signal,
            barrier,
            inc=1,
            device_id=target_of(shift, d),
            device_id_type=pl.DeviceIdType.MESH,
        )
        gate(receiver(shift), signal)
    for c in range(3):
        own_copy(c).start()
    for n in range(len(tables)):
        table_copy(n).start()

    def spread(r, carry):
        ease_ref[pl.ds(r, 1), :] = jnp.full((1, columns_full), 2.0 * anisotropy_ref[r])
        return carry

    lax.fori_loop(0, slab, spread, 0)
    ends = first.astype(jnp.int32) + last.astype(jnp.int32)
    pl.semaphore_wait(barrier, len(routes) - groups * ends)
    film_copy(0).start()

    @pl.when(jnp.logical_not(last))
    def _():
        ahead_copy().start()

    @pl.when(jnp.logical_not(first))
    def _():
        behind_copy().start()

    for c in range(3):
        own_copy(c).wait()
    fill_rims()
    for c in range(1, 3):
        film_copy(c).start()

    for q in range(local_planes):
        tensor_copy(q).start()

    for c in range(3):
        transform_layers(c, 0)
    for n in range(len(tables)):
        table_copy(n).wait()
    tensor_copy(0).wait()

    @pl.when(seat == 0)
    def _():
        pack_edges()
        for copy in kernel_copies():
            copy.start()

    for c in range(3):
        film_copy(c).wait_recv()
        if c > 0:
            for slot in range(parts - 1):
                plane_copy(c - 1, 1, slot).wait_send()
        transform_layers(c, 1)
        for kind in range(2):
            for slot in range(parts - 1):
                plane_arrival(c, kind, slot).wait_recv()

        def forward(i, carry):
            fy = jnp.concatenate([fy_ref[0], fy_ref[0], fy_ref[1]], axis=0)
            fx = jnp.concatenate([fx_ref[0], fx_ref[0], fx_ref[1]], axis=1)
            places = [(width * i + n, part) for n in range(width) for part in range(2)]
            cells = jnp.concatenate(
                [held_ref[c, g, q, part] for q, part in places for g in range(groups)], axis=0
            )
            lines = dot32(three_limbs(cells, 1), fy)
            for n, (q, part) in enumerate(places):
                spec_ref[q, 2 * c + part] = dot32(
                    fx, three_limbs(lines[n * rows_full : (n + 1) * rows_full], 0)
                )
            return carry

        width = math.gcd(local_planes, 2)
        lax.fori_loop(0, local_planes // width, forward, 0)
        if c == 0:
            wait_rims()
        if c < 2:
            local_fields(c)

    for q in range(1, local_planes):
        tensor_copy(q).wait()

    for c in range(3):

        def backward(i, carry):
            q = local_planes - 1 - i
            twin = (seat == 0) & (q == 0)

            @pl.when(twin)
            def _():
                for copy in kernel_copies()[:4] if c == 0 else kernel_copies()[c + 3 : c + 4]:
                    copy.wait_recv()
                if c == 0:
                    unpack_edges()

            second = jnp.where(twin, local_planes, q)
            kernels = (tensor_ref.at[pl.ds(6 * q, 6)], tensor_ref.at[pl.ds(6 * second, 4)])
            tensor_part(c, spec_ref.at[q], kernels, result_ref)
            gx = jnp.concatenate([gx_ref[0], gx_ref[0], gx_ref[1]], axis=1)
            gy = jnp.concatenate([gy_ref[0], gy_ref[0], gy_ref[1]], axis=0)
            lines = [dot32(gx, three_limbs(result_ref[part], 0)) for part in range(2)]
            cells = dot32(three_limbs(jnp.concatenate(lines, axis=0), 1), gy)
            for part in range(2):
                for g in range(groups):
                    start = part * rows_full + g * slab
                    held_ref[c, g, q, part] = cells[start : start + slab]
            for kind in (1, 0):
                for slot in range(parts - 1):
                    back_copy(c, q, kind, slot).start()

            return carry

        lax.fori_loop(0, local_planes, backward, 0)
        for kind in (1, 0):
            for q in range(local_planes):
                for slot in range(parts - 1):
                    back_arrival(c, q, kind, slot).wait_recv()
            transform_planes(c, kind)
            if kind == 1:
                last_copy(c).start()

    neighbour_sums()
    for c in range(3):
        field_sums(half, c, False)
    for c in range(3):
        last_copy(c).wait_recv()
        field_sums(1 - half, c, True)

    rows = [
        jnp.sum(get_sum(i, k), axis=0, keepdims=True) for i in range(2) for k in range(7)
    ] + [jnp.zeros((1, lane), jnp.float32)] * 2
    tile = jnp.sum(jnp.concatenate(rows, axis=0), axis=1, keepdims=True)
    tile_ref[...] = jnp.broadcast_to(tile, tile_ref.shape)
    for n, shift, d in routes:
        gate(receiver(shift), swap_copy(n, shift, d, me).start)
    swap_ref[1, me] = tile_ref[...]
    for n, end in ((0, first), (2, last)):

        @pl.when(end)
        def _():
            swap_ref[n] = jnp.zeros(swap_ref.shape[1:], jnp.float32)

    for n, shift, d in routes:
        gate(sender(shift), swap_copy(n, shift, d, lax.rem(me + groups - d, groups)).wait_recv)
    totals = []
    for n in range(3):
        total = swap_ref[n, 0]
        for g in range(1, groups):
            total = total + swap_ref[n, g]
        totals.append(total)

    def entry(n, i, k):
        return totals[n][7 * i + k : 7 * i + k + 1]

    cell_count = float(layer_count * rows_full * columns_full)
    energies = [-0.5 * entry(*at, 0) for at in ((0, 1), (1, 0), (1, 1), (2, 0))]
    distances = [jnp.sqrt(entry(*at, 1) / cell_count) for at in ((0, 1), (1, 0), (1, 1))]
    pulls = []
    for i in range(2):
        weight_next, weight_prior = tangent_weights(energies[i + 1], energies[i + 2], energies[i])
        length_square = (
            weight_next * weight_next * entry(1, i, 2)
            + 2.0 * weight_next * weight_prior * entry(1, i, 3)
            + weight_prior * weight_prior * entry(1, i, 4)
        )
        drive = weight_next * entry(1, i, 5) + weight_prior * entry(1, i, 6)
        size = jnp.sqrt(jnp.maximum(length_square, 0.0) / cell_count + epsilon)
        spring = spring_strength * (distances[i + 1] - distances[i])
        pull = (spring - drive / (cell_count * size)) / size
        pulls.append((pull * weight_next, pull * weight_prior))
    for n, shift, d in routes:
        gate(receiver(shift), swap_copy(n, shift, d, me).wait_send)
    peaks = []
    for i in range(2):
        end = first if i == 0 else last
        ahead_pull, behind_pull = [
            jnp.concatenate([jnp.broadcast_to(pull, (row_step, 128))] * (lane // 128), axis=1)
            for pull in pulls[i]
        ]

        def step(z, start, peak):
            rows = pl.ds(start, row_step)
            place = tangent_rows(z, start)
            here = [cells_ref[i, c, z, rows, :] for c in range(3)]
            force = []
            for c in range(3):
                ahead = spec_ref[0, 3 * i + c, place, 0:columns_full]
                behind = spec_ref[0, 3 * i + c, place, columns_full : 2 * columns_full]
                field = field_ref[i, c, z, rows, :]
                force.append(field + ahead_pull * ahead + behind_pull * behind)
            along = dot3(force, here)
            force = [jnp.where(end, 0.0, force[c] - along * here[c]) for c in range(3)]
            for c in range(3):
                field_ref[i, c, z, rows, :] = force[c]
            return (jnp.maximum(peak[0], dot3(force, force)),)

        (peak,) = cell_loop(step, zeros(1))
        peaks.append(jnp.max(peak, axis=0, keepdims=True))
    peak = jnp.concatenate(peaks + [jnp.zeros((6, lane), jnp.float32)], axis=0)
    peak = jnp.broadcast_to(jnp.max(peak, axis=1, keepdims=True), (8, 128))
    tile_ref[0:8] = peak
    for d in range(1, groups):
        peak_copy(d, me).start()
    peak_ref[me] = peak
    for d in range(1, groups):
        peak_copy(d, lax.rem(me + groups - d, groups)).wait_recv()
    largest = peak_ref[0]
    for g in range(1, groups):
        largest = jnp.maximum(largest, peak_ref[g])
    moves = jnp.minimum(step_limit, rotation_limit / (jnp.sqrt(largest) + epsilon))
    energy = jnp.concatenate(energies[1:3], axis=0) / cell_count
    small_ref[...] = jnp.concatenate([moves[0:2], energy, jnp.zeros((4, 128), jnp.float32)], axis=0)
    for d in range(1, groups):
        peak_copy(d, me).wait_send()
    for c in range(3):
        film_copy(c).wait_send()
        last_copy(c).wait_send()
        for kind in range(2):
            for slot in range(parts - 1):
                if kind == 0 or c == 2:
                    plane_copy(c, kind, slot).wait_send()
                for q in range(local_planes):
                    back_copy(c, q, kind, slot).wait_send()

    @pl.when(seat == 0)
    def _():
        for copy in kernel_copies():
            copy.wait_send()

    for side in range(2):
        open_side = me != groups - 1 if side == 0 else me != 0

        @pl.when(open_side)
        def _():
            rim_copy(side).wait_send()

    @pl.when(jnp.logical_not(last))
    def _():
        ahead_copy().wait_send()

    @pl.when(jnp.logical_not(first))
    def _():
        behind_copy().wait_send()


def band_step(magnet, anisotropy, kernel):
    layer_count, row_count, column_count = magnet.shape[2:]
    groups = lax.axis_size("space")
    local_planes = 2 * layer_count // groups
    full_rows = row_count * groups
    slots = groups // 2 - 1
    table_y = parity_table(column_count)
    table_x = parity_table(full_rows)
    square = full_rows == column_count
    tables = [table_limbs(t) for t in (table_y, table_x.T, table_x, table_y.T)][: 2 if square else 4]

    def entry(magnet_ref, kernel_ref, anisotropy_ref, *refs):
        count = len(tables)
        sources, outs = refs[:count], refs[count : count + 2]
        held, rest = refs[count + 2 : 2 * count + 2], refs[2 * count + 2 :]
        scale = -4.0 / padded_cells
        band_kernel(
            scale, magnet_ref, kernel_ref, anisotropy_ref, sources, *outs, held, *rest
        )

    slab = (row_count, column_count)
    film = (layer_count,) + slab
    block = (local_planes, 2) + slab
    anywhere = pl.BlockSpec(memory_space=pl.ANY)
    inside = pl.BlockSpec(memory_space=pltpu.VMEM)
    dots = 6 * local_planes * 4 * full_rows * column_count * 3 * (full_rows + column_count // 2)
    padded_cells = 8 * layer_count * full_rows * column_count
    signals = pltpu.SemaphoreType.DMA
    scratch = [
        (2, 3) + film,
        (3,) + film,
        (full_rows, 128),
        (full_rows, 128),
        (4, slots) + block,
        (3, 2, slots) + block,
        (3, groups) + block,
        (local_planes, 6, 2 * full_rows, 2 * column_count),
        (3,) + film,
        (3,) + film,
        (3,) + film,
        (2, 2, 3, layer_count, column_count),
        (2, 2, 3, layer_count, column_count),
        (16, 128),
        (3, groups, 16, 128),
        (groups, 8, 128),
        (6 * local_planes + 4, full_rows + 8, column_count + 128),
    ]
    semaphores = [
        (3,),
        (local_planes,),
        (3,),
        (3,),
        (6,),
        (6,),
        (3, 2, slots),
        (3, 2, slots),
        (3, local_planes, 2, slots),
        (3, local_planes, 2, slots),
        (3,),
        (3,),
        (2,),
        (2,),
        (2,),
        (2,),
        (3, groups),
        (3, groups),
        (groups,),
        (groups,),
        (len(tables),),
    ]
    return pl.pallas_call(
        entry,
        in_specs=[anywhere, anywhere, pl.BlockSpec(memory_space=pltpu.SMEM)]
        + [anywhere] * len(tables),
        out_specs=[inside, inside],
        out_shape=[
            pltpu.VMEM(magnet.shape, jnp.float32),
            jax.ShapeDtypeStruct((8, 128), jnp.float32),
        ],
        scratch_shapes=[pltpu.VMEM(t.shape, jnp.bfloat16) for t in tables]
        + [pltpu.VMEM(dims, jnp.float32) for dims in scratch]
        + [pltpu.VMEM((2, 2 * full_rows, 2 * column_count), jnp.float32)]
        + [signals(dims) for dims in semaphores],
        compiler_params=pltpu.CompilerParams(
            vmem_limit_bytes=67043328 - 4 * magnet.size, collective_id=0, has_side_effects=True
        ),
        cost_estimate=pl.CostEstimate(
            flops=4 * dots, bytes_accessed=4 * magnet.size * 4, transcendentals=0
        ),
        name="band_kernel",
    )(magnet, kernel, anisotropy, *[jnp.asarray(t) for t in tables])


def move_kernel(
    small_ref,
    magnet_ref,
    force_ref,
    updated_ref,
    out_ref,
    energy_ref,
    cells_ref,
    cells_sem,
    updated_sem,
    out_sem,
):
    images, _, layer_count, slab, columns = cells_ref.shape
    pieces = updated_sem.shape[1]
    layers = layer_count // pieces

    def piece_copy(src, dst, sem, i, k):
        part = pl.ds(k * layers, layers)
        return pltpu.make_async_copy(src.at[i, :, part], dst.at[i, :, part], sem.at[i, k])

    def out_copy(i):
        return pltpu.make_async_copy(force_ref.at[i], out_ref.at[i], out_sem.at[i])

    places = [(i, k) for i in range(images) for k in range(pieces)]
    for i, k in places:
        piece_copy(magnet_ref, cells_ref, cells_sem, i, k).start()
    for i in range(images):
        out_copy(i).start()
    for n in range(images):
        energy_ref[n] = jnp.max(small_ref[n + 2 : n + 3, :])
    row_step = 8
    unrolled = min(4, slab // row_step)
    steps = slab // (unrolled * row_step)
    for i, k in places:
        move = jnp.broadcast_to(small_ref[i : i + 1, :], (row_step, 128))
        move = jnp.concatenate([move] * (columns // 128), axis=1)

        piece_copy(magnet_ref, cells_ref, cells_sem, i, k).wait()

        def chunk(index, carry):
            z = k * layers + index // steps
            for n in range(unrolled):
                start = (lax.rem(index, steps) * unrolled + n) * row_step
                rows = pl.ds(pl.multiple_of(start, row_step), row_step)
                moved = [
                    cells_ref[i, c, z, rows, :] + move * force_ref[i, c, z, rows, :]
                    for c in range(3)
                ]
                inverse = lax.rsqrt(dot3(moved, moved))
                for c in range(3):
                    cells_ref[i, c, z, rows, :] = inverse * moved[c]
            return carry

        lax.fori_loop(0, layers * steps, chunk, 0)
        piece_copy(cells_ref, updated_ref, updated_sem, i, k).start()
    for i in range(images):
        out_copy(i).wait()
    for i, k in places:
        piece_copy(cells_ref, updated_ref, updated_sem, i, k).wait()


def move_images(magnet, force, small):
    images, _, layer_count = magnet.shape[:3]
    pieces = math.gcd(layer_count, 4)
    inside = pl.BlockSpec(memory_space=pltpu.VMEM)
    anywhere = pl.BlockSpec(memory_space=pl.ANY)
    return pl.pallas_call(
        move_kernel,
        in_specs=[inside, anywhere, inside],
        out_specs=[anywhere, anywhere, pl.BlockSpec(memory_space=pltpu.SMEM)],
        out_shape=[
            jax.ShapeDtypeStruct(magnet.shape, jnp.float32),
            jax.ShapeDtypeStruct(magnet.shape, jnp.float32),
            jax.ShapeDtypeStruct((images,), jnp.float32),
        ],
        scratch_shapes=[
            pltpu.VMEM(magnet.shape, jnp.float32),
            pltpu.SemaphoreType.DMA((images, pieces)),
            pltpu.SemaphoreType.DMA((images, pieces)),
            pltpu.SemaphoreType.DMA((images,)),
        ],
        name="move_kernel",
    )(small, magnet, pltpu.with_memory_space_constraint(force, pltpu.VMEM))


def body(magnet, anisotropy, kernel):
    force, small = band_step(magnet, anisotropy, kernel)
    return move_images(magnet, force, small)


def solution(mesh):
    in_specs = (P("image", None, None, "space", None), P("space"), P(None, "space", None, None))
    out_specs = (
        P("image", None, None, "space", None),
        P("image", None, None, "space", None),
        P("image"),
    )
    return jax.shard_map(body, mesh=mesh, in_specs=in_specs, out_specs=out_specs, check_vma=False)
```
